32 devices in a mesh: grp: 2 (over y), pts: 8 (over z, x), sen: 2 (over core).
Axes of the slice: x: 2, y: 2, z: 4, core: 2. Of those that a mesh axis runs over, the one named last changes fastest.
Arguments:
- probes: bfloat16 [16, 64, 420], P(None, ('grp', 'pts')), parts along dimension 1, may hold values from -6 to 6
- kernel: bfloat16 [2, 64, 128, 421], P(None, ('grp', 'pts'), 'sen'), parts along dimension 1, may hold values from -1 to 1
- noise_weight: float32 [256], P(('grp', 'sen')), parts along dimension 0, may hold values from 0.3 to 3
- prior_scale: float32 [32], P('pts'), may hold values from 0.3 to 3
- basis: bfloat16 [13440, 1024], P('pts', 'sen'), may hold values from -0.15625 to 0.15625
- deflation: float32 [1024], P('sen'), may hold values from 0.3 to 0.95
Outputs:
- deflated: float32 [16, 64, 420], P(None, ('grp', 'pts')), parts along dimension 1
The draws below stay inside these ranges and needn't reach their ends.
There are 2 independent parts, one for each index of `grp`. The reference program is written for one: setup_inputs(seed, part) draws one part's arguments, and reference() takes and returns one part's arrays. A program takes and returns all parts, laid end to end along the dimension named above; an argument that names none is the same for every part. Nothing has to cross between parts.
All inputs are finite; a program needn't handle non-finite values.
Results may differ from the reference program's by a relative error of at most 0.015.
Values may be sent and summed in bfloat16 or wider, within the bound.
No kernel may reach another device: no remote copies, remote signals or barrier semaphores. Data moves between devices by JAX's collectives and lax.ppermute only.
A program may use at most 64 MiB of HBM per device.

```python
import math
import jax
import jax.numpy as jnp
from jax import lax

NPROBE = 16
STEPS = 420
RANK = 1024
BINS = 421
POINTS = 32
SENSORS = 128
PARAM = 13440


def shard_levels(key, extent, pieces, least, top_value):
    loudness = 1.0
    for dim, shards_of in pieces:
        draws = jax.random.uniform(jax.random.fold_in(jax.random.fold_in(key, 6), dim), (shards_of,), jnp.float32, least / len(pieces), top_value / len(pieces))
        loudness = loudness * jnp.repeat(jnp.exp(draws), extent[dim] // shards_of).reshape((-1,) + (1,) * (len(extent) - 1 - dim))
    return loudness


def normal_values(key, extent, deviation, most, split=(), kind=jnp.bfloat16):
    factor_of = shard_levels(key, extent, split, -0.22, 0.18) if split else 1.0
    drawn = jax.random.normal(key, extent, jnp.float32) * deviation * factor_of
    return jnp.minimum(jnp.maximum(drawn, -most), most).astype(kind)


def setup_inputs(seed: int = 0, part: int = 0) -> dict:
    streams_of = jax.random.split(jax.random.key(seed), 7)
    part_splits = jax.random.split(jax.random.fold_in(streams_of[6], part), 7)
    return {
        "probes": normal_values(part_splits[0], (NPROBE, POINTS, STEPS), 1.0, 6.0, ((1, 8),)),
        "kernel": normal_values(part_splits[1], (2, POINTS, SENSORS, BINS), POINTS ** -0.5, 1.0, ((1, 8), (2, 2))),
        "noise_weight": jnp.clip(jnp.exp(math.log(3.0) - 2.3025851 * jax.random.uniform(part_splits[2], (SENSORS,), jnp.float32) ** shard_levels(part_splits[2], (SENSORS,), ((0, 2),), -0.2, 0.2)), 0.3, 3.0),
        "prior_scale": jnp.clip(jnp.exp(math.log(3.0) - 2.3025851 * jax.random.uniform(streams_of[3], (POINTS,), jnp.float32) ** shard_levels(streams_of[3], (POINTS,), ((0, 8),), -0.2, 0.2)), 0.3, 3.0),
        "basis": normal_values(streams_of[4], (PARAM, RANK), (PARAM // 8) ** -0.5, 0.15625, ((0, 8), (1, 2))),
        "deflation": jnp.clip(0.3 + 0.65 * jax.random.uniform(streams_of[5], (RANK,), jnp.float32) ** shard_levels(streams_of[5], (RANK,), ((0, 2),), -0.2, 0.2), 0.3, 0.95),
    }


def tables(steps_count):
    bins_count = steps_count + 1
    turns = (jnp.arange(steps_count, dtype=jnp.int32)[:, None] * jnp.arange(bins_count, dtype=jnp.int32)[None, :]) % (2 * steps_count)
    angle = turns.astype(jnp.float32) * (math.pi / steps_count)
    cosine = jnp.cos(angle)
    sine = jnp.sin(angle)
    freq = jnp.arange(bins_count, dtype=jnp.int32)
    edge = (freq == 0) | (freq == steps_count)
    weights = jnp.where(edge, 1.0, 2.0).astype(jnp.float32) / (2.0 * steps_count)
    forward = jnp.concatenate([cosine, -sine], axis=1)
    inverse = jnp.concatenate([cosine * weights[None, :], -sine * weights[None, :]], axis=1)
    return forward, inverse


def rounded(value):
    return lax.optimization_barrier(value.astype(jnp.bfloat16)).astype(jnp.float32)


def reference(probes, kernel, noise_weight, prior_scale, basis, deflation):
    highest = lax.Precision.HIGHEST
    forward, inverse = tables(STEPS)
    bins_count = STEPS + 1
    scaled = probes.astype(jnp.float32) * prior_scale[None, :, None]
    spectrum = rounded(jnp.dot(scaled, forward, precision=highest))
    spec_real = spectrum[..., :bins_count]
    spec_imag = spectrum[..., bins_count:]
    kern = kernel.astype(jnp.float32)
    kern_real = kern[0]
    kern_imag = kern[1]
    data_real = jnp.einsum("kpf,psf->ksf", spec_real, kern_real, precision=highest) - jnp.einsum("kpf,psf->ksf", spec_imag, kern_imag, precision=highest)
    data_imag = jnp.einsum("kpf,psf->ksf", spec_real, kern_imag, precision=highest) + jnp.einsum("kpf,psf->ksf", spec_imag, kern_real, precision=highest)
    data = jnp.concatenate([data_real, data_imag], axis=-1)
    observed = jnp.dot(data, inverse.T, precision=highest)
    residual = rounded(observed * noise_weight[None, :, None])
    weighted = rounded(jnp.dot(residual, inverse, precision=highest))
    weight_real = weighted[..., :bins_count]
    weight_imag = weighted[..., bins_count:]
    adj_real = jnp.einsum("ksf,psf->kpf", weight_real, kern_real, precision=highest) + jnp.einsum("ksf,psf->kpf", weight_imag, kern_imag, precision=highest)
    adj_imag = jnp.einsum("ksf,psf->kpf", weight_imag, kern_real, precision=highest) - jnp.einsum("ksf,psf->kpf", weight_real, kern_imag, precision=highest)
    back = jnp.dot(jnp.concatenate([adj_real, adj_imag], axis=-1), forward.T, precision=highest)
    hessian = back * prior_scale[None, :, None]
    flat = hessian.reshape(NPROBE, POINTS * STEPS)
    flat_low = flat.astype(jnp.bfloat16)
    coeff = jnp.dot(flat_low, basis, preferred_element_type=jnp.float32)
    shrunk = (coeff * deflation[None, :]).astype(jnp.bfloat16)
    correction = jnp.dot(shrunk, basis.T, preferred_element_type=jnp.float32)
    return (flat - correction).reshape(NPROBE, POINTS, STEPS)
```

```python
import functools
import math

import jax
import jax.numpy as jnp
import numpy as np
from jax import lax
from jax.experimental import pallas as pl
from jax.experimental.pallas import tpu as pltpu
from jax.sharding import PartitionSpec as P

LANES = 128
ROWS = 8


def tables(steps_count):
    bins_count = steps_count + 1
    turns = (
        jnp.arange(steps_count, dtype=jnp.int32)[:, None]
        * jnp.arange(bins_count, dtype=jnp.int32)[None, :]
        % (2 * steps_count)
    )
    angle = turns.astype(jnp.float32) * (math.pi / steps_count)
    cosine = jnp.cos(angle)
    sine = jnp.sin(angle)
    freq = jnp.arange(bins_count, dtype=jnp.int32)
    edge = (freq == 0) | (freq == steps_count)
    weights = jnp.where(edge, 1.0, 2.0).astype(jnp.float32) / (2.0 * steps_count)
    forward = jnp.concatenate([cosine, -sine], axis=1)
    inverse = jnp.concatenate([cosine * weights[None, :], -sine * weights[None, :]], axis=1)
    return (forward, inverse)


def widened(value):
    return lax.optimization_barrier(value).astype(jnp.float32)


def complex_data(spec_real, spec_imag, kern_real, kern_imag):
    data_real = jnp.einsum(
        "kpf,psf->ksf", spec_real, kern_real, preferred_element_type=jnp.float32
    ) - jnp.einsum("kpf,psf->ksf", spec_imag, kern_imag, preferred_element_type=jnp.float32)
    data_imag = jnp.einsum(
        "kpf,psf->ksf", spec_real, kern_imag, preferred_element_type=jnp.float32
    ) + jnp.einsum("kpf,psf->ksf", spec_imag, kern_real, preferred_element_type=jnp.float32)
    return (data_real, data_imag)


def complex_adjoint(weight_real, weight_imag, kern_real, kern_imag):
    adj_real = jnp.einsum(
        "ksf,psf->kpf", weight_real, kern_real, preferred_element_type=jnp.float32
    ) + jnp.einsum("ksf,psf->kpf", weight_imag, kern_imag, preferred_element_type=jnp.float32)
    adj_imag = jnp.einsum(
        "ksf,psf->kpf", weight_imag, kern_real, preferred_element_type=jnp.float32
    ) - jnp.einsum("ksf,psf->kpf", weight_real, kern_imag, preferred_element_type=jnp.float32)
    return (adj_real, adj_imag)


def local(probes, kernel, noise_weight, prior_scale, basis, deflation):
    highest = lax.Precision.HIGHEST
    probe_count, point_count, steps_count = probes.shape
    bins_count = steps_count + 1
    sensor_count = noise_weight.shape[0]
    forward, inverse = tables(steps_count)
    scaled = probes.astype(jnp.float32) * prior_scale[None, :, None]
    spectrum = jnp.dot(scaled, forward, precision=highest).astype(jnp.bfloat16)
    noise_rows = jnp.tile(noise_weight, probe_count)
    width = lax.axis_size("pts")
    block = (bins_count + width - 1) // width
    extra = block * width - bins_count
    kern_pad = jnp.pad(kernel, ((0, 0), (0, 0), (0, 0), (0, extra)))
    spec_pad = jnp.pad(
        spectrum.reshape(probe_count, point_count, 2, bins_count),
        ((0, 0), (0, 0), (0, 0), (0, extra)),
    )
    kern_bins, spec_bins = (
        lax.all_to_all(kern_pad, "pts", split_axis=3, concat_axis=1, tiled=True),
        lax.all_to_all(spec_pad, "pts", split_axis=3, concat_axis=1, tiled=True),
    )
    bin_kern_real = kern_bins[0]
    bin_kern_imag = kern_bins[1]
    data_real, data_imag = complex_data(
        spec_bins[:, :, 0], spec_bins[:, :, 1], bin_kern_real, bin_kern_imag
    )
    data_bins = jnp.stack([data_real, data_imag], axis=2).reshape(
        probe_count * sensor_count, 2, block
    )
    rows_time = lax.all_to_all(
        data_bins.astype(jnp.bfloat16), "pts", split_axis=0, concat_axis=2, tiled=True
    ).astype(data_bins.dtype)
    local_rows = rows_time.shape[0]
    begin = lax.axis_index("pts") * local_rows
    local_noise = lax.dynamic_slice_in_dim(noise_rows, begin, local_rows)
    data_rows = rows_time[:, :, :bins_count].reshape(local_rows, 2 * bins_count)
    observed = jnp.dot(data_rows, inverse.T, precision=highest)
    residual = (observed * local_noise[:, None]).astype(jnp.bfloat16)
    weighted_local = (
        jnp.dot(widened(residual), inverse, precision=highest)
        .astype(jnp.bfloat16)
        .reshape(local_rows, 2, bins_count)
    )
    weighted_pad = jnp.pad(weighted_local, ((0, 0), (0, 0), (0, extra)))
    weighted_bins = lax.all_to_all(weighted_pad, "pts", split_axis=2, concat_axis=0, tiled=True)
    weighted_bins = weighted_bins.reshape(probe_count, sensor_count, 2, block)
    adj_real, adj_imag = complex_adjoint(
        weighted_bins[:, :, 0], weighted_bins[:, :, 1], bin_kern_real, bin_kern_imag
    )
    adj_bins = jnp.stack([adj_real, adj_imag], axis=2)
    adj_points = lax.all_to_all(
        adj_bins.astype(jnp.bfloat16), "pts", split_axis=1, concat_axis=3, tiled=True
    ).astype(adj_bins.dtype)
    adjoint = adj_points[..., :bins_count].reshape(probe_count, point_count, 2 * bins_count)
    back = jnp.dot(adjoint, forward.T, precision=highest)
    back = lax.psum(back.astype(jnp.bfloat16), "sen").astype(jnp.float32)
    hessian = back * prior_scale[None, :, None]
    flat = hessian.reshape(probe_count, point_count * steps_count)
    flat_low = flat.astype(jnp.bfloat16)
    coeff = jnp.dot(flat_low, basis, preferred_element_type=jnp.float32)
    coeff = lax.psum(coeff, "pts")
    shrunk = (coeff * deflation[None, :]).astype(jnp.bfloat16)
    correction = lax.dot_general(
        shrunk, basis, (((1,), (1,)), ((), ())), preferred_element_type=jnp.float32
    )
    correction = lax.psum(correction.astype(jnp.bfloat16), "sen").astype(jnp.float32)
    return (flat - correction).reshape(probe_count, point_count, steps_count)


def round_up(value, step):
    return (value + step - 1) // step * step


def packed_tables(steps_count, wide):
    bins_count = steps_count + 1
    turns = np.arange(steps_count)[:, None] * np.arange(bins_count)[None, :] % (2 * steps_count)
    angle = turns.astype(np.float64) * (math.pi / steps_count)
    table = np.zeros((steps_count, 2 * wide), np.float32)
    table[:, :bins_count] = np.cos(angle)
    table[:, wide : wide + bins_count] = -np.sin(angle)
    weights = np.zeros((1, wide), np.float32)
    weights[0, :bins_count] = 2.0 / (2.0 * steps_count)
    weights[0, 0] = weights[0, steps_count] = 1.0 / (2.0 * steps_count)
    return jnp.asarray(table.astype(jnp.bfloat16)), jnp.asarray(weights)


NT = (((1,), (1,)), ((), ()))


def gathered_at(relative, width):
    place = 0
    step = width // 2
    bit = 1
    while step:
        place += (relative // step) % 2 * bit
        step //= 2
        bit *= 2
    return place


def bins_kernel(
    index_ref, b0, b1, b2, b3, own, other, noise, table, weights, out,
    kern, wide_spec, data, wdata, adjoint,
    *, width, points, sens, probes_half, wide,
):
    me = index_ref[0]
    tiles = wide // LANES
    block = points * probes_half
    f32 = jnp.float32
    table_v = table[...]
    rows = 0
    for ref in (b0, b1, b2, b3):
        count = ref.shape[0] * block
        got = jnp.dot(ref[...].reshape(count, ref.shape[2]), table_v, preferred_element_type=f32)
        real = got[:, :wide]
        imag = got[:, wide:]
        wide_spec[0, rows : rows + count] = real + imag
        wide_spec[1, rows : rows + count] = imag
        wide_spec[2, rows : rows + count] = real
        rows += count
    for half, ref in ((0, own), (1, other)):
        def widen(j, carry, half=half, ref=ref):
            for p in range(points):
                real = ref[j, 0, p].astype(f32)
                imag = ref[j, 1, p].astype(f32)
                lo = half * sens
                kern[0, j * points + p, lo : lo + sens] = real
                kern[1, j * points + p, lo : lo + sens] = real + imag
                kern[2, j * points + p, lo : lo + sens] = real - imag
            return carry
        lax.fori_loop(0, width, widen, 0)
    all_sens = 2 * sens
    weight_rows = weights[...]
    for s0 in range(0, all_sens, sens):
        def tile_step(ft, carry, s0=s0):
            lanes = pl.ds(pl.multiple_of(ft * LANES, LANES), LANES)

            def source(j, acc):
                acc = list(acc)
                base = gathered_at(me ^ j, width) * block
                for p in range(points):
                    at = pl.ds(pl.multiple_of(base + p * probes_half, ROWS), probes_half)
                    both = wide_spec[0, at, lanes]
                    imag = wide_spec[1, at, lanes]
                    real = wide_spec[2, at, lanes]
                    for s in range(sens):
                        row = pl.ds(s0 + s, 1)
                        acc[3 * s] += kern[0, j * points + p, row, lanes] * both
                        acc[3 * s + 1] += kern[1, j * points + p, row, lanes] * imag
                        acc[3 * s + 2] += kern[2, j * points + p, row, lanes] * real
                return tuple(acc)

            zero = jnp.zeros((probes_half, LANES), f32)
            acc = lax.fori_loop(0, width, source, (zero,) * (3 * sens))
            factor = weights[:, lanes]
            for s in range(sens):
                at = slice((s0 + s) * probes_half, (s0 + s + 1) * probes_half)
                data[at, lanes] = (acc[3 * s] - acc[3 * s + 1]) * factor
                shifted = pl.ds(pl.multiple_of(wide + ft * LANES, LANES), LANES)
                data[at, shifted] = (acc[3 * s] - acc[3 * s + 2]) * factor
            return carry

        lax.fori_loop(0, tiles, tile_step, 0)
    observed = lax.dot_general(
        data[...].astype(jnp.bfloat16), table_v, NT, preferred_element_type=f32
    )
    residual = (observed * noise[...]).astype(jnp.bfloat16)
    weighted = jnp.dot(residual, table_v, preferred_element_type=f32)
    real = weighted[:, :wide] * weight_rows
    imag = weighted[:, wide:] * weight_rows
    wdata[0] = real + imag
    wdata[1] = imag
    wdata[2] = real

    def adjoint_tile(step, carry):
        j = step // tiles
        ft = step % tiles
        lanes = pl.ds(pl.multiple_of(ft * LANES, LANES), LANES)
        shifted = pl.ds(pl.multiple_of(wide + ft * LANES, LANES), LANES)
        zero = jnp.zeros((probes_half, LANES), f32)
        acc = [zero] * (3 * points)
        for s in range(all_sens):
            at = slice(s * probes_half, (s + 1) * probes_half)
            both = wdata[0, at, lanes]
            imag = wdata[1, at, lanes]
            real = wdata[2, at, lanes]
            for p in range(points):
                row = slice(s, s + 1)
                acc[3 * p] += kern[0, j * points + p, row, lanes] * both
                acc[3 * p + 1] += kern[2, j * points + p, row, lanes] * imag
                acc[3 * p + 2] += kern[1, j * points + p, row, lanes] * real
        for p in range(points):
            at = pl.ds(pl.multiple_of((j * points + p) * probes_half, ROWS), probes_half)
            adjoint[at, lanes] = acc[3 * p] - acc[3 * p + 1]
            adjoint[at, shifted] = acc[3 * p] - acc[3 * p + 2]
        return carry

    lax.fori_loop(0, width * tiles, adjoint_tile, 0)
    back = lax.dot_general(
        adjoint[...].astype(jnp.bfloat16), table_v, NT, preferred_element_type=f32
    )
    out[...] = back.astype(jnp.bfloat16).reshape(out.shape)


def coeff_kernel(parts, prior, basis_own, basis_other, flat, coeff, *, points, steps, probes_half, rank):
    f32 = jnp.float32
    total = parts[0].astype(f32)
    for j in range(1, parts.shape[0]):
        total += parts[j].astype(f32)
    total = total * prior[...]
    for p in range(points):
        flat[:, p * steps : (p + 1) * steps] = total[p * probes_half : (p + 1) * probes_half]
    low = flat[...].astype(jnp.bfloat16)
    own = jnp.dot(low, basis_own[...], preferred_element_type=f32).astype(jnp.bfloat16)
    other = jnp.dot(low, basis_other[...], preferred_element_type=f32).astype(jnp.bfloat16)
    for j in range(coeff.shape[0]):
        coeff[j, :, :rank] = own
        coeff[j, :, rank:] = other


def deflate_kernel(parts, deflation, flat, basis_own, basis_other, out, *, points, steps, rank):
    f32 = jnp.float32
    total = parts[0].astype(f32)
    for j in range(1, parts.shape[0]):
        total += parts[j].astype(f32)
    shrunk = (total * deflation[...]).astype(jnp.bfloat16)
    correction = lax.dot_general(shrunk[:, :rank], basis_own[...], NT, preferred_element_type=f32)
    correction += lax.dot_general(shrunk[:, rank:], basis_other[...], NT, preferred_element_type=f32)
    result = flat[...] - correction
    for p in range(points):
        out[:, p, :] = result[:, p * steps : (p + 1) * steps]


def whole_specs(count):
    return [pl.BlockSpec(memory_space=pltpu.VMEM) for _ in range(count)]


def local_split(probes, kernel, noise_weight, prior_scale, basis, deflation):
    bf16 = jnp.bfloat16
    f32 = jnp.float32
    probe_count, points, steps = probes.shape
    bins_count = steps + 1
    width = lax.axis_size("pts")
    sens = noise_weight.shape[0] // width
    half = probe_count // 2
    rank = basis.shape[1]
    wide = round_up(bins_count, LANES)
    me = lax.axis_index("pts")
    core = lax.axis_index("sen")
    swap = [(0, 1), (1, 0)]
    table, weights = packed_tables(steps, wide)

    send = kernel.reshape(2, points, width, sens, bins_count).transpose(2, 0, 1, 3, 4)
    send = jnp.pad(send, ((0, 0),) * 4 + ((0, wide - bins_count),))
    own = lax.all_to_all(send, "pts", split_axis=0, concat_axis=0, tiled=False)
    other = lax.ppermute(own, "sen", swap)

    mine = lax.dynamic_slice_in_dim(probes, core * half, half, axis=0)
    scaled = (mine.astype(f32) * prior_scale[None, :, None]).astype(bf16)
    b0 = scaled.transpose(1, 0, 2).reshape(1, points * half, steps)
    blocks = [b0]
    step = width // 2
    while step:
        sent = blocks[0] if len(blocks) == 1 else jnp.concatenate(blocks, axis=0)
        blocks.append(lax.ppermute(sent, "pts", [(i, i ^ step) for i in range(width)]))
        step //= 2
    noise_other = lax.ppermute(noise_weight, "sen", swap)
    noise = jnp.concatenate(
        [lax.dynamic_slice_in_dim(v, me * sens, sens) for v in (noise_weight, noise_other)]
    )
    noise_rows = jnp.repeat(noise, half)[:, None]
    basis_other = lax.ppermute(basis, "sen", swap)
    deflation_both = jnp.concatenate([deflation, lax.ppermute(deflation, "sen", swap)])[None, :]
    perm = jnp.full((1,), me, jnp.int32)
    all_rows = width * points * half
    back = pl.pallas_call(
        functools.partial(
            bins_kernel, width=width, points=points, sens=sens, probes_half=half, wide=wide
        ),
        out_shape=jax.ShapeDtypeStruct((width, points * half, steps), bf16),
        in_specs=[pl.BlockSpec(memory_space=pltpu.SMEM)] + whole_specs(9),
        out_specs=pl.BlockSpec(memory_space=pltpu.VMEM),
        scratch_shapes=[
            pltpu.VMEM((3, width * points, 2 * sens, wide), f32),
            pltpu.VMEM((3, all_rows, wide), f32),
            pltpu.VMEM((2 * sens * half, 2 * wide), f32),
            pltpu.VMEM((3, 2 * sens * half, wide), f32),
            pltpu.VMEM((all_rows, 2 * wide), f32),
        ],
        name="bins",
    )(perm, *blocks, own, other, noise_rows, table, weights)
    parts = lax.all_to_all(back, "pts", split_axis=0, concat_axis=0, tiled=False)
    prior_rows = jnp.repeat(prior_scale, half)[:, None]
    flat, coeff = pl.pallas_call(
        functools.partial(
            coeff_kernel, points=points, steps=steps, probes_half=half, rank=rank
        ),
        out_shape=(
            jax.ShapeDtypeStruct((half, points * steps), f32),
            jax.ShapeDtypeStruct((width, half, 2 * rank), bf16),
        ),
        in_specs=whole_specs(4),
        out_specs=tuple(whole_specs(2)),
        name="coeff",
    )(parts, prior_rows, basis, basis_other)
    coeff_parts = lax.all_to_all(coeff, "pts", split_axis=0, concat_axis=0, tiled=False)
    result = pl.pallas_call(
        functools.partial(deflate_kernel, points=points, steps=steps, rank=rank),
        out_shape=jax.ShapeDtypeStruct((half, points, steps), f32),
        in_specs=whole_specs(5),
        out_specs=pl.BlockSpec(memory_space=pltpu.VMEM),
        name="deflate",
    )(coeff_parts, deflation_both, flat, basis, basis_other)
    return lax.all_gather(result, "sen", axis=0, tiled=True)


def solution(mesh):
    placed = (
        P(None, ("grp", "pts"), None),
        P(None, ("grp", "pts"), "sen", None),
        P(("grp", "sen")),
        P("pts"),
        P("pts", "sen"),
        P("sen"),
    )

    def body(*args):
        width = mesh.shape["pts"]
        probe_count = args[0].shape[0]
        sensors = args[2].shape[0]
        power = width & (width - 1) == 0
        split = mesh.shape["sen"] == 2 and power and 1 < width <= 8
        if split and sensors == width * ROWS and probe_count == 2 * ROWS:
            return local_split(*args)
        return local(*args)

    return jax.shard_map(
        body, mesh=mesh, in_specs=placed, out_specs=P(None, ("grp", "pts"), None), check_vma=False
    )
```

```python
import functools
import math

import jax
import jax.numpy as jnp
import numpy as np
from jax import lax
from jax.experimental import pallas as pl
from jax.experimental.pallas import tpu as pltpu
from jax.sharding import PartitionSpec as P

LANES = 128
ROWS = 8


def tables(steps_count):
    bins_count = steps_count + 1
    turns = (
        jnp.arange(steps_count, dtype=jnp.int32)[:, None]
        * jnp.arange(bins_count, dtype=jnp.int32)[None, :]
        % (2 * steps_count)
    )
    angle = turns.astype(jnp.float32) * (math.pi / steps_count)
    cosine = jnp.cos(angle)
    sine = jnp.sin(angle)
    freq = jnp.arange(bins_count, dtype=jnp.int32)
    edge = (freq == 0) | (freq == steps_count)
    weights = jnp.where(edge, 1.0, 2.0).astype(jnp.float32) / (2.0 * steps_count)
    forward = jnp.concatenate([cosine, -sine], axis=1)
    inverse = jnp.concatenate([cosine * weights[None, :], -sine * weights[None, :]], axis=1)
    return (forward, inverse)


def widened(value):
    return lax.optimization_barrier(value).astype(jnp.float32)


def complex_data(spec_real, spec_imag, kern_real, kern_imag):
    data_real = jnp.einsum(
        "kpf,psf->ksf", spec_real, kern_real, preferred_element_type=jnp.float32
    ) - jnp.einsum("kpf,psf->ksf", spec_imag, kern_imag, preferred_element_type=jnp.float32)
    data_imag = jnp.einsum(
        "kpf,psf->ksf", spec_real, kern_imag, preferred_element_type=jnp.float32
    ) + jnp.einsum("kpf,psf->ksf", spec_imag, kern_real, preferred_element_type=jnp.float32)
    return (data_real, data_imag)


def complex_adjoint(weight_real, weight_imag, kern_real, kern_imag):
    adj_real = jnp.einsum(
        "ksf,psf->kpf", weight_real, kern_real, preferred_element_type=jnp.float32
    ) + jnp.einsum("ksf,psf->kpf", weight_imag, kern_imag, preferred_element_type=jnp.float32)
    adj_imag = jnp.einsum(
        "ksf,psf->kpf", weight_imag, kern_real, preferred_element_type=jnp.float32
    ) - jnp.einsum("ksf,psf->kpf", weight_real, kern_imag, preferred_element_type=jnp.float32)
    return (adj_real, adj_imag)


def local(probes, kernel, noise_weight, prior_scale, basis, deflation):
    highest = lax.Precision.HIGHEST
    probe_count, point_count, steps_count = probes.shape
    bins_count = steps_count + 1
    sensor_count = noise_weight.shape[0]
    forward, inverse = tables(steps_count)
    scaled = probes.astype(jnp.float32) * prior_scale[None, :, None]
    spectrum = jnp.dot(scaled, forward, precision=highest).astype(jnp.bfloat16)
    noise_rows = jnp.tile(noise_weight, probe_count)
    width = lax.axis_size("pts")
    block = (bins_count + width - 1) // width
    extra = block * width - bins_count
    kern_pad = jnp.pad(kernel, ((0, 0), (0, 0), (0, 0), (0, extra)))
    spec_pad = jnp.pad(
        spectrum.reshape(probe_count, point_count, 2, bins_count),
        ((0, 0), (0, 0), (0, 0), (0, extra)),
    )
    kern_bins, spec_bins = (
        lax.all_to_all(kern_pad, "pts", split_axis=3, concat_axis=1, tiled=True),
        lax.all_to_all(spec_pad, "pts", split_axis=3, concat_axis=1, tiled=True),
    )
    bin_kern_real = kern_bins[0]
    bin_kern_imag = kern_bins[1]
    data_real, data_imag = complex_data(
        spec_bins[:, :, 0], spec_bins[:, :, 1], bin_kern_real, bin_kern_imag
    )
    data_bins = jnp.stack([data_real, data_imag], axis=2).reshape(
        probe_count * sensor_count, 2, block
    )
    rows_time = lax.all_to_all(
        data_bins.astype(jnp.bfloat16), "pts", split_axis=0, concat_axis=2, tiled=True
    ).astype(data_bins.dtype)
    local_rows = rows_time.shape[0]
    begin = lax.axis_index("pts") * local_rows
    local_noise = lax.dynamic_slice_in_dim(noise_rows, begin, local_rows)
    data_rows = rows_time[:, :, :bins_count].reshape(local_rows, 2 * bins_count)
    observed = jnp.dot(data_rows, inverse.T, precision=highest)
    residual = (observed * local_noise[:, None]).astype(jnp.bfloat16)
    weighted_local = (
        jnp.dot(widened(residual), inverse, precision=highest)
        .astype(jnp.bfloat16)
        .reshape(local_rows, 2, bins_count)
    )
    weighted_pad = jnp.pad(weighted_local, ((0, 0), (0, 0), (0, extra)))
    weighted_bins = lax.all_to_all(weighted_pad, "pts", split_axis=2, concat_axis=0, tiled=True)
    weighted_bins = weighted_bins.reshape(probe_count, sensor_count, 2, block)
    adj_real, adj_imag = complex_adjoint(
        weighted_bins[:, :, 0], weighted_bins[:, :, 1], bin_kern_real, bin_kern_imag
    )
    adj_bins = jnp.stack([adj_real, adj_imag], axis=2)
    adj_points = lax.all_to_all(
        adj_bins.astype(jnp.bfloat16), "pts", split_axis=1, concat_axis=3, tiled=True
    ).astype(adj_bins.dtype)
    adjoint = adj_points[..., :bins_count].reshape(probe_count, point_count, 2 * bins_count)
    back = jnp.dot(adjoint, forward.T, precision=highest)
    back = lax.psum(back.astype(jnp.bfloat16), "sen").astype(jnp.float32)
    hessian = back * prior_scale[None, :, None]
    flat = hessian.reshape(probe_count, point_count * steps_count)
    flat_low = flat.astype(jnp.bfloat16)
    coeff = jnp.dot(flat_low, basis, preferred_element_type=jnp.float32)
    coeff = lax.psum(coeff, "pts")
    shrunk = (coeff * deflation[None, :]).astype(jnp.bfloat16)
    correction = lax.dot_general(
        shrunk, basis, (((1,), (1,)), ((), ())), preferred_element_type=jnp.float32
    )
    correction = lax.psum(correction.astype(jnp.bfloat16), "sen").astype(jnp.float32)
    return (flat - correction).reshape(probe_count, point_count, steps_count)


def round_up(value, step):
    return (value + step - 1) // step * step


def packed_tables(steps_count, wide):
    bins_count = steps_count + 1
    turns = np.arange(steps_count)[:, None] * np.arange(bins_count)[None, :] % (2 * steps_count)
    angle = turns.astype(np.float64) * (math.pi / steps_count)
    table = np.zeros((wide, 2 * wide), np.float32)
    table[:steps_count, :bins_count] = np.cos(angle)
    table[:steps_count, wide : wide + bins_count] = -np.sin(angle)
    weights = np.zeros((1, wide), np.float32)
    weights[0, :bins_count] = 2.0 / (2.0 * steps_count)
    weights[0, 0] = weights[0, steps_count] = 1.0 / (2.0 * steps_count)
    return jnp.asarray(table.astype(jnp.bfloat16)), jnp.asarray(weights)


NT = (((1,), (1,)), ((), ()))


class Packing:
    def __init__(self, rows, length):
        self.full = length // LANES
        self.tail = length % LANES
        self.slots = LANES // self.tail
        self.first_tail = rows * self.full
        self.tiles = self.first_tail + -(-rows // self.slots)

    def place(self, row):
        return self.first_tail + row // self.slots, row % self.slots * self.tail


def turned(tile, lanes):
    lanes = lanes % LANES
    return pltpu.roll(tile, lanes, axis=tile.ndim - 1) if lanes else tile


def store_packed(out_tile, packing, row, value, merged):
    for t in range(packing.full):
        lanes = slice(t * LANES, (t + 1) * LANES)
        out_tile(row * packing.full + t, value[..., lanes].astype(jnp.bfloat16))
    tile, lane = packing.place(row)
    tail = value[..., packing.full * LANES : (packing.full + 1) * LANES]
    where = lax.broadcasted_iota(jnp.int32, tail.shape, tail.ndim - 1)
    tail = turned(jnp.where(where < packing.tail, tail, 0.0), lane)
    merged[tile] = merged[tile] + tail if tile in merged else tail


def store_tails(out_tile, merged):
    for tile, value in merged.items():
        out_tile(tile, value.astype(jnp.bfloat16))


def pack_kernel(
    core, prior_far, kernel, probes, out, prior, kernel_here, probes_here, sems, *, packing
):
    f32 = jnp.float32
    width, _, sens, _ = out.shape
    half, points, _ = probes_here.shape
    edge = packing.full * LANES
    mine = pl.multiple_of(core[0] * half, half)
    copies = [pltpu.make_async_copy(probes.at[pl.ds(mine, half)], probes_here, sems.at[0])]
    for row in range(2 * points):
        at = (row // points, row % points)
        copies.append(
            pltpu.make_async_copy(kernel.at[at], kernel_here.at[at], sems.at[row + 1])
        )
    copies.append(pltpu.make_async_copy(prior_far, prior, sems.at[2 * points + 1]))
    for copy in copies:
        copy.start()

    def out_tile(tile, value):
        out[:, tile] = value

    def padded(value):
        missing = jnp.zeros((value.shape[0], edge + LANES - value.shape[1]), f32)
        return jnp.concatenate([value, missing], axis=1)

    merged = {}
    copies[-1].wait()
    copies[0].wait()
    scaled = probes_here[...].astype(f32)
    for p in range(points):
        value = padded(scaled[:, p, :] * prior[p])
        value = jnp.broadcast_to(value[None], (width, sens, edge + LANES))
        store_packed(out_tile, packing, 2 * points + p, value, merged)
    for row in range(2 * points):
        copies[row + 1].wait()
        value = padded(kernel_here[row // points, row % points].astype(f32))
        store_packed(out_tile, packing, row, value.reshape(width, sens, edge + LANES), merged)
    store_tails(out_tile, merged)


def unpack(source, j, row, packing):
    f32 = jnp.float32
    tiles = [source[j, row * packing.full + t].astype(f32) for t in range(packing.full)]
    tile, lane = packing.place(row)
    tiles.append(turned(source[j, tile].astype(f32), -lane))
    return tiles


def widen(source, kern, *, packing, width, points):
    def step(j, carry):
        for p in range(points):
            real = unpack(source, j, p, packing)
            imag = unpack(source, j, points + p, packing)
            for t, (a, b) in enumerate(zip(real, imag)):
                lanes = slice(t * LANES, (t + 1) * LANES)
                kern[0, j * points + p, :, lanes] = a
                kern[1, j * points + p, :, lanes] = a + b
                kern[2, j * points + p, :, lanes] = a - b
        return carry

    lax.fori_loop(0, width, step, 0)


def forward_sum(kern, spec, weights, data, base, *, width, points, sens, probes_half, wide):
    f32 = jnp.float32

    def tile_step(ft, carry):
        lanes = pl.ds(pl.multiple_of(ft * LANES, LANES), LANES)
        shifted = pl.ds(pl.multiple_of(wide + ft * LANES, LANES), LANES)

        def source(j, acc):
            acc = list(acc)
            for p in range(points):
                q = j * points + p
                at = pl.ds(pl.multiple_of(q * probes_half, ROWS), probes_half)
                both = spec[0, at, lanes]
                imag = spec[1, at, lanes]
                real = spec[2, at, lanes]
                for s in range(sens):
                    row = slice(s, s + 1)
                    acc[3 * s] += kern[0, q, row, lanes] * both
                    acc[3 * s + 1] += kern[1, q, row, lanes] * imag
                    acc[3 * s + 2] += kern[2, q, row, lanes] * real
            return tuple(acc)

        zero = jnp.zeros((probes_half, LANES), f32)
        acc = lax.fori_loop(0, width, source, (zero,) * (3 * sens))
        factor = weights[:, lanes]
        for s in range(sens):
            at = slice(base + s * probes_half, base + (s + 1) * probes_half)
            data[at, lanes] = (acc[3 * s] - acc[3 * s + 1]) * factor
            data[at, shifted] = (acc[3 * s] - acc[3 * s + 2]) * factor
        return carry

    lax.fori_loop(0, wide // LANES, tile_step, 0)


def own_kernel(own, table, weights, spec, kern, data, rows, *, sizes, packing):
    width, points, half = sizes["width"], sizes["points"], sizes["probes_half"]
    wide = sizes["wide"]
    for j in range(width):
        for p in range(points):
            at = slice((j * points + p) * half, (j * points + p + 1) * half)
            for t, tile in enumerate(unpack(own, j, 2 * points + p, packing)):
                rows[at, t * LANES : (t + 1) * LANES] = tile
    got = jnp.dot(rows[...].astype(jnp.bfloat16), table[...], preferred_element_type=jnp.float32)
    real = got[:, :wide]
    imag = got[:, wide:]
    spec[0] = real + imag
    spec[1] = imag
    spec[2] = real
    widen(own, kern, packing=packing, width=width, points=points)
    forward_sum(kern, spec, weights, data, 0, **sizes)


def bins_kernel(
    index, noise_own, noise_other, other, spec, kern_own, data_own, table, weights, out,
    kern, data, wdata, adjoint,
    *, sizes, packing, packing_back,
):
    width, points, sens = sizes["width"], sizes["points"], sizes["sens"]
    probes_half, wide = sizes["probes_half"], sizes["wide"]
    tiles = wide // LANES
    f32 = jnp.float32
    half_rows = sens * probes_half
    widen(other, kern, packing=packing, width=width, points=points)
    forward_sum(kern, spec, weights, data, half_rows, **sizes)
    data[:half_rows] = data_own[...]
    table_v = table[...]
    observed = lax.dot_general(
        data[...].astype(jnp.bfloat16), table_v, NT, preferred_element_type=f32
    )
    first = index[0] * sens
    scales = [noise_own[first + s] for s in range(sens)]
    scales += [noise_other[first + s] for s in range(sens)]
    residual = jnp.concatenate(
        [
            (observed[s * probes_half : (s + 1) * probes_half] * scale)
            for s, scale in enumerate(scales)
        ],
        axis=0,
    ).astype(jnp.bfloat16)
    weighted = jnp.dot(residual, table_v, preferred_element_type=f32)
    weight_rows = weights[...]
    real = weighted[:, :wide] * weight_rows
    imag = weighted[:, wide:] * weight_rows
    wdata[0] = real + imag
    wdata[1] = imag
    wdata[2] = real

    def adjoint_tile(step, carry):
        j = step // tiles
        ft = step % tiles
        lanes = pl.ds(pl.multiple_of(ft * LANES, LANES), LANES)
        shifted = pl.ds(pl.multiple_of(wide + ft * LANES, LANES), LANES)
        zero = jnp.zeros((probes_half, LANES), f32)
        acc = [zero] * (3 * points)
        for half, source in ((0, kern_own), (1, kern)):
            for s in range(sens):
                at = slice(half * half_rows + s * probes_half, half * half_rows + (s + 1) * probes_half)
                both = wdata[0, at, lanes]
                imag = wdata[1, at, lanes]
                real = wdata[2, at, lanes]
                row = slice(s, s + 1)
                for p in range(points):
                    q = j * points + p
                    acc[3 * p] += source[0, q, row, lanes] * both
                    acc[3 * p + 1] += source[2, q, row, lanes] * imag
                    acc[3 * p + 2] += source[1, q, row, lanes] * real
        for p in range(points):
            at = pl.ds(pl.multiple_of((j * points + p) * probes_half, ROWS), probes_half)
            adjoint[at, lanes] = acc[3 * p] - acc[3 * p + 1]
            adjoint[at, shifted] = acc[3 * p] - acc[3 * p + 2]
        return carry

    lax.fori_loop(0, width * tiles, adjoint_tile, 0)
    back = lax.dot_general(
        adjoint[...].astype(jnp.bfloat16), table_v, NT, preferred_element_type=f32
    )
    back = back.reshape(width, points, probes_half, wide)

    def out_tile(tile, value):
        out[:, tile] = value

    merged = {}
    for p in range(points):
        store_packed(out_tile, packing_back, p, back[:, p], merged)
    store_tails(out_tile, merged)


def summed(parts):
    total = parts[0].astype(jnp.float32)
    for j in range(1, parts.shape[0]):
        total += parts[j].astype(jnp.float32)
    return total


def coeff_kernel(prior, parts, basis_own, basis_other, flat, coeff, *, points, steps, rank, packing):
    f32 = jnp.float32
    total = summed(parts)
    for p in range(points):
        tiles = [total[p * packing.full + t] for t in range(packing.full)]
        tile, lane = packing.place(p)
        tiles.append(turned(total[tile], -lane))
        piece = jnp.concatenate(tiles, axis=1) * prior[p]
        flat[:, p * steps : (p + 1) * steps] = piece[:, :steps]
    low = flat[...].astype(jnp.bfloat16)
    own = jnp.dot(low, basis_own[...], preferred_element_type=f32).astype(jnp.bfloat16)
    other = jnp.dot(low, basis_other[...], preferred_element_type=f32).astype(jnp.bfloat16)
    for j in range(coeff.shape[0]):
        coeff[j, :, :rank] = own
        coeff[j, :, rank:] = other


def deflate_kernel(
    core, parts_own, parts_other, deflation_own, deflation_other, flat_own, flat_other,
    basis_own, basis_other, out,
    *, points, steps, rank,
):
    f32 = jnp.float32
    bf16 = jnp.bfloat16
    own = summed(parts_own)
    other = summed(parts_other)
    half = own.shape[0]
    here = jnp.concatenate([own[:, :rank], other[:, rank:]], axis=0) * deflation_own[...]
    there = jnp.concatenate([own[:, rank:], other[:, :rank]], axis=0) * deflation_other[...]
    correction = lax.dot_general(here.astype(bf16), basis_own[...], NT, preferred_element_type=f32)
    correction += lax.dot_general(there.astype(bf16), basis_other[...], NT, preferred_element_type=f32)
    result = jnp.concatenate([flat_own[...], flat_other[...]], axis=0) - correction
    mine = core[0] * half
    for p in range(points):
        piece = result[:, p * steps : (p + 1) * steps]
        out[pl.ds(mine, half), p, :] = piece[:half]
        out[pl.ds(half - mine, half), p, :] = piece[half:]


def kept(space, *values):
    return [pltpu.with_memory_space_constraint(value, space) for value in values]


def in_vmem(count):
    return [pl.BlockSpec(memory_space=pltpu.VMEM) for _ in range(count)]


def in_smem(count):
    return [pl.BlockSpec(memory_space=pltpu.SMEM) for _ in range(count)]


def limit(mib):
    return pltpu.CompilerParams(vmem_limit_bytes=mib * 1024 * 1024)


def local_split(probes, kernel, noise_weight, prior_scale, basis, deflation):
    bf16 = jnp.bfloat16
    f32 = jnp.float32
    probe_count, points, steps = probes.shape
    bins_count = steps + 1
    width = lax.axis_size("pts")
    sens = noise_weight.shape[0] // width
    half = probe_count // 2
    rank = basis.shape[1]
    wide = round_up(bins_count, LANES)
    me = jnp.full((1,), lax.axis_index("pts"), jnp.int32)
    core_index = lax.axis_index("sen")
    core = jnp.full((1,), core_index, jnp.int32)

    def swap(value):
        return lax.ppermute(value, "sen", [(0, 1), (1, 0)])

    def exchange(value):
        return lax.all_to_all(value, "pts", split_axis=0, concat_axis=0, tiled=False)

    table, weights = packed_tables(steps, wide)
    sizes = dict(width=width, points=points, sens=sens, probes_half=half, wide=wide)
    all_rows = width * points * half

    packing = Packing(3 * points, bins_count)
    packing_back = Packing(points, steps)
    in_hbm = pl.BlockSpec(memory_space=pltpu.HBM)
    send = pl.pallas_call(
        functools.partial(pack_kernel, packing=packing),
        out_shape=pltpu.VMEM((width, packing.tiles, sens, LANES), bf16),
        in_specs=in_smem(1) + [in_hbm] * 3,
        out_specs=in_vmem(1)[0],
        scratch_shapes=[
            pltpu.SMEM(prior_scale.shape, f32),
            pltpu.VMEM(kernel.shape, bf16),
            pltpu.VMEM((half, points, steps), bf16),
            pltpu.SemaphoreType.DMA((2 * points + 2,)),
        ],
        compiler_params=limit(8),
        name="pack",
    )(core, *kept(pltpu.HBM, prior_scale, kernel, probes))
    own = exchange(send)
    noise_other = swap(noise_weight)
    deflation_other = swap(deflation)
    basis_other = swap(basis)
    basis, basis_other = kept(pltpu.VMEM, basis, basis_other)
    other = swap(own)
    other, basis_other, noise_other, deflation_other = lax.optimization_barrier(
        (other, basis_other, noise_other, deflation_other)
    )
    spec, kern_own, data_own = pl.pallas_call(
        functools.partial(own_kernel, sizes=sizes, packing=packing),
        out_shape=(
            jax.ShapeDtypeStruct((3, all_rows, wide), f32),
            jax.ShapeDtypeStruct((3, width * points, sens, wide), f32),
            jax.ShapeDtypeStruct((sens * half, 2 * wide), f32),
        ),
        in_specs=in_vmem(3),
        out_specs=tuple(in_vmem(3)),
        scratch_shapes=[pltpu.VMEM((all_rows, wide), f32)],
        compiler_params=limit(10),
        name="own",
    )(own, table, weights)
    back = pl.pallas_call(
        functools.partial(bins_kernel, sizes=sizes, packing=packing, packing_back=packing_back),
        out_shape=pltpu.VMEM((width, packing_back.tiles, half, LANES), bf16),
        in_specs=in_smem(3) + in_vmem(6),
        out_specs=in_vmem(1)[0],
        scratch_shapes=[
            pltpu.VMEM((3, width * points, sens, wide), f32),
            pltpu.VMEM((2 * sens * half, 2 * wide), f32),
            pltpu.VMEM((3, 2 * sens * half, wide), f32),
            pltpu.VMEM((all_rows, 2 * wide), f32),
        ],
        compiler_params=limit(20),
        name="bins",
    )(me, noise_weight, noise_other, other, spec, kern_own, data_own, table, weights)
    parts = exchange(back)
    flat, coeff = pl.pallas_call(
        functools.partial(coeff_kernel, points=points, steps=steps, rank=rank, packing=packing_back),
        out_shape=(
            jax.ShapeDtypeStruct((half, points * steps), f32),
            jax.ShapeDtypeStruct((width, half, 2 * rank), bf16),
        ),
        in_specs=in_smem(1) + in_vmem(3),
        out_specs=tuple(in_vmem(2)),
        compiler_params=limit(12),
        name="coeff",
    )(prior_scale, parts, basis, basis_other)
    flat_other = swap(flat)
    coeff_parts = exchange(coeff)
    coeff_other = swap(coeff_parts)
    return pl.pallas_call(
        functools.partial(deflate_kernel, points=points, steps=steps, rank=rank),
        out_shape=jax.ShapeDtypeStruct((probe_count, points, steps), f32),
        in_specs=in_smem(1) + in_vmem(8),
        out_specs=in_vmem(1)[0],
        compiler_params=limit(12),
        name="deflate",
    )(
        core, coeff_parts, coeff_other, deflation[None, :], deflation_other[None, :],
        flat, flat_other, basis, basis_other,
    )


def solution(mesh):
    placed = (
        P(None, ("grp", "pts"), None),
        P(None, ("grp", "pts"), "sen", None),
        P(("grp", "sen")),
        P("pts"),
        P("pts", "sen"),
        P("sen"),
    )

    def body(*args):
        width = mesh.shape["pts"]
        split = mesh.shape["sen"] == 2 and width > 1
        whole_tiles = args[2].shape[0] == width * ROWS and args[0].shape[0] == 2 * ROWS
        if not (split and whole_tiles):
            return local(*args)
        return local_split(*args)

    return jax.shard_map(
        body, mesh=mesh, in_specs=placed, out_specs=P(None, ("grp", "pts"), None), check_vma=False
    )
```

```python
import functools
import math

import jax
import jax.numpy as jnp
import numpy as np
from jax import lax
from jax.experimental import pallas as pl
from jax.experimental.pallas import tpu as pltpu
from jax.sharding import PartitionSpec as P

LANES = 128
ROWS = 8


def tables(steps_count):
    bins_count = steps_count + 1
    turns = (
        jnp.arange(steps_count, dtype=jnp.int32)[:, None]
        * jnp.arange(bins_count, dtype=jnp.int32)[None, :]
        % (2 * steps_count)
    )
    angle = turns.astype(jnp.float32) * (math.pi / steps_count)
    cosine = jnp.cos(angle)
    sine = jnp.sin(angle)
    freq = jnp.arange(bins_count, dtype=jnp.int32)
    edge = (freq == 0) | (freq == steps_count)
    weights = jnp.where(edge, 1.0, 2.0).astype(jnp.float32) / (2.0 * steps_count)
    forward = jnp.concatenate([cosine, -sine], axis=1)
    inverse = jnp.concatenate([cosine * weights[None, :], -sine * weights[None, :]], axis=1)
    return (forward, inverse)


def widened(value):
    return lax.optimization_barrier(value).astype(jnp.float32)


def complex_data(spec_real, spec_imag, kern_real, kern_imag):
    data_real = jnp.einsum(
        "kpf,psf->ksf", spec_real, kern_real, preferred_element_type=jnp.float32
    ) - jnp.einsum("kpf,psf->ksf", spec_imag, kern_imag, preferred_element_type=jnp.float32)
    data_imag = jnp.einsum(
        "kpf,psf->ksf", spec_real, kern_imag, preferred_element_type=jnp.float32
    ) + jnp.einsum("kpf,psf->ksf", spec_imag, kern_real, preferred_element_type=jnp.float32)
    return (data_real, data_imag)


def complex_adjoint(weight_real, weight_imag, kern_real, kern_imag):
    adj_real = jnp.einsum(
        "ksf,psf->kpf", weight_real, kern_real, preferred_element_type=jnp.float32
    ) + jnp.einsum("ksf,psf->kpf", weight_imag, kern_imag, preferred_element_type=jnp.float32)
    adj_imag = jnp.einsum(
        "ksf,psf->kpf", weight_imag, kern_real, preferred_element_type=jnp.float32
    ) - jnp.einsum("ksf,psf->kpf", weight_real, kern_imag, preferred_element_type=jnp.float32)
    return (adj_real, adj_imag)


def local(probes, kernel, noise_weight, prior_scale, basis, deflation):
    highest = lax.Precision.HIGHEST
    probe_count, point_count, steps_count = probes.shape
    bins_count = steps_count + 1
    sensor_count = noise_weight.shape[0]
    forward, inverse = tables(steps_count)
    scaled = probes.astype(jnp.float32) * prior_scale[None, :, None]
    spectrum = jnp.dot(scaled, forward, precision=highest).astype(jnp.bfloat16)
    noise_rows = jnp.tile(noise_weight, probe_count)
    width = lax.axis_size("pts")
    block = (bins_count + width - 1) // width
    extra = block * width - bins_count
    kern_pad = jnp.pad(kernel, ((0, 0), (0, 0), (0, 0), (0, extra)))
    spec_pad = jnp.pad(
        spectrum.reshape(probe_count, point_count, 2, bins_count),
        ((0, 0), (0, 0), (0, 0), (0, extra)),
    )
    kern_bins, spec_bins = (
        lax.all_to_all(kern_pad, "pts", split_axis=3, concat_axis=1, tiled=True),
        lax.all_to_all(spec_pad, "pts", split_axis=3, concat_axis=1, tiled=True),
    )
    bin_kern_real = kern_bins[0]
    bin_kern_imag = kern_bins[1]
    data_real, data_imag = complex_data(
        spec_bins[:, :, 0], spec_bins[:, :, 1], bin_kern_real, bin_kern_imag
    )
    data_bins = jnp.stack([data_real, data_imag], axis=2).reshape(
        probe_count * sensor_count, 2, block
    )
    rows_time = lax.all_to_all(
        data_bins.astype(jnp.bfloat16), "pts", split_axis=0, concat_axis=2, tiled=True
    ).astype(data_bins.dtype)
    local_rows = rows_time.shape[0]
    begin = lax.axis_index("pts") * local_rows
    local_noise = lax.dynamic_slice_in_dim(noise_rows, begin, local_rows)
    data_rows = rows_time[:, :, :bins_count].reshape(local_rows, 2 * bins_count)
    observed = jnp.dot(data_rows, inverse.T, precision=highest)
    residual = (observed * local_noise[:, None]).astype(jnp.bfloat16)
    weighted_local = (
        jnp.dot(widened(residual), inverse, precision=highest)
        .astype(jnp.bfloat16)
        .reshape(local_rows, 2, bins_count)
    )
    weighted_pad = jnp.pad(weighted_local, ((0, 0), (0, 0), (0, extra)))
    weighted_bins = lax.all_to_all(weighted_pad, "pts", split_axis=2, concat_axis=0, tiled=True)
    weighted_bins = weighted_bins.reshape(probe_count, sensor_count, 2, block)
    adj_real, adj_imag = complex_adjoint(
        weighted_bins[:, :, 0], weighted_bins[:, :, 1], bin_kern_real, bin_kern_imag
    )
    adj_bins = jnp.stack([adj_real, adj_imag], axis=2)
    adj_points = lax.all_to_all(
        adj_bins.astype(jnp.bfloat16), "pts", split_axis=1, concat_axis=3, tiled=True
    ).astype(adj_bins.dtype)
    adjoint = adj_points[..., :bins_count].reshape(probe_count, point_count, 2 * bins_count)
    back = jnp.dot(adjoint, forward.T, precision=highest)
    back = lax.psum(back.astype(jnp.bfloat16), "sen").astype(jnp.float32)
    hessian = back * prior_scale[None, :, None]
    flat = hessian.reshape(probe_count, point_count * steps_count)
    flat_low = flat.astype(jnp.bfloat16)
    coeff = jnp.dot(flat_low, basis, preferred_element_type=jnp.float32)
    coeff = lax.psum(coeff, "pts")
    shrunk = (coeff * deflation[None, :]).astype(jnp.bfloat16)
    correction = lax.dot_general(
        shrunk, basis, (((1,), (1,)), ((), ())), preferred_element_type=jnp.float32
    )
    correction = lax.psum(correction.astype(jnp.bfloat16), "sen").astype(jnp.float32)
    return (flat - correction).reshape(probe_count, point_count, steps_count)


def round_up(value, step):
    return (value + step - 1) // step * step


def packed_tables(steps_count, wide):
    bins_count = steps_count + 1
    turns = np.arange(steps_count)[:, None] * np.arange(bins_count)[None, :] % (2 * steps_count)
    angle = turns.astype(np.float64) * (math.pi / steps_count)
    table = np.zeros((wide, 2 * wide), np.float32)
    table[:steps_count, :bins_count] = np.cos(angle)
    table[:steps_count, wide : wide + bins_count] = -np.sin(angle)
    weights = np.zeros((1, wide), np.float32)
    weights[0, :bins_count] = 2.0 / (2.0 * steps_count)
    weights[0, 0] = weights[0, steps_count] = 1.0 / (2.0 * steps_count)
    return jnp.asarray(table.astype(jnp.bfloat16)), jnp.asarray(weights)


NT = (((1,), (1,)), ((), ()))


class Packing:
    def __init__(self, rows, length):
        self.full = length // LANES
        self.tail = length % LANES
        self.slots = LANES // self.tail
        self.first_tail = rows * self.full
        self.tiles = self.first_tail + -(-rows // self.slots)

    def place(self, row):
        return self.first_tail + row // self.slots, row % self.slots * self.tail


def turned(tile, lanes):
    lanes = lanes % LANES
    return pltpu.roll(tile, lanes, axis=tile.ndim - 1) if lanes else tile


def store_packed(out_tile, packing, row, value, merged):
    for t in range(packing.full):
        lanes = slice(t * LANES, (t + 1) * LANES)
        out_tile(row * packing.full + t, value[..., lanes].astype(jnp.bfloat16))
    tile, lane = packing.place(row)
    tail = value[..., packing.full * LANES : (packing.full + 1) * LANES]
    where = lax.broadcasted_iota(jnp.int32, tail.shape, tail.ndim - 1)
    tail = turned(jnp.where(where < packing.tail, tail, 0.0), lane)
    merged[tile] = merged[tile] + tail if tile in merged else tail


def store_tails(out_tile, merged):
    for tile, value in merged.items():
        out_tile(tile, value.astype(jnp.bfloat16))


def pack_kernel(index, prior_far, kernel, probes, *refs, order, sens, half, packing):
    outs = refs[: len(order)]
    prior, kernel_here, probes_here, sems = refs[len(order) :]
    f32 = jnp.float32
    _, points, _ = probes_here.shape
    edge = packing.full * LANES
    me = index[0]
    mine = pl.multiple_of(index[1] * half, half)
    copies = [
        pltpu.make_async_copy(probes.at[pl.ds(mine, half)], probes_here, sems.at[0]),
        pltpu.make_async_copy(prior_far, prior, sems.at[1]),
    ]
    for slot, relative in enumerate(order):
        rows = pl.ds(pl.multiple_of((me ^ relative) * sens, sens), sens)
        copies.append(
            pltpu.make_async_copy(
                kernel.at[:, :, rows, :], kernel_here.at[slot], sems.at[2 + slot]
            )
        )
    for copy in copies:
        copy.start()

    def padded(value):
        missing = jnp.zeros((value.shape[0], edge + LANES - value.shape[1]), f32)
        return jnp.concatenate([value, missing], axis=1)

    copies[0].wait()
    copies[1].wait()
    scaled = probes_here[...].astype(f32)
    scaled = [padded(scaled[:, p, :] * prior[p]) for p in range(points)]
    for slot, out in enumerate(outs):
        copies[2 + slot].wait()

        def out_tile(tile, value, out=out):
            out[tile] = value

        merged = {}
        for row in range(2 * points):
            value = padded(kernel_here[slot, row // points, row % points].astype(f32))
            store_packed(out_tile, packing, row, value, merged)
        for p in range(points):
            store_packed(out_tile, packing, 2 * points + p, scaled[p], merged)
        store_tails(out_tile, merged)


def unpack(source, row, packing):
    f32 = jnp.float32
    tiles = [source[row * packing.full + t].astype(f32) for t in range(packing.full)]
    tile, lane = packing.place(row)
    tiles.append(turned(source[tile].astype(f32), -lane))
    return tiles


def widen(sources, kern, *, packing, points, sens):
    for b, pair in enumerate(sources):
        for half, source in enumerate(pair):
            at = slice(half * sens, (half + 1) * sens)
            for p in range(points):
                real = unpack(source, p, packing)
                imag = unpack(source, points + p, packing)
                for t, (x, y) in enumerate(zip(real, imag)):
                    lanes = slice(t * LANES, (t + 1) * LANES)
                    kern[0, b * points + p, at, lanes] = x
                    kern[1, b * points + p, at, lanes] = x + y
                    kern[2, b * points + p, at, lanes] = x - y


def spectra(sources, table, spec, rows, *, packing, points, half, wide):
    for b, (own, _) in enumerate(sources):
        for p in range(points):
            at = slice((b * points + p) * half, (b * points + p + 1) * half)
            for t, tile in enumerate(unpack(own, 2 * points + p, packing)):
                rows[at, t * LANES : (t + 1) * LANES] = tile
    got = jnp.dot(rows[...].astype(jnp.bfloat16), table[...], preferred_element_type=jnp.float32)
    real = got[:, :wide]
    imag = got[:, wide:]
    spec[0] = real + imag
    spec[1] = imag
    spec[2] = real


def forward_sum(kern, spec, data, earlier, *, points, sens, half, wide):
    f32 = jnp.float32
    blocks = kern.shape[1] // points

    def tile_step(ft, carry):
        lanes = pl.ds(pl.multiple_of(ft * LANES, LANES), LANES)
        shifted = pl.ds(pl.multiple_of(wide + ft * LANES, LANES), LANES)
        for first in range(0, 2 * sens, sens):

            def source(b, acc, first=first):
                acc = list(acc)
                for p in range(points):
                    q = b * points + p
                    at = pl.ds(pl.multiple_of(q * half, ROWS), half)
                    both = spec[0, at, lanes]
                    imag = spec[1, at, lanes]
                    real = spec[2, at, lanes]
                    for s in range(sens):
                        row = slice(first + s, first + s + 1)
                        acc[3 * s] += kern[0, q, row, lanes] * both
                        acc[3 * s + 1] += kern[1, q, row, lanes] * imag
                        acc[3 * s + 2] += kern[2, q, row, lanes] * real
                return tuple(acc)

            zero = jnp.zeros((half, LANES), f32)
            acc = lax.fori_loop(0, blocks, source, (zero,) * (3 * sens))
            for s in range(sens):
                at = slice((first + s) * half, (first + s + 1) * half)
                real = acc[3 * s] - acc[3 * s + 1]
                imag = acc[3 * s] - acc[3 * s + 2]
                if earlier is not None:
                    real += earlier[at, lanes]
                    imag += earlier[at, shifted]
                data[at, lanes] = real
                data[at, shifted] = imag
        return carry

    lax.fori_loop(0, wide // LANES, tile_step, 0)


def paired(refs, count):
    return list(zip(refs[:count], refs[count : 2 * count]))


def first_kernel(table, *refs, count, points, sens, half, wide, packing):
    sources = paired(refs, count)
    kern, data, spec, rows = refs[2 * count :]
    spectra(sources, table, spec, rows, packing=packing, points=points, half=half, wide=wide)
    widen(sources, kern, packing=packing, points=points, sens=sens)
    forward_sum(kern, spec, data, None, points=points, sens=sens, half=half, wide=wide)


def bins_kernel(
    index, noise_own, noise_other, table, weights, kern_first, data_first, *refs,
    orders, points, sens, half, wide, packing, packing_back,
):
    count = len(orders[1])
    sources = paired(refs, count)
    out, kern, spec, rows, data, wdata, adjoint = refs[2 * count :]
    tiles = wide // LANES
    f32 = jnp.float32
    bf16 = jnp.bfloat16
    spectra(sources, table, spec, rows, packing=packing, points=points, half=half, wide=wide)
    widen(sources, kern, packing=packing, points=points, sens=sens)
    forward_sum(kern, spec, data, data_first, points=points, sens=sens, half=half, wide=wide)
    table_v = table[...]
    weight_rows = weights[...]
    scaled = jnp.concatenate(
        [data[:, :wide] * weight_rows, data[:, wide:] * weight_rows], axis=1
    ).astype(bf16)
    observed = lax.dot_general(scaled, table_v, NT, preferred_element_type=f32)
    mine = index[0] * sens
    scales = [noise_own[mine + s] for s in range(sens)]
    scales += [noise_other[mine + s] for s in range(sens)]
    residual = jnp.concatenate(
        [observed[s * half : (s + 1) * half] * scale for s, scale in enumerate(scales)], axis=0
    ).astype(bf16)
    weighted = jnp.dot(residual, table_v, preferred_element_type=f32)
    real = weighted[:, :wide] * weight_rows
    imag = weighted[:, wide:] * weight_rows
    wdata[0] = real + imag
    wdata[1] = imag
    wdata[2] = real

    base = 0
    for source, order in ((kern_first, orders[0]), (kern, orders[1])):

        def adjoint_tile(step, carry, source=source, base=base):
            b = step // tiles
            ft = step % tiles
            lanes = pl.ds(pl.multiple_of(ft * LANES, LANES), LANES)
            shifted = pl.ds(pl.multiple_of(wide + ft * LANES, LANES), LANES)
            zero = jnp.zeros((half, LANES), f32)
            acc = [zero] * (3 * points)
            for s in range(2 * sens):
                at = slice(s * half, (s + 1) * half)
                both = wdata[0, at, lanes]
                imag = wdata[1, at, lanes]
                real = wdata[2, at, lanes]
                row = slice(s, s + 1)
                for p in range(points):
                    q = b * points + p
                    acc[3 * p] += source[0, q, row, lanes] * both
                    acc[3 * p + 1] += source[2, q, row, lanes] * imag
                    acc[3 * p + 2] += source[1, q, row, lanes] * real
            for p in range(points):
                at = pl.ds(pl.multiple_of((base + b * points + p) * half, ROWS), half)
                adjoint[at, lanes] = acc[3 * p] - acc[3 * p + 1]
                adjoint[at, shifted] = acc[3 * p] - acc[3 * p + 2]
            return carry

        lax.fori_loop(0, len(order) * tiles, adjoint_tile, 0)
        base += len(order) * points
    back = lax.dot_general(adjoint[...].astype(bf16), table_v, NT, preferred_element_type=f32)
    for b, relative in enumerate(orders[0] + orders[1]):
        there = index[0] ^ relative

        def out_tile(tile, value, there=there):
            out[there, tile] = value

        merged = {}
        for p in range(points):
            at = slice((b * points + p) * half, (b * points + p + 1) * half)
            store_packed(out_tile, packing_back, p, back[at], merged)
        store_tails(out_tile, merged)


def summed(parts):
    total = parts[0].astype(jnp.float32)
    for j in range(1, parts.shape[0]):
        total += parts[j].astype(jnp.float32)
    return total


def coeff_kernel(prior, parts, basis_own, basis_other, flat, coeff, *, points, steps, rank, packing):
    f32 = jnp.float32
    total = summed(parts)
    for p in range(points):
        tiles = [total[p * packing.full + t] for t in range(packing.full)]
        tile, lane = packing.place(p)
        tiles.append(turned(total[tile], -lane))
        piece = jnp.concatenate(tiles, axis=1) * prior[p]
        flat[:, p * steps : (p + 1) * steps] = piece[:, :steps]
    low = flat[...].astype(jnp.bfloat16)
    own = jnp.dot(low, basis_own[...], preferred_element_type=f32).astype(jnp.bfloat16)
    other = jnp.dot(low, basis_other[...], preferred_element_type=f32).astype(jnp.bfloat16)
    for j in range(coeff.shape[0]):
        coeff[j, :, :rank] = own
        coeff[j, :, rank:] = other


def deflate_kernel(
    core, parts_own, parts_other, deflation_own, deflation_other, flat_own, flat_other,
    basis_own, basis_other, out,
    *, points, steps, rank,
):
    f32 = jnp.float32
    bf16 = jnp.bfloat16
    own = summed(parts_own)
    other = summed(parts_other)
    half = own.shape[0]
    here = jnp.concatenate([own[:, :rank], other[:, rank:]], axis=0) * deflation_own[...]
    there = jnp.concatenate([own[:, rank:], other[:, :rank]], axis=0) * deflation_other[...]
    correction = lax.dot_general(here.astype(bf16), basis_own[...], NT, preferred_element_type=f32)
    correction += lax.dot_general(there.astype(bf16), basis_other[...], NT, preferred_element_type=f32)
    result = jnp.concatenate([flat_own[...], flat_other[...]], axis=0) - correction
    mine = core[0] * half
    for p in range(points):
        piece = result[:, p * steps : (p + 1) * steps]
        out[pl.ds(mine, half), p, :] = piece[:half]
        out[pl.ds(half - mine, half), p, :] = piece[half:]


def split_order(width):
    far = list(range(width // 2, width))
    near = list(range(width // 4, width // 2)) + list(range(1, width // 4))
    return [0] + far, near


def stage_kernel(far, near, sem):
    copy = pltpu.make_async_copy(far, near, sem)
    copy.start()
    copy.wait()


def kept(space, *values):
    return [pltpu.with_memory_space_constraint(value, space) for value in values]


def in_vmem(count):
    return [pl.BlockSpec(memory_space=pltpu.VMEM) for _ in range(count)]


def in_smem(count):
    return [pl.BlockSpec(memory_space=pltpu.SMEM) for _ in range(count)]


def limit(mib):
    return pltpu.CompilerParams(vmem_limit_bytes=mib * 1024 * 1024)


def local_split(probes, kernel, noise_weight, prior_scale, basis, deflation):
    bf16 = jnp.bfloat16
    f32 = jnp.float32
    probe_count, points, steps = probes.shape
    bins_count = steps + 1
    width = lax.axis_size("pts")
    sens = noise_weight.shape[0] // width
    half = probe_count // 2
    rank = basis.shape[1]
    wide = round_up(bins_count, LANES)
    me = jnp.full((1,), lax.axis_index("pts"), jnp.int32)
    core_index = lax.axis_index("sen")
    core = jnp.full((1,), core_index, jnp.int32)

    def swap(value):
        return lax.ppermute(value, "sen", [(0, 1), (1, 0)])

    def exchange(value):
        return lax.all_to_all(value, "pts", split_axis=0, concat_axis=0, tiled=False)

    table, weights = packed_tables(steps, wide)
    packing = Packing(3 * points, bins_count)
    packing_back = Packing(points, steps)
    sizes = dict(points=points, sens=sens, half=half, wide=wide, packing=packing)
    orders = split_order(width)
    order = orders[0] + orders[1]
    places = jnp.stack([me[0], core[0]])
    chunk = jax.ShapeDtypeStruct((packing.tiles, sens, LANES), bf16)
    in_hbm = pl.BlockSpec(memory_space=pltpu.HBM)
    sent = pl.pallas_call(
        functools.partial(pack_kernel, order=order, sens=sens, half=half, packing=packing),
        out_shape=(chunk,) * width,
        in_specs=in_smem(1) + [in_hbm] * 3,
        out_specs=tuple(in_vmem(width)),
        scratch_shapes=[
            pltpu.SMEM(prior_scale.shape, f32),
            pltpu.VMEM((width, 2, points, sens, bins_count), bf16),
            pltpu.VMEM((half, points, steps), bf16),
            pltpu.SemaphoreType.DMA((2 + width,)),
        ],
        compiler_params=limit(8),
        name="pack",
    )(places, *kept(pltpu.HBM, prior_scale, kernel, probes))
    blocks = {}
    others = {}
    for relative, value in zip(order, sent):
        if relative:
            value = lax.ppermute(value, "pts", [(i, i ^ relative) for i in range(width)])
        blocks[relative] = value
        others[relative] = swap(value)
    noise_other = swap(noise_weight)
    deflation_other = swap(deflation)
    basis_other = swap(basis)

    def scratch(count):
        return [
            pltpu.VMEM((3, count * points * half, wide), f32),
            pltpu.VMEM((count * points * half, wide), f32),
        ]

    def ready(part):
        return [blocks[r] for r in part] + [others[r] for r in part]

    table = pl.pallas_call(
        stage_kernel,
        out_shape=pltpu.VMEM(table.shape, bf16),
        in_specs=[in_hbm],
        out_specs=in_vmem(1)[0],
        scratch_shapes=[pltpu.SemaphoreType.DMA],
        compiler_params=limit(2),
        name="stage",
    )(*kept(pltpu.HBM, table))
    count = len(orders[0])
    kern_first, data_first = pl.pallas_call(
        functools.partial(first_kernel, count=count, **sizes),
        out_shape=(
            jax.ShapeDtypeStruct((3, count * points, 2 * sens, wide), f32),
            jax.ShapeDtypeStruct((2 * sens * half, 2 * wide), f32),
        ),
        in_specs=in_vmem(1 + 2 * count),
        out_specs=tuple(in_vmem(2)),
        scratch_shapes=scratch(count),
        compiler_params=limit(12),
        name="first",
    )(table, *ready(orders[0]))
    count = len(orders[1])
    back = pl.pallas_call(
        functools.partial(bins_kernel, orders=orders, packing_back=packing_back, **sizes),
        out_shape=jax.ShapeDtypeStruct((width, packing_back.tiles, half, LANES), bf16),
        in_specs=in_smem(3) + in_vmem(4 + 2 * count),
        out_specs=in_vmem(1)[0],
        scratch_shapes=[pltpu.VMEM((3, count * points, 2 * sens, wide), f32)]
        + scratch(count)
        + [
            pltpu.VMEM((2 * sens * half, 2 * wide), f32),
            pltpu.VMEM((3, 2 * sens * half, wide), f32),
            pltpu.VMEM((width * points * half, 2 * wide), f32),
        ],
        compiler_params=limit(20),
        name="bins",
    )(me, noise_weight, noise_other, table, weights, kern_first, data_first, *ready(orders[1]))
    back, basis_other, deflation_other = lax.optimization_barrier(
        (back, basis_other, deflation_other)
    )
    basis, basis_other = kept(pltpu.VMEM, basis, basis_other)
    parts = exchange(back)
    flat, coeff = pl.pallas_call(
        functools.partial(coeff_kernel, points=points, steps=steps, rank=rank, packing=packing_back),
        out_shape=(
            jax.ShapeDtypeStruct((half, points * steps), f32),
            jax.ShapeDtypeStruct((width, half, 2 * rank), bf16),
        ),
        in_specs=in_smem(1) + in_vmem(3),
        out_specs=tuple(in_vmem(2)),
        compiler_params=limit(12),
        name="coeff",
    )(prior_scale, parts, basis, basis_other)
    flat_other = swap(flat)
    coeff_parts = exchange(coeff)
    coeff_other = swap(coeff_parts)
    return pl.pallas_call(
        functools.partial(deflate_kernel, points=points, steps=steps, rank=rank),
        out_shape=jax.ShapeDtypeStruct((probe_count, points, steps), f32),
        in_specs=in_smem(1) + in_vmem(8),
        out_specs=in_vmem(1)[0],
        compiler_params=limit(12),
        name="deflate",
    )(
        core, coeff_parts, coeff_other, deflation[None, :], deflation_other[None, :],
        flat, flat_other, basis, basis_other,
    )


def solution(mesh):
    placed = (
        P(None, ("grp", "pts"), None),
        P(None, ("grp", "pts"), "sen", None),
        P(("grp", "sen")),
        P("pts"),
        P("pts", "sen"),
        P("sen"),
    )

    def body(*args):
        width = mesh.shape["pts"]
        split = mesh.shape["sen"] == 2 and width == ROWS
        whole_tiles = args[2].shape[0] == width * ROWS and args[0].shape[0] == 2 * ROWS
        if not (split and whole_tiles):
            return local(*args)
        return local_split(*args)

    return jax.shard_map(
        body, mesh=mesh, in_specs=placed, out_specs=P(None, ("grp", "pts"), None), check_vma=False
    )
```

```python
import functools
import math

import jax
import jax.numpy as jnp
import numpy as np
from jax import lax
from jax.experimental import pallas as pl
from jax.experimental.pallas import tpu as pltpu
from jax.sharding import PartitionSpec as P

LANES = 128
ROWS = 8


def tables(steps_count):
    bins_count = steps_count + 1
    turns = (
        jnp.arange(steps_count, dtype=jnp.int32)[:, None]
        * jnp.arange(bins_count, dtype=jnp.int32)[None, :]
        % (2 * steps_count)
    )
    angle = turns.astype(jnp.float32) * (math.pi / steps_count)
    cosine = jnp.cos(angle)
    sine = jnp.sin(angle)
    freq = jnp.arange(bins_count, dtype=jnp.int32)
    edge = (freq == 0) | (freq == steps_count)
    weights = jnp.where(edge, 1.0, 2.0).astype(jnp.float32) / (2.0 * steps_count)
    forward = jnp.concatenate([cosine, -sine], axis=1)
    inverse = jnp.concatenate([cosine * weights[None, :], -sine * weights[None, :]], axis=1)
    return (forward, inverse)


def widened(value):
    return lax.optimization_barrier(value).astype(jnp.float32)


def complex_data(spec_real, spec_imag, kern_real, kern_imag):
    data_real = jnp.einsum(
        "kpf,psf->ksf", spec_real, kern_real, preferred_element_type=jnp.float32
    ) - jnp.einsum("kpf,psf->ksf", spec_imag, kern_imag, preferred_element_type=jnp.float32)
    data_imag = jnp.einsum(
        "kpf,psf->ksf", spec_real, kern_imag, preferred_element_type=jnp.float32
    ) + jnp.einsum("kpf,psf->ksf", spec_imag, kern_real, preferred_element_type=jnp.float32)
    return (data_real, data_imag)


def complex_adjoint(weight_real, weight_imag, kern_real, kern_imag):
    adj_real = jnp.einsum(
        "ksf,psf->kpf", weight_real, kern_real, preferred_element_type=jnp.float32
    ) + jnp.einsum("ksf,psf->kpf", weight_imag, kern_imag, preferred_element_type=jnp.float32)
    adj_imag = jnp.einsum(
        "ksf,psf->kpf", weight_imag, kern_real, preferred_element_type=jnp.float32
    ) - jnp.einsum("ksf,psf->kpf", weight_real, kern_imag, preferred_element_type=jnp.float32)
    return (adj_real, adj_imag)


def local(probes, kernel, noise_weight, prior_scale, basis, deflation):
    highest = lax.Precision.HIGHEST
    probe_count, point_count, steps_count = probes.shape
    bins_count = steps_count + 1
    sensor_count = noise_weight.shape[0]
    forward, inverse = tables(steps_count)
    scaled = probes.astype(jnp.float32) * prior_scale[None, :, None]
    spectrum = jnp.dot(scaled, forward, precision=highest).astype(jnp.bfloat16)
    noise_rows = jnp.tile(noise_weight, probe_count)
    width = lax.axis_size("pts")
    block = (bins_count + width - 1) // width
    extra = block * width - bins_count
    kern_pad = jnp.pad(kernel, ((0, 0), (0, 0), (0, 0), (0, extra)))
    spec_pad = jnp.pad(
        spectrum.reshape(probe_count, point_count, 2, bins_count),
        ((0, 0), (0, 0), (0, 0), (0, extra)),
    )
    kern_bins, spec_bins = (
        lax.all_to_all(kern_pad, "pts", split_axis=3, concat_axis=1, tiled=True),
        lax.all_to_all(spec_pad, "pts", split_axis=3, concat_axis=1, tiled=True),
    )
    bin_kern_real = kern_bins[0]
    bin_kern_imag = kern_bins[1]
    data_real, data_imag = complex_data(
        spec_bins[:, :, 0], spec_bins[:, :, 1], bin_kern_real, bin_kern_imag
    )
    data_bins = jnp.stack([data_real, data_imag], axis=2).reshape(
        probe_count * sensor_count, 2, block
    )
    rows_time = lax.all_to_all(
        data_bins.astype(jnp.bfloat16), "pts", split_axis=0, concat_axis=2, tiled=True
    ).astype(data_bins.dtype)
    local_rows = rows_time.shape[0]
    begin = lax.axis_index("pts") * local_rows
    local_noise = lax.dynamic_slice_in_dim(noise_rows, begin, local_rows)
    data_rows = rows_time[:, :, :bins_count].reshape(local_rows, 2 * bins_count)
    observed = jnp.dot(data_rows, inverse.T, precision=highest)
    residual = (observed * local_noise[:, None]).astype(jnp.bfloat16)
    weighted_local = (
        jnp.dot(widened(residual), inverse, precision=highest)
        .astype(jnp.bfloat16)
        .reshape(local_rows, 2, bins_count)
    )
    weighted_pad = jnp.pad(weighted_local, ((0, 0), (0, 0), (0, extra)))
    weighted_bins = lax.all_to_all(weighted_pad, "pts", split_axis=2, concat_axis=0, tiled=True)
    weighted_bins = weighted_bins.reshape(probe_count, sensor_count, 2, block)
    adj_real, adj_imag = complex_adjoint(
        weighted_bins[:, :, 0], weighted_bins[:, :, 1], bin_kern_real, bin_kern_imag
    )
    adj_bins = jnp.stack([adj_real, adj_imag], axis=2)
    adj_points = lax.all_to_all(
        adj_bins.astype(jnp.bfloat16), "pts", split_axis=1, concat_axis=3, tiled=True
    ).astype(adj_bins.dtype)
    adjoint = adj_points[..., :bins_count].reshape(probe_count, point_count, 2 * bins_count)
    back = jnp.dot(adjoint, forward.T, precision=highest)
    back = lax.psum(back.astype(jnp.bfloat16), "sen").astype(jnp.float32)
    hessian = back * prior_scale[None, :, None]
    flat = hessian.reshape(probe_count, point_count * steps_count)
    flat_low = flat.astype(jnp.bfloat16)
    coeff = jnp.dot(flat_low, basis, preferred_element_type=jnp.float32)
    coeff = lax.psum(coeff, "pts")
    shrunk = (coeff * deflation[None, :]).astype(jnp.bfloat16)
    correction = lax.dot_general(
        shrunk, basis, (((1,), (1,)), ((), ())), preferred_element_type=jnp.float32
    )
    correction = lax.psum(correction.astype(jnp.bfloat16), "sen").astype(jnp.float32)
    return (flat - correction).reshape(probe_count, point_count, steps_count)


def round_up(value, step):
    return (value + step - 1) // step * step


def packed_tables(steps_count, wide):
    bins_count = steps_count + 1
    turns = np.arange(steps_count)[:, None] * np.arange(bins_count)[None, :] % (2 * steps_count)
    angle = turns.astype(np.float64) * (math.pi / steps_count)
    table = np.zeros((wide, 2 * wide), np.float32)
    table[:steps_count, :bins_count] = np.cos(angle)
    table[:steps_count, wide : wide + bins_count] = -np.sin(angle)
    weights = np.zeros((1, wide), np.float32)
    weights[0, :bins_count] = 2.0 / (2.0 * steps_count)
    weights[0, 0] = weights[0, steps_count] = 1.0 / (2.0 * steps_count)
    return jnp.asarray(table.astype(jnp.bfloat16)), jnp.asarray(weights)


NT = (((1,), (1,)), ((), ()))


class Packing:
    def __init__(self, rows, length):
        self.full = length // LANES
        self.tail = length % LANES
        self.slots = LANES // self.tail
        self.first_tail = rows * self.full
        self.tiles = self.first_tail + -(-rows // self.slots)

    def place(self, row):
        return self.first_tail + row // self.slots, row % self.slots * self.tail


def turned(tile, lanes):
    lanes = lanes % LANES
    return pltpu.roll(tile, lanes, axis=tile.ndim - 1) if lanes else tile


def add_tail(packing, row, value, merged):
    tile, lane = packing.place(row)
    tail = value[..., packing.full * LANES : (packing.full + 1) * LANES]
    where = lax.broadcasted_iota(jnp.int32, tail.shape, tail.ndim - 1)
    tail = turned(jnp.where(where < packing.tail, tail, 0.0), lane)
    merged[tile] = merged[tile] + tail if tile in merged else tail


def store_packed(out_tile, packing, row, value, merged):
    for t in range(packing.full):
        lanes = slice(t * LANES, (t + 1) * LANES)
        out_tile(row * packing.full + t, value[..., lanes].astype(jnp.bfloat16))
    add_tail(packing, row, value, merged)


def store_tails(out_tile, merged):
    for tile, value in merged.items():
        out_tile(tile, value.astype(jnp.bfloat16))


def pack_kernel(index, prior_far, kernel, probes, *refs, order, sens, half, packing):
    outs = refs[: len(order)]
    prior, kernel_here, probes_here, sems = refs[len(order) :]
    f32 = jnp.float32
    _, points, _ = probes_here.shape
    edge = packing.full * LANES
    me = index[0]
    mine = pl.multiple_of(index[1] * half, half)
    copies = [
        pltpu.make_async_copy(probes.at[pl.ds(mine, half)], probes_here, sems.at[0]),
        pltpu.make_async_copy(prior_far, prior, sems.at[1]),
    ]
    for slot, relative in enumerate(order):
        rows = pl.ds(pl.multiple_of((me ^ relative) * sens, sens), sens)
        copies.append(
            pltpu.make_async_copy(
                kernel.at[:, :, rows, :], kernel_here.at[slot], sems.at[2 + slot]
            )
        )
    for copy in copies:
        copy.start()

    def padded(value):
        missing = jnp.zeros((value.shape[0], edge + LANES - value.shape[1]), f32)
        return jnp.concatenate([value, missing], axis=1)

    copies[0].wait()
    copies[1].wait()
    scaled = probes_here[...].astype(f32)
    tiles = {}
    tails = {}
    for p in range(points):
        store_packed(tiles.__setitem__, packing, 2 * points + p, padded(scaled[:, p, :] * prior[p]), tails)
    for slot, out in enumerate(outs):
        copies[2 + slot].wait()

        def out_tile(tile, value, out=out):
            out[tile] = value

        merged = dict(tails)
        for tile, value in tiles.items():
            out_tile(tile, value)
        for row in range(2 * points):
            value = padded(kernel_here[slot, row // points, row % points].astype(f32))
            store_packed(out_tile, packing, row, value, merged)
        store_tails(out_tile, merged)


def unpack(source, row, packing):
    f32 = jnp.float32
    tiles = [source[row * packing.full + t].astype(f32) for t in range(packing.full)]
    tile, lane = packing.place(row)
    tiles.append(turned(source[tile].astype(f32), -lane))
    return tiles


def widen(sources, kern, *, packing, points, sens):
    for b, pair in enumerate(sources):
        for half, source in enumerate(pair):
            at = slice(half * sens, (half + 1) * sens)
            for p in range(points):
                real = unpack(source, p, packing)
                imag = unpack(source, points + p, packing)
                for t, (x, y) in enumerate(zip(real, imag)):
                    lanes = slice(t * LANES, (t + 1) * LANES)
                    kern[0, b * points + p, at, lanes] = x
                    kern[1, b * points + p, at, lanes] = x + y
                    kern[2, b * points + p, at, lanes] = x - y


def spectra(sources, table, spec, rows, *, packing, points, half, wide):
    for b, (own, _) in enumerate(sources):
        for p in range(points):
            at = slice((b * points + p) * half, (b * points + p + 1) * half)
            for t, tile in enumerate(unpack(own, 2 * points + p, packing)):
                rows[at, t * LANES : (t + 1) * LANES] = tile
    got = jnp.dot(rows[...].astype(jnp.bfloat16), table[...], preferred_element_type=jnp.float32)
    real = got[:, :wide]
    imag = got[:, wide:]
    spec[0] = real + imag
    spec[1] = imag
    spec[2] = real


def forward_sum(kern, spec, data, earlier, *, points, sens, half, wide):
    f32 = jnp.float32
    blocks = kern.shape[1] // points

    def tile_step(ft, carry):
        lanes = pl.ds(pl.multiple_of(ft * LANES, LANES), LANES)
        shifted = pl.ds(pl.multiple_of(wide + ft * LANES, LANES), LANES)
        for first in range(0, 2 * sens, sens):

            def source(b, acc, first=first):
                acc = list(acc)
                for p in range(points):
                    q = b * points + p
                    at = pl.ds(pl.multiple_of(q * half, ROWS), half)
                    both = spec[0, at, lanes]
                    imag = spec[1, at, lanes]
                    real = spec[2, at, lanes]
                    for s in range(sens):
                        row = slice(first + s, first + s + 1)
                        acc[3 * s] += kern[0, q, row, lanes] * both
                        acc[3 * s + 1] += kern[1, q, row, lanes] * imag
                        acc[3 * s + 2] += kern[2, q, row, lanes] * real
                return tuple(acc)

            zero = jnp.zeros((half, LANES), f32)
            acc = lax.fori_loop(0, blocks, source, (zero,) * (3 * sens))
            for s in range(sens):
                at = slice((first + s) * half, (first + s + 1) * half)
                real = acc[3 * s] - acc[3 * s + 1]
                imag = acc[3 * s] - acc[3 * s + 2]
                if earlier is not None:
                    real += earlier[at, lanes]
                    imag += earlier[at, shifted]
                data[at, lanes] = real
                data[at, shifted] = imag
        return carry

    lax.fori_loop(0, wide // LANES, tile_step, 0)


def paired(refs, count):
    return list(zip(refs[:count], refs[count : 2 * count]))


def first_kernel(table, *refs, count, points, sens, half, wide, packing):
    sources = paired(refs, count)
    kern, data, spec, rows = refs[2 * count :]
    spectra(sources, table, spec, rows, packing=packing, points=points, half=half, wide=wide)
    widen(sources, kern, packing=packing, points=points, sens=sens)
    forward_sum(kern, spec, data, None, points=points, sens=sens, half=half, wide=wide)


def bins_kernel(
    index, noise_own, noise_other, table, weights, kern_first, data_first, *refs,
    orders, points, sens, half, wide, packing, packing_back,
):
    count = len(orders[1])
    sources = paired(refs, count)
    out, kern, spec, rows, data, wdata, adjoint = refs[2 * count :]
    tiles = wide // LANES
    f32 = jnp.float32
    bf16 = jnp.bfloat16
    spectra(sources, table, spec, rows, packing=packing, points=points, half=half, wide=wide)
    widen(sources, kern, packing=packing, points=points, sens=sens)
    forward_sum(kern, spec, data, data_first, points=points, sens=sens, half=half, wide=wide)
    table_v = table[...]
    weight_rows = weights[...]
    scaled = jnp.concatenate(
        [data[:, :wide] * weight_rows, data[:, wide:] * weight_rows], axis=1
    ).astype(bf16)
    observed = lax.dot_general(scaled, table_v, NT, preferred_element_type=f32)
    mine = index[0] * sens
    scales = [noise_own[mine + s] for s in range(sens)]
    scales += [noise_other[mine + s] for s in range(sens)]
    residual = jnp.concatenate(
        [observed[s * half : (s + 1) * half] * scale for s, scale in enumerate(scales)], axis=0
    ).astype(bf16)
    weighted = jnp.dot(residual, table_v, preferred_element_type=f32)
    real = weighted[:, :wide] * weight_rows
    imag = weighted[:, wide:] * weight_rows
    wdata[0] = real + imag
    wdata[1] = imag
    wdata[2] = real

    base = 0
    for source, order in ((kern_first, orders[0]), (kern, orders[1])):

        def adjoint_tile(step, carry, source=source, base=base):
            b = step // tiles
            ft = step % tiles
            lanes = pl.ds(pl.multiple_of(ft * LANES, LANES), LANES)
            shifted = pl.ds(pl.multiple_of(wide + ft * LANES, LANES), LANES)
            zero = jnp.zeros((half, LANES), f32)
            acc = [zero] * (3 * points)
            for s in range(2 * sens):
                at = slice(s * half, (s + 1) * half)
                both = wdata[0, at, lanes]
                imag = wdata[1, at, lanes]
                real = wdata[2, at, lanes]
                row = slice(s, s + 1)
                for p in range(points):
                    q = b * points + p
                    acc[3 * p] += source[0, q, row, lanes] * both
                    acc[3 * p + 1] += source[2, q, row, lanes] * imag
                    acc[3 * p + 2] += source[1, q, row, lanes] * real
            for p in range(points):
                at = pl.ds(pl.multiple_of((base + b * points + p) * half, ROWS), half)
                adjoint[at, lanes] = acc[3 * p] - acc[3 * p + 1]
                adjoint[at, shifted] = acc[3 * p] - acc[3 * p + 2]
            return carry

        lax.fori_loop(0, len(order) * tiles, adjoint_tile, 0)
        base += len(order) * points
    back = lax.dot_general(adjoint[...].astype(bf16), table_v, NT, preferred_element_type=f32)
    for b, relative in enumerate(orders[0] + orders[1]):
        there = index[0] ^ relative

        def out_tile(tile, value, there=there):
            out[there, tile] = value

        merged = {}
        for p in range(points):
            at = slice((b * points + p) * half, (b * points + p + 1) * half)
            store_packed(out_tile, packing_back, p, back[at], merged)
        store_tails(out_tile, merged)


def summed(parts):
    total = parts[0].astype(jnp.float32)
    for j in range(1, parts.shape[0]):
        total += parts[j].astype(jnp.float32)
    return total


def coeff_kernel(prior, parts, basis_own, basis_other, flat, coeff, *, points, steps, rank, packing):
    f32 = jnp.float32
    total = summed(parts)
    for p in range(points):
        tiles = [total[p * packing.full + t] for t in range(packing.full)]
        tile, lane = packing.place(p)
        tiles.append(turned(total[tile], -lane))
        piece = jnp.concatenate(tiles, axis=1) * prior[p]
        flat[:, p * steps : (p + 1) * steps] = piece[:, :steps]
    low = flat[...].astype(jnp.bfloat16)
    own = jnp.dot(low, basis_own[...], preferred_element_type=f32).astype(jnp.bfloat16)
    other = jnp.dot(low, basis_other[...], preferred_element_type=f32).astype(jnp.bfloat16)
    for j in range(coeff.shape[0]):
        coeff[j, :, :rank] = own
        coeff[j, :, rank:] = other


def deflate_kernel(
    core, parts_own, parts_other, deflation_own, deflation_other, flat_own, flat_other,
    basis_own, basis_other, out,
    *, points, steps, rank,
):
    f32 = jnp.float32
    bf16 = jnp.bfloat16
    own = summed(parts_own)
    other = summed(parts_other)
    half = own.shape[0]
    here = jnp.concatenate([own[:, :rank], other[:, rank:]], axis=0) * deflation_own[...]
    there = jnp.concatenate([own[:, rank:], other[:, :rank]], axis=0) * deflation_other[...]
    correction = lax.dot_general(here.astype(bf16), basis_own[...], NT, preferred_element_type=f32)
    correction += lax.dot_general(there.astype(bf16), basis_other[...], NT, preferred_element_type=f32)
    result = jnp.concatenate([flat_own[...], flat_other[...]], axis=0) - correction
    mine = core[0] * half
    for p in range(points):
        piece = result[:, p * steps : (p + 1) * steps]
        out[pl.ds(mine, half), p, :] = piece[:half]
        out[pl.ds(half - mine, half), p, :] = piece[half:]


def split_order(width):
    return list(range(width // 2)), list(range(width // 2, width))


def stage_kernel(far, near, sem):
    copy = pltpu.make_async_copy(far, near, sem)
    copy.start()
    copy.wait()


def kept(space, *values):
    return [pltpu.with_memory_space_constraint(value, space) for value in values]


def in_vmem(count):
    return [pl.BlockSpec(memory_space=pltpu.VMEM) for _ in range(count)]


def in_smem(count):
    return [pl.BlockSpec(memory_space=pltpu.SMEM) for _ in range(count)]


def limit(mib):
    return pltpu.CompilerParams(vmem_limit_bytes=mib * 1024 * 1024)


def local_split(probes, kernel, noise_weight, prior_scale, basis, deflation):
    bf16 = jnp.bfloat16
    f32 = jnp.float32
    probe_count, points, steps = probes.shape
    bins_count = steps + 1
    width = lax.axis_size("pts")
    sens = noise_weight.shape[0] // width
    half = probe_count // 2
    rank = basis.shape[1]
    wide = round_up(bins_count, LANES)
    me = jnp.full((1,), lax.axis_index("pts"), jnp.int32)
    core_index = lax.axis_index("sen")
    core = jnp.full((1,), core_index, jnp.int32)

    def swap(value):
        return lax.ppermute(value, "sen", [(0, 1), (1, 0)])

    def exchange(value):
        return lax.all_to_all(value, "pts", split_axis=0, concat_axis=0, tiled=False)

    table, weights = packed_tables(steps, wide)
    packing = Packing(3 * points, bins_count)
    packing_back = Packing(points, steps)
    sizes = dict(points=points, sens=sens, half=half, wide=wide, packing=packing)
    orders = split_order(width)
    order = orders[0] + orders[1]
    places = jnp.stack([me[0], core[0]])
    chunk = jax.ShapeDtypeStruct((packing.tiles, sens, LANES), bf16)
    in_hbm = pl.BlockSpec(memory_space=pltpu.HBM)
    sent = pl.pallas_call(
        functools.partial(pack_kernel, order=order, sens=sens, half=half, packing=packing),
        out_shape=(chunk,) * width,
        in_specs=in_smem(1) + [in_hbm] * 3,
        out_specs=tuple(in_vmem(width)),
        scratch_shapes=[
            pltpu.SMEM(prior_scale.shape, f32),
            pltpu.VMEM((width, 2, points, sens, bins_count), bf16),
            pltpu.VMEM((half, points, steps), bf16),
            pltpu.SemaphoreType.DMA((2 + width,)),
        ],
        compiler_params=limit(8),
        name="pack",
    )(places, *kept(pltpu.HBM, prior_scale, kernel, probes))
    blocks = {}
    others = {}
    for relative, value in zip(order, sent):
        if relative:
            value = lax.ppermute(value, "pts", [(i, i ^ relative) for i in range(width)])
        blocks[relative] = value
        others[relative] = swap(value)
    noise_other = swap(noise_weight)
    deflation_other = swap(deflation)
    basis_other = swap(basis)

    def scratch(count):
        return [
            pltpu.VMEM((3, count * points * half, wide), f32),
            pltpu.VMEM((count * points * half, wide), f32),
        ]

    def ready(part):
        return [blocks[r] for r in part] + [others[r] for r in part]

    table = pl.pallas_call(
        stage_kernel,
        out_shape=pltpu.VMEM(table.shape, bf16),
        in_specs=[in_hbm],
        out_specs=in_vmem(1)[0],
        scratch_shapes=[pltpu.SemaphoreType.DMA],
        compiler_params=limit(2),
        name="stage",
    )(*kept(pltpu.HBM, table))
    count = len(orders[0])
    kern_first, data_first = pl.pallas_call(
        functools.partial(first_kernel, count=count, **sizes),
        out_shape=(
            jax.ShapeDtypeStruct((3, count * points, 2 * sens, wide), f32),
            jax.ShapeDtypeStruct((2 * sens * half, 2 * wide), f32),
        ),
        in_specs=in_vmem(1 + 2 * count),
        out_specs=tuple(in_vmem(2)),
        scratch_shapes=scratch(count),
        compiler_params=limit(12),
        name="first",
    )(table, *ready(orders[0]))
    count = len(orders[1])
    back = pl.pallas_call(
        functools.partial(bins_kernel, orders=orders, packing_back=packing_back, **sizes),
        out_shape=jax.ShapeDtypeStruct((width, packing_back.tiles, half, LANES), bf16),
        in_specs=in_smem(3) + in_vmem(4 + 2 * count),
        out_specs=in_vmem(1)[0],
        scratch_shapes=[pltpu.VMEM((3, count * points, 2 * sens, wide), f32)]
        + scratch(count)
        + [
            pltpu.VMEM((2 * sens * half, 2 * wide), f32),
            pltpu.VMEM((3, 2 * sens * half, wide), f32),
            pltpu.VMEM((width * points * half, 2 * wide), f32),
        ],
        compiler_params=limit(20),
        name="bins",
    )(me, noise_weight, noise_other, table, weights, kern_first, data_first, *ready(orders[1]))
    back, basis_other, deflation_other = lax.optimization_barrier(
        (back, basis_other, deflation_other)
    )
    basis, basis_other = kept(pltpu.VMEM, basis, basis_other)
    parts = exchange(back)
    flat, coeff = pl.pallas_call(
        functools.partial(coeff_kernel, points=points, steps=steps, rank=rank, packing=packing_back),
        out_shape=(
            jax.ShapeDtypeStruct((half, points * steps), f32),
            jax.ShapeDtypeStruct((width, half, 2 * rank), bf16),
        ),
        in_specs=in_smem(1) + in_vmem(3),
        out_specs=tuple(in_vmem(2)),
        compiler_params=limit(12),
        name="coeff",
    )(prior_scale, parts, basis, basis_other)
    flat_other = swap(flat)
    coeff_parts = exchange(coeff)
    coeff_other = swap(coeff_parts)
    return pl.pallas_call(
        functools.partial(deflate_kernel, points=points, steps=steps, rank=rank),
        out_shape=jax.ShapeDtypeStruct((probe_count, points, steps), f32),
        in_specs=in_smem(1) + in_vmem(8),
        out_specs=in_vmem(1)[0],
        compiler_params=limit(12),
        name="deflate",
    )(
        core, coeff_parts, coeff_other, deflation[None, :], deflation_other[None, :],
        flat, flat_other, basis, basis_other,
    )


def solution(mesh):
    placed = (
        P(None, ("grp", "pts"), None),
        P(None, ("grp", "pts"), "sen", None),
        P(("grp", "sen")),
        P("pts"),
        P("pts", "sen"),
        P("sen"),
    )

    def body(*args):
        width = mesh.shape["pts"]
        split = mesh.shape["sen"] == 2 and width == ROWS
        whole_tiles = args[2].shape[0] == width * ROWS and args[0].shape[0] == 2 * ROWS
        if not (split and whole_tiles):
            return local(*args)
        return local_split(*args)

    return jax.shard_map(
        body, mesh=mesh, in_specs=placed, out_specs=P(None, ("grp", "pts"), None), check_vma=False
    )
```

```python
import functools
import math

import jax
import jax.numpy as jnp
import numpy as np
from jax import lax
from jax.experimental import pallas as pl
from jax.experimental.pallas import tpu as pltpu
from jax.sharding import PartitionSpec as P

LANES = 128
ROWS = 8


def tables(steps_count):
    bins_count = steps_count + 1
    turns = (
        jnp.arange(steps_count, dtype=jnp.int32)[:, None]
        * jnp.arange(bins_count, dtype=jnp.int32)[None, :]
        % (2 * steps_count)
    )
    angle = turns.astype(jnp.float32) * (math.pi / steps_count)
    cosine = jnp.cos(angle)
    sine = jnp.sin(angle)
    freq = jnp.arange(bins_count, dtype=jnp.int32)
    edge = (freq == 0) | (freq == steps_count)
    weights = jnp.where(edge, 1.0, 2.0).astype(jnp.float32) / (2.0 * steps_count)
    forward = jnp.concatenate([cosine, -sine], axis=1)
    inverse = jnp.concatenate([cosine * weights[None, :], -sine * weights[None, :]], axis=1)
    return (forward, inverse)


def widened(value):
    return lax.optimization_barrier(value).astype(jnp.float32)


def complex_data(spec_real, spec_imag, kern_real, kern_imag):
    data_real = jnp.einsum(
        "kpf,psf->ksf", spec_real, kern_real, preferred_element_type=jnp.float32
    ) - jnp.einsum("kpf,psf->ksf", spec_imag, kern_imag, preferred_element_type=jnp.float32)
    data_imag = jnp.einsum(
        "kpf,psf->ksf", spec_real, kern_imag, preferred_element_type=jnp.float32
    ) + jnp.einsum("kpf,psf->ksf", spec_imag, kern_real, preferred_element_type=jnp.float32)
    return (data_real, data_imag)


def complex_adjoint(weight_real, weight_imag, kern_real, kern_imag):
    adj_real = jnp.einsum(
        "ksf,psf->kpf", weight_real, kern_real, preferred_element_type=jnp.float32
    ) + jnp.einsum("ksf,psf->kpf", weight_imag, kern_imag, preferred_element_type=jnp.float32)
    adj_imag = jnp.einsum(
        "ksf,psf->kpf", weight_imag, kern_real, preferred_element_type=jnp.float32
    ) - jnp.einsum("ksf,psf->kpf", weight_real, kern_imag, preferred_element_type=jnp.float32)
    return (adj_real, adj_imag)


def local(probes, kernel, noise_weight, prior_scale, basis, deflation):
    highest = lax.Precision.HIGHEST
    probe_count, point_count, steps_count = probes.shape
    bins_count = steps_count + 1
    sensor_count = noise_weight.shape[0]
    forward, inverse = tables(steps_count)
    scaled = probes.astype(jnp.float32) * prior_scale[None, :, None]
    spectrum = jnp.dot(scaled, forward, precision=highest).astype(jnp.bfloat16)
    noise_rows = jnp.tile(noise_weight, probe_count)
    width = lax.axis_size("pts")
    block = (bins_count + width - 1) // width
    extra = block * width - bins_count
    kern_pad = jnp.pad(kernel, ((0, 0), (0, 0), (0, 0), (0, extra)))
    spec_pad = jnp.pad(
        spectrum.reshape(probe_count, point_count, 2, bins_count),
        ((0, 0), (0, 0), (0, 0), (0, extra)),
    )
    kern_bins, spec_bins = (
        lax.all_to_all(kern_pad, "pts", split_axis=3, concat_axis=1, tiled=True),
        lax.all_to_all(spec_pad, "pts", split_axis=3, concat_axis=1, tiled=True),
    )
    bin_kern_real = kern_bins[0]
    bin_kern_imag = kern_bins[1]
    data_real, data_imag = complex_data(
        spec_bins[:, :, 0], spec_bins[:, :, 1], bin_kern_real, bin_kern_imag
    )
    data_bins = jnp.stack([data_real, data_imag], axis=2).reshape(
        probe_count * sensor_count, 2, block
    )
    rows_time = lax.all_to_all(
        data_bins.astype(jnp.bfloat16), "pts", split_axis=0, concat_axis=2, tiled=True
    ).astype(data_bins.dtype)
    local_rows = rows_time.shape[0]
    begin = lax.axis_index("pts") * local_rows
    local_noise = lax.dynamic_slice_in_dim(noise_rows, begin, local_rows)
    data_rows = rows_time[:, :, :bins_count].reshape(local_rows, 2 * bins_count)
    observed = jnp.dot(data_rows, inverse.T, precision=highest)
    residual = (observed * local_noise[:, None]).astype(jnp.bfloat16)
    weighted_local = (
        jnp.dot(widened(residual), inverse, precision=highest)
        .astype(jnp.bfloat16)
        .reshape(local_rows, 2, bins_count)
    )
    weighted_pad = jnp.pad(weighted_local, ((0, 0), (0, 0), (0, extra)))
    weighted_bins = lax.all_to_all(weighted_pad, "pts", split_axis=2, concat_axis=0, tiled=True)
    weighted_bins = weighted_bins.reshape(probe_count, sensor_count, 2, block)
    adj_real, adj_imag = complex_adjoint(
        weighted_bins[:, :, 0], weighted_bins[:, :, 1], bin_kern_real, bin_kern_imag
    )
    adj_bins = jnp.stack([adj_real, adj_imag], axis=2)
    adj_points = lax.all_to_all(
        adj_bins.astype(jnp.bfloat16), "pts", split_axis=1, concat_axis=3, tiled=True
    ).astype(adj_bins.dtype)
    adjoint = adj_points[..., :bins_count].reshape(probe_count, point_count, 2 * bins_count)
    back = jnp.dot(adjoint, forward.T, precision=highest)
    back = lax.psum(back.astype(jnp.bfloat16), "sen").astype(jnp.float32)
    hessian = back * prior_scale[None, :, None]
    flat = hessian.reshape(probe_count, point_count * steps_count)
    flat_low = flat.astype(jnp.bfloat16)
    coeff = jnp.dot(flat_low, basis, preferred_element_type=jnp.float32)
    coeff = lax.psum(coeff, "pts")
    shrunk = (coeff * deflation[None, :]).astype(jnp.bfloat16)
    correction = lax.dot_general(
        shrunk, basis, (((1,), (1,)), ((), ())), preferred_element_type=jnp.float32
    )
    correction = lax.psum(correction.astype(jnp.bfloat16), "sen").astype(jnp.float32)
    return (flat - correction).reshape(probe_count, point_count, steps_count)


def round_up(value, step):
    return (value + step - 1) // step * step


def packed_tables(steps_count, wide):
    bins_count = steps_count + 1
    turns = np.arange(steps_count)[:, None] * np.arange(bins_count)[None, :] % (2 * steps_count)
    angle = turns.astype(np.float64) * (math.pi / steps_count)
    table = np.zeros((wide, 2 * wide), np.float32)
    table[:steps_count, :bins_count] = np.cos(angle)
    table[:steps_count, wide : wide + bins_count] = -np.sin(angle)
    weights = np.zeros((1, wide), np.float32)
    weights[0, :bins_count] = 2.0 / (2.0 * steps_count)
    weights[0, 0] = weights[0, steps_count] = 1.0 / (2.0 * steps_count)
    return jnp.asarray(table.astype(jnp.bfloat16)), jnp.asarray(weights)


NT = (((1,), (1,)), ((), ()))


class Packing:
    def __init__(self, rows, length):
        self.full = length // LANES
        self.tail = length % LANES
        self.slots = LANES // self.tail
        self.first_tail = rows * self.full
        self.tiles = self.first_tail + -(-rows // self.slots)

    def place(self, row):
        return self.first_tail + row // self.slots, row % self.slots * self.tail


def turned(tile, lanes):
    lanes = lanes % LANES
    return pltpu.roll(tile, lanes, axis=tile.ndim - 1) if lanes else tile


def add_tail(packing, row, value, merged):
    tile, lane = packing.place(row)
    tail = value[..., packing.full * LANES : (packing.full + 1) * LANES]
    where = lax.broadcasted_iota(jnp.int32, tail.shape, tail.ndim - 1)
    tail = turned(jnp.where(where < packing.tail, tail, 0.0), lane)
    merged[tile] = merged[tile] + tail if tile in merged else tail


def store_packed(out_tile, packing, row, value, merged):
    for t in range(packing.full):
        lanes = slice(t * LANES, (t + 1) * LANES)
        out_tile(row * packing.full + t, value[..., lanes].astype(jnp.bfloat16))
    add_tail(packing, row, value, merged)


def store_tails(out_tile, merged):
    for tile, value in merged.items():
        out_tile(tile, value.astype(jnp.bfloat16))


def pack_kernel(index, prior_far, kernel, probes, *refs, order, half, packing):
    outs = refs[: len(order)]
    prior, kernel_here, probes_here, sems = refs[len(order) :]
    f32 = jnp.float32
    _, points, _ = probes_here.shape
    edge = packing.full * LANES
    me = index[0]
    mine = pl.multiple_of(index[1] * half, half)
    copies = [
        pltpu.make_async_copy(probes.at[pl.ds(mine, half)], probes_here, sems.at[0]),
        pltpu.make_async_copy(prior_far, prior, sems.at[1]),
    ]
    for row in range(2 * points):
        at = (row // points, row % points)
        copies.append(pltpu.make_async_copy(kernel.at[at], kernel_here.at[at], sems.at[2 + row]))
    for copy in copies:
        copy.start()

    def padded(value):
        missing = jnp.zeros((value.shape[0], edge + LANES - value.shape[1]), f32)
        return jnp.concatenate([value, missing], axis=1)

    copies[0].wait()
    copies[1].wait()
    scaled = probes_here[...].astype(f32)
    tiles = {}
    tails = {}
    for p in range(points):
        store_packed(tiles.__setitem__, packing, 2 * points + p, padded(scaled[:, p, :] * prior[p]), tails)
    for copy in copies[2:]:
        copy.wait()
    for relative, out in zip(order, outs):

        def out_tile(tile, value, out=out):
            out[tile] = value

        merged = dict(tails)
        for tile, value in tiles.items():
            out_tile(tile, value)
        for row in range(2 * points):
            value = padded(kernel_here[row // points, row % points, me ^ relative].astype(f32))
            store_packed(out_tile, packing, row, value, merged)
        store_tails(out_tile, merged)


def unpack(source, row, packing):
    f32 = jnp.float32
    tiles = [source[row * packing.full + t].astype(f32) for t in range(packing.full)]
    tile, lane = packing.place(row)
    tiles.append(turned(source[tile].astype(f32), -lane))
    return tiles


def widen(sources, kern, *, packing, points, sens):
    for b, pair in enumerate(sources):
        for half, source in enumerate(pair):
            at = slice(half * sens, (half + 1) * sens)
            for p in range(points):
                real = unpack(source, p, packing)
                imag = unpack(source, points + p, packing)
                for t, (x, y) in enumerate(zip(real, imag)):
                    lanes = slice(t * LANES, (t + 1) * LANES)
                    kern[0, b * points + p, at, lanes] = x
                    kern[1, b * points + p, at, lanes] = x + y
                    kern[2, b * points + p, at, lanes] = x - y


def spectra(sources, table, spec, rows, *, packing, points, half, wide):
    for b, (own, _) in enumerate(sources):
        for p in range(points):
            at = slice((b * points + p) * half, (b * points + p + 1) * half)
            for t, tile in enumerate(unpack(own, 2 * points + p, packing)):
                rows[at, t * LANES : (t + 1) * LANES] = tile
    got = jnp.dot(rows[...].astype(jnp.bfloat16), table[...], preferred_element_type=jnp.float32)
    real = got[:, :wide]
    imag = got[:, wide:]
    spec[0] = real + imag
    spec[1] = imag
    spec[2] = real


def forward_sum(kern, spec, data, earlier, *, points, sens, half, wide):
    f32 = jnp.float32
    blocks = kern.shape[1] // points

    def tile_step(ft, carry):
        lanes = pl.ds(pl.multiple_of(ft * LANES, LANES), LANES)
        shifted = pl.ds(pl.multiple_of(wide + ft * LANES, LANES), LANES)
        for first in range(0, 2 * sens, sens):

            def source(b, acc, first=first):
                acc = list(acc)
                for p in range(points):
                    q = b * points + p
                    at = pl.ds(pl.multiple_of(q * half, ROWS), half)
                    both = spec[0, at, lanes]
                    imag = spec[1, at, lanes]
                    real = spec[2, at, lanes]
                    for s in range(sens):
                        row = slice(first + s, first + s + 1)
                        acc[3 * s] += kern[0, q, row, lanes] * both
                        acc[3 * s + 1] += kern[1, q, row, lanes] * imag
                        acc[3 * s + 2] += kern[2, q, row, lanes] * real
                return tuple(acc)

            zero = jnp.zeros((half, LANES), f32)
            acc = lax.fori_loop(0, blocks, source, (zero,) * (3 * sens))
            for s in range(sens):
                at = slice((first + s) * half, (first + s + 1) * half)
                real = acc[3 * s] - acc[3 * s + 1]
                imag = acc[3 * s] - acc[3 * s + 2]
                if earlier is not None:
                    real += earlier[at, lanes]
                    imag += earlier[at, shifted]
                data[at, lanes] = real
                data[at, shifted] = imag
        return carry

    lax.fori_loop(0, wide // LANES, tile_step, 0)


def paired(refs, count):
    return list(zip(refs[:count], refs[count : 2 * count]))


def first_kernel(table, *refs, count, points, sens, half, wide, packing):
    sources = paired(refs, count)
    kern, data, spec, rows = refs[2 * count :]
    spectra(sources, table, spec, rows, packing=packing, points=points, half=half, wide=wide)
    widen(sources, kern, packing=packing, points=points, sens=sens)
    forward_sum(kern, spec, data, None, points=points, sens=sens, half=half, wide=wide)


def bins_kernel(
    index, noise_far, noise_other_far, table, weights, kern_first, data_first, *refs,
    orders, points, sens, half, wide, packing, packing_back,
):
    count = len(orders[1])
    sources = paired(refs, count)
    out, kern, spec, rows, data, wdata, adjoint, noise_own, noise_other, sems = refs[2 * count :]
    copies = [
        pltpu.make_async_copy(noise_far, noise_own, sems.at[0]),
        pltpu.make_async_copy(noise_other_far, noise_other, sems.at[1]),
    ]
    for copy in copies:
        copy.start()
    tiles = wide // LANES
    f32 = jnp.float32
    bf16 = jnp.bfloat16
    spectra(sources, table, spec, rows, packing=packing, points=points, half=half, wide=wide)
    widen(sources, kern, packing=packing, points=points, sens=sens)
    forward_sum(kern, spec, data, data_first, points=points, sens=sens, half=half, wide=wide)
    table_v = table[...]
    weight_rows = weights[...]
    scaled = jnp.concatenate(
        [data[:, :wide] * weight_rows, data[:, wide:] * weight_rows], axis=1
    ).astype(bf16)
    observed = lax.dot_general(scaled, table_v, NT, preferred_element_type=f32)
    for copy in copies:
        copy.wait()
    mine = index[0] * sens
    scales = [noise_own[mine + s] for s in range(sens)]
    scales += [noise_other[mine + s] for s in range(sens)]
    residual = jnp.concatenate(
        [observed[s * half : (s + 1) * half] * scale for s, scale in enumerate(scales)], axis=0
    ).astype(bf16)
    weighted = jnp.dot(residual, table_v, preferred_element_type=f32)
    real = weighted[:, :wide] * weight_rows
    imag = weighted[:, wide:] * weight_rows
    wdata[0] = real + imag
    wdata[1] = imag
    wdata[2] = real

    base = 0
    group = 2 * points
    for source, order in ((kern_first, orders[0]), (kern, orders[1])):

        def adjoint_tile(step, carry, source=source, base=base):
            first = step // tiles * group
            ft = step % tiles
            lanes = pl.ds(pl.multiple_of(ft * LANES, LANES), LANES)
            shifted = pl.ds(pl.multiple_of(wide + ft * LANES, LANES), LANES)
            zero = jnp.zeros((half, LANES), f32)
            acc = [zero] * (3 * group)
            for s in range(2 * sens):
                at = slice(s * half, (s + 1) * half)
                both = wdata[0, at, lanes]
                imag = wdata[1, at, lanes]
                real = wdata[2, at, lanes]
                row = slice(s, s + 1)
                for p in range(group):
                    acc[3 * p] += source[0, first + p, row, lanes] * both
                    acc[3 * p + 1] += source[2, first + p, row, lanes] * imag
                    acc[3 * p + 2] += source[1, first + p, row, lanes] * real
            for p in range(group):
                at = pl.ds(pl.multiple_of((base + first + p) * half, ROWS), half)
                adjoint[at, lanes] = acc[3 * p] - acc[3 * p + 1]
                adjoint[at, shifted] = acc[3 * p] - acc[3 * p + 2]
            return carry

        lax.fori_loop(0, len(order) * points // group * tiles, adjoint_tile, 0)
        base += len(order) * points
    back = lax.dot_general(adjoint[...].astype(bf16), table_v, NT, preferred_element_type=f32)
    for b, relative in enumerate(orders[0] + orders[1]):
        there = index[0] ^ relative

        def out_tile(tile, value, there=there):
            out[there, tile] = value

        merged = {}
        for p in range(points):
            at = slice((b * points + p) * half, (b * points + p + 1) * half)
            store_packed(out_tile, packing_back, p, back[at], merged)
        store_tails(out_tile, merged)


def summed(parts):
    total = parts[0].astype(jnp.float32)
    for j in range(1, parts.shape[0]):
        total += parts[j].astype(jnp.float32)
    return total


def coeff_kernel(
    prior, parts, basis_own, basis_other, flat, coeff, *, points, steps, rank, packing
):
    f32 = jnp.float32
    total = summed(parts)
    for p in range(points):
        tiles = [total[p * packing.full + t] for t in range(packing.full)]
        tile, lane = packing.place(p)
        tiles.append(turned(total[tile], -lane))
        piece = jnp.concatenate(tiles, axis=1) * prior[:, p : p + 1]
        flat[:, p * steps : (p + 1) * steps] = piece[:, :steps]
    low = flat[...].astype(jnp.bfloat16)
    own = jnp.dot(low, basis_own[...], preferred_element_type=f32).astype(jnp.bfloat16)
    other = jnp.dot(low, basis_other[...], preferred_element_type=f32).astype(jnp.bfloat16)
    for j in range(coeff.shape[0]):
        coeff[j, :, :rank] = own
        coeff[j, :, rank:] = other


def deflate_kernel(
    core, parts_own, parts_other, deflation_own, deflation_other, flat_own, flat_other,
    basis_own, basis_other, out,
    *, points, steps, rank,
):
    f32 = jnp.float32
    bf16 = jnp.bfloat16
    own = summed(parts_own)
    other = summed(parts_other)
    half = own.shape[0]
    here = jnp.concatenate([own[:, :rank], other[:, rank:]], axis=0) * deflation_own[...]
    there = jnp.concatenate([own[:, rank:], other[:, :rank]], axis=0) * deflation_other[...]
    correction = lax.dot_general(here.astype(bf16), basis_own[...], NT, preferred_element_type=f32)
    correction += lax.dot_general(there.astype(bf16), basis_other[...], NT, preferred_element_type=f32)
    result = jnp.concatenate([flat_own[...], flat_other[...]], axis=0) - correction
    mine = core[0] * half
    for p in range(points):
        piece = result[:, p * steps : (p + 1) * steps]
        out[pl.ds(mine, half), p, :] = piece[:half]
        out[pl.ds(half - mine, half), p, :] = piece[half:]


def split_order(width):
    return list(range(width // 2)), list(range(width // 2, width))


def stage_kernel(far, near, sem):
    copy = pltpu.make_async_copy(far, near, sem)
    copy.start()
    copy.wait()


def kept(space, *values):
    return [pltpu.with_memory_space_constraint(value, space) for value in values]


def in_vmem(count):
    return [pl.BlockSpec(memory_space=pltpu.VMEM) for _ in range(count)]


def in_smem(count):
    return [pl.BlockSpec(memory_space=pltpu.SMEM) for _ in range(count)]


def limit(mib):
    return pltpu.CompilerParams(vmem_limit_bytes=mib * 1024 * 1024)


def local_split(probes, kernel, noise_weight, prior_scale, basis, deflation):
    bf16 = jnp.bfloat16
    f32 = jnp.float32
    probe_count, points, steps = probes.shape
    bins_count = steps + 1
    width = lax.axis_size("pts")
    sens = noise_weight.shape[0] // width
    half = probe_count // 2
    rank = basis.shape[1]
    wide = round_up(bins_count, LANES)
    me = jnp.full((1,), lax.axis_index("pts"), jnp.int32)
    core_index = lax.axis_index("sen")
    core = jnp.full((1,), core_index, jnp.int32)

    def swap(value):
        return lax.ppermute(value, "sen", [(0, 1), (1, 0)])

    def exchange(value):
        return lax.all_to_all(value, "pts", split_axis=0, concat_axis=0, tiled=False)

    table, weights = packed_tables(steps, wide)
    packing = Packing(3 * points, bins_count)
    packing_back = Packing(points, steps)
    sizes = dict(points=points, sens=sens, half=half, wide=wide, packing=packing)
    orders = split_order(width)
    order = orders[0] + orders[1]
    places = jnp.stack([me[0], core[0]])
    chunk = jax.ShapeDtypeStruct((packing.tiles, sens, LANES), bf16)
    in_hbm = pl.BlockSpec(memory_space=pltpu.HBM)
    sent = pl.pallas_call(
        functools.partial(pack_kernel, order=order, half=half, packing=packing),
        out_shape=(chunk,) * width,
        in_specs=in_smem(1) + [in_hbm] * 3,
        out_specs=tuple(in_vmem(width)),
        scratch_shapes=[
            pltpu.SMEM(prior_scale.shape, f32),
            pltpu.VMEM((2, points, width, sens, bins_count), bf16),
            pltpu.VMEM((half, points, steps), bf16),
            pltpu.SemaphoreType.DMA((2 + 2 * points,)),
        ],
        compiler_params=limit(8),
        name="pack",
    )(places, *kept(pltpu.HBM, prior_scale, kernel.reshape(2, points, width, sens, bins_count), probes))
    blocks = {}
    others = {}
    for relative, value in zip(order, sent):
        if relative:
            value = lax.ppermute(value, "pts", [(i, i ^ relative) for i in range(width)])
        blocks[relative] = value
        others[relative] = swap(value)
    noise_other = swap(noise_weight)
    deflation_other = swap(deflation)
    basis_other = swap(basis)

    def scratch(count):
        return [
            pltpu.VMEM((3, count * points * half, wide), f32),
            pltpu.VMEM((count * points * half, wide), f32),
        ]

    def ready(part):
        return [blocks[r] for r in part] + [others[r] for r in part]

    table = pl.pallas_call(
        stage_kernel,
        out_shape=pltpu.VMEM(table.shape, bf16),
        in_specs=[in_hbm],
        out_specs=in_vmem(1)[0],
        scratch_shapes=[pltpu.SemaphoreType.DMA],
        compiler_params=limit(2),
        name="stage",
    )(*kept(pltpu.HBM, table))
    count = len(orders[0])
    kern_first, data_first = pl.pallas_call(
        functools.partial(first_kernel, count=count, **sizes),
        out_shape=(
            jax.ShapeDtypeStruct((3, count * points, 2 * sens, wide), f32),
            jax.ShapeDtypeStruct((2 * sens * half, 2 * wide), f32),
        ),
        in_specs=in_vmem(1 + 2 * count),
        out_specs=tuple(in_vmem(2)),
        scratch_shapes=scratch(count),
        compiler_params=limit(12),
        name="first",
    )(table, *ready(orders[0]))
    count = len(orders[1])
    back = pl.pallas_call(
        functools.partial(bins_kernel, orders=orders, packing_back=packing_back, **sizes),
        out_shape=jax.ShapeDtypeStruct((width, packing_back.tiles, half, LANES), bf16),
        in_specs=in_smem(1) + [in_hbm] * 2 + in_vmem(4 + 2 * count),
        out_specs=in_vmem(1)[0],
        scratch_shapes=[pltpu.VMEM((3, count * points, 2 * sens, wide), f32)]
        + scratch(count)
        + [
            pltpu.VMEM((2 * sens * half, 2 * wide), f32),
            pltpu.VMEM((3, 2 * sens * half, wide), f32),
            pltpu.VMEM((width * points * half, 2 * wide), f32),
            pltpu.SMEM(noise_weight.shape, f32),
            pltpu.SMEM(noise_weight.shape, f32),
            pltpu.SemaphoreType.DMA((2,)),
        ],
        compiler_params=limit(20),
        name="bins",
    )(
        me, *kept(pltpu.HBM, noise_weight, noise_other), table, weights, kern_first, data_first,
        *ready(orders[1]),
    )
    back, basis_other, deflation_other = lax.optimization_barrier(
        (back, basis_other, deflation_other)
    )
    basis, basis_other = kept(pltpu.VMEM, basis, basis_other)
    parts = exchange(back)
    flat, coeff = pl.pallas_call(
        functools.partial(coeff_kernel, points=points, steps=steps, rank=rank, packing=packing_back),
        out_shape=(
            jax.ShapeDtypeStruct((half, points * steps), f32),
            jax.ShapeDtypeStruct((width, half, 2 * rank), bf16),
        ),
        in_specs=in_vmem(4),
        out_specs=tuple(in_vmem(2)),
        compiler_params=limit(12),
        name="coeff",
    )(prior_scale[None, :], parts, basis, basis_other)
    flat_other = swap(flat)
    coeff_parts = exchange(coeff)
    coeff_other = swap(coeff_parts)
    return pl.pallas_call(
        functools.partial(deflate_kernel, points=points, steps=steps, rank=rank),
        out_shape=jax.ShapeDtypeStruct((probe_count, points, steps), f32),
        in_specs=in_smem(1) + in_vmem(8),
        out_specs=in_vmem(1)[0],
        compiler_params=limit(12),
        name="deflate",
    )(
        core, coeff_parts, coeff_other, deflation[None, :], deflation_other[None, :],
        flat, flat_other, basis, basis_other,
    )


def solution(mesh):
    placed = (
        P(None, ("grp", "pts"), None),
        P(None, ("grp", "pts"), "sen", None),
        P(("grp", "sen")),
        P("pts"),
        P("pts", "sen"),
        P("sen"),
    )

    def body(*args):
        width = mesh.shape["pts"]
        split = mesh.shape["sen"] == 2 and width == ROWS
        whole_tiles = args[2].shape[0] == width * ROWS and args[0].shape[0] == 2 * ROWS
        if not (split and whole_tiles):
            return local(*args)
        return local_split(*args)

    return jax.shard_map(
        body, mesh=mesh, in_specs=placed, out_specs=P(None, ("grp", "pts"), None), check_vma=False
    )
```

```python
import functools
import math

import jax
import jax.numpy as jnp
import numpy as np
from jax import lax
from jax.experimental import pallas as pl
from jax.experimental.pallas import tpu as pltpu
from jax.sharding import PartitionSpec as P

LANES = 128
ROWS = 8


def tables(steps_count):
    bins_count = steps_count + 1
    turns = (
        jnp.arange(steps_count, dtype=jnp.int32)[:, None]
        * jnp.arange(bins_count, dtype=jnp.int32)[None, :]
        % (2 * steps_count)
    )
    angle = turns.astype(jnp.float32) * (math.pi / steps_count)
    cosine = jnp.cos(angle)
    sine = jnp.sin(angle)
    freq = jnp.arange(bins_count, dtype=jnp.int32)
    edge = (freq == 0) | (freq == steps_count)
    weights = jnp.where(edge, 1.0, 2.0).astype(jnp.float32) / (2.0 * steps_count)
    forward = jnp.concatenate([cosine, -sine], axis=1)
    inverse = jnp.concatenate([cosine * weights[None, :], -sine * weights[None, :]], axis=1)
    return (forward, inverse)


def widened(value):
    return lax.optimization_barrier(value).astype(jnp.float32)


def complex_data(spec_real, spec_imag, kern_real, kern_imag):
    data_real = jnp.einsum(
        "kpf,psf->ksf", spec_real, kern_real, preferred_element_type=jnp.float32
    ) - jnp.einsum("kpf,psf->ksf", spec_imag, kern_imag, preferred_element_type=jnp.float32)
    data_imag = jnp.einsum(
        "kpf,psf->ksf", spec_real, kern_imag, preferred_element_type=jnp.float32
    ) + jnp.einsum("kpf,psf->ksf", spec_imag, kern_real, preferred_element_type=jnp.float32)
    return (data_real, data_imag)


def complex_adjoint(weight_real, weight_imag, kern_real, kern_imag):
    adj_real = jnp.einsum(
        "ksf,psf->kpf", weight_real, kern_real, preferred_element_type=jnp.float32
    ) + jnp.einsum("ksf,psf->kpf", weight_imag, kern_imag, preferred_element_type=jnp.float32)
    adj_imag = jnp.einsum(
        "ksf,psf->kpf", weight_imag, kern_real, preferred_element_type=jnp.float32
    ) - jnp.einsum("ksf,psf->kpf", weight_real, kern_imag, preferred_element_type=jnp.float32)
    return (adj_real, adj_imag)


def local(probes, kernel, noise_weight, prior_scale, basis, deflation):
    highest = lax.Precision.HIGHEST
    probe_count, point_count, steps_count = probes.shape
    bins_count = steps_count + 1
    sensor_count = noise_weight.shape[0]
    forward, inverse = tables(steps_count)
    scaled = probes.astype(jnp.float32) * prior_scale[None, :, None]
    spectrum = jnp.dot(scaled, forward, precision=highest).astype(jnp.bfloat16)
    noise_rows = jnp.tile(noise_weight, probe_count)
    width = lax.axis_size("pts")
    block = (bins_count + width - 1) // width
    extra = block * width - bins_count
    kern_pad = jnp.pad(kernel, ((0, 0), (0, 0), (0, 0), (0, extra)))
    spec_pad = jnp.pad(
        spectrum.reshape(probe_count, point_count, 2, bins_count),
        ((0, 0), (0, 0), (0, 0), (0, extra)),
    )
    kern_bins, spec_bins = (
        lax.all_to_all(kern_pad, "pts", split_axis=3, concat_axis=1, tiled=True),
        lax.all_to_all(spec_pad, "pts", split_axis=3, concat_axis=1, tiled=True),
    )
    bin_kern_real = kern_bins[0]
    bin_kern_imag = kern_bins[1]
    data_real, data_imag = complex_data(
        spec_bins[:, :, 0], spec_bins[:, :, 1], bin_kern_real, bin_kern_imag
    )
    data_bins = jnp.stack([data_real, data_imag], axis=2).reshape(
        probe_count * sensor_count, 2, block
    )
    rows_time = lax.all_to_all(
        data_bins.astype(jnp.bfloat16), "pts", split_axis=0, concat_axis=2, tiled=True
    ).astype(data_bins.dtype)
    local_rows = rows_time.shape[0]
    begin = lax.axis_index("pts") * local_rows
    local_noise = lax.dynamic_slice_in_dim(noise_rows, begin, local_rows)
    data_rows = rows_time[:, :, :bins_count].reshape(local_rows, 2 * bins_count)
    observed = jnp.dot(data_rows, inverse.T, precision=highest)
    residual = (observed * local_noise[:, None]).astype(jnp.bfloat16)
    weighted_local = (
        jnp.dot(widened(residual), inverse, precision=highest)
        .astype(jnp.bfloat16)
        .reshape(local_rows, 2, bins_count)
    )
    weighted_pad = jnp.pad(weighted_local, ((0, 0), (0, 0), (0, extra)))
    weighted_bins = lax.all_to_all(weighted_pad, "pts", split_axis=2, concat_axis=0, tiled=True)
    weighted_bins = weighted_bins.reshape(probe_count, sensor_count, 2, block)
    adj_real, adj_imag = complex_adjoint(
        weighted_bins[:, :, 0], weighted_bins[:, :, 1], bin_kern_real, bin_kern_imag
    )
    adj_bins = jnp.stack([adj_real, adj_imag], axis=2)
    adj_points = lax.all_to_all(
        adj_bins.astype(jnp.bfloat16), "pts", split_axis=1, concat_axis=3, tiled=True
    ).astype(adj_bins.dtype)
    adjoint = adj_points[..., :bins_count].reshape(probe_count, point_count, 2 * bins_count)
    back = jnp.dot(adjoint, forward.T, precision=highest)
    back = lax.psum(back.astype(jnp.bfloat16), "sen").astype(jnp.float32)
    hessian = back * prior_scale[None, :, None]
    flat = hessian.reshape(probe_count, point_count * steps_count)
    flat_low = flat.astype(jnp.bfloat16)
    coeff = jnp.dot(flat_low, basis, preferred_element_type=jnp.float32)
    coeff = lax.psum(coeff, "pts")
    shrunk = (coeff * deflation[None, :]).astype(jnp.bfloat16)
    correction = lax.dot_general(
        shrunk, basis, (((1,), (1,)), ((), ())), preferred_element_type=jnp.float32
    )
    correction = lax.psum(correction.astype(jnp.bfloat16), "sen").astype(jnp.float32)
    return (flat - correction).reshape(probe_count, point_count, steps_count)


def round_up(value, step):
    return (value + step - 1) // step * step


def packed_tables(steps_count, wide):
    bins_count = steps_count + 1
    turns = np.arange(steps_count)[:, None] * np.arange(bins_count)[None, :] % (2 * steps_count)
    angle = turns.astype(np.float64) * (math.pi / steps_count)
    table = np.zeros((wide, 2 * wide), np.float32)
    table[:steps_count, :bins_count] = np.cos(angle)
    table[:steps_count, wide : wide + bins_count] = -np.sin(angle)
    weights = np.zeros((1, wide), np.float32)
    weights[0, :bins_count] = 2.0 / (2.0 * steps_count)
    weights[0, 0] = weights[0, steps_count] = 1.0 / (2.0 * steps_count)
    return jnp.asarray(table.astype(jnp.bfloat16)), jnp.asarray(weights)


NT = (((1,), (1,)), ((), ()))


class Packing:
    def __init__(self, rows, length):
        self.full = length // LANES
        self.tail = length % LANES
        self.slots = LANES // self.tail
        self.first_tail = rows * self.full
        self.tiles = self.first_tail + -(-rows // self.slots)

    def place(self, row):
        return self.first_tail + row // self.slots, row % self.slots * self.tail


def turned(tile, lanes):
    lanes = lanes % LANES
    return pltpu.roll(tile, lanes, axis=tile.ndim - 1) if lanes else tile


def add_tail(packing, row, value, merged):
    tile, lane = packing.place(row)
    tail = value[..., packing.full * LANES : (packing.full + 1) * LANES]
    where = lax.broadcasted_iota(jnp.int32, tail.shape, tail.ndim - 1)
    tail = turned(jnp.where(where < packing.tail, tail, 0.0), lane)
    merged[tile] = merged[tile] + tail if tile in merged else tail


def store_packed(out_tile, packing, row, value, merged):
    for t in range(packing.full):
        lanes = slice(t * LANES, (t + 1) * LANES)
        out_tile(row * packing.full + t, value[..., lanes].astype(jnp.bfloat16))
    add_tail(packing, row, value, merged)


def store_tails(out_tile, merged):
    for tile, value in merged.items():
        out_tile(tile, value.astype(jnp.bfloat16))


def pack_kernel(index, prior_far, kernel, probes, *refs, order, half, packing):
    outs = refs[: len(order)]
    prior, kernel_here, probes_here, sems = refs[len(order) :]
    f32 = jnp.float32
    _, points, _ = probes_here.shape
    edge = packing.full * LANES
    me = index[0]
    mine = pl.multiple_of(index[1] * half, half)
    copies = [
        pltpu.make_async_copy(probes.at[pl.ds(mine, half)], probes_here, sems.at[0]),
        pltpu.make_async_copy(prior_far, prior, sems.at[1]),
    ]
    for row in range(2 * points):
        at = (row // points, row % points)
        copies.append(pltpu.make_async_copy(kernel.at[at], kernel_here.at[at], sems.at[2 + row]))
    for copy in copies:
        copy.start()

    def padded(value):
        missing = jnp.zeros((value.shape[0], edge + LANES - value.shape[1]), f32)
        return jnp.concatenate([value, missing], axis=1)

    copies[0].wait()
    copies[1].wait()
    scaled = probes_here[...].astype(f32)
    tiles = {}
    tails = {}
    for p in range(points):
        store_packed(tiles.__setitem__, packing, 2 * points + p, padded(scaled[:, p, :] * prior[p]), tails)
    for copy in copies[2:]:
        copy.wait()
    for relative, out in zip(order, outs):

        def out_tile(tile, value, out=out):
            out[tile] = value

        merged = dict(tails)
        for tile, value in tiles.items():
            out_tile(tile, value)
        for row in range(2 * points):
            value = padded(kernel_here[row // points, row % points, me ^ relative].astype(f32))
            store_packed(out_tile, packing, row, value, merged)
        store_tails(out_tile, merged)


def unpack(source, row, packing):
    f32 = jnp.float32
    tiles = [source[row * packing.full + t].astype(f32) for t in range(packing.full)]
    tile, lane = packing.place(row)
    tiles.append(turned(source[tile].astype(f32), -lane))
    return tiles


def widen(sources, kern, *, packing, points, sens):
    for b, pair in enumerate(sources):
        for half, source in enumerate(pair):
            at = slice(half * sens, (half + 1) * sens)
            for p in range(points):
                real = unpack(source, p, packing)
                imag = unpack(source, points + p, packing)
                for t, (x, y) in enumerate(zip(real, imag)):
                    lanes = slice(t * LANES, (t + 1) * LANES)
                    kern[0, b * points + p, at, lanes] = x
                    kern[1, b * points + p, at, lanes] = x + y
                    kern[2, b * points + p, at, lanes] = x - y


def spectra(sources, table, spec, rows, *, packing, points, half, wide):
    for b, (own, _) in enumerate(sources):
        for p in range(points):
            at = slice((b * points + p) * half, (b * points + p + 1) * half)
            for t, tile in enumerate(unpack(own, 2 * points + p, packing)):
                rows[at, t * LANES : (t + 1) * LANES] = tile
    got = jnp.dot(rows[...].astype(jnp.bfloat16), table[...], preferred_element_type=jnp.float32)
    real = got[:, :wide]
    imag = got[:, wide:]
    spec[0] = real + imag
    spec[1] = imag
    spec[2] = real


def forward_sum(kern, spec, data, earlier, *, points, sens, half, wide):
    f32 = jnp.float32
    blocks = kern.shape[1] // points

    def tile_step(ft, carry):
        lanes = pl.ds(pl.multiple_of(ft * LANES, LANES), LANES)
        shifted = pl.ds(pl.multiple_of(wide + ft * LANES, LANES), LANES)
        for first in range(0, 2 * sens, sens):

            def source(b, acc, first=first):
                acc = list(acc)
                for p in range(points):
                    q = b * points + p
                    at = pl.ds(pl.multiple_of(q * half, ROWS), half)
                    both = spec[0, at, lanes]
                    imag = spec[1, at, lanes]
                    real = spec[2, at, lanes]
                    for s in range(sens):
                        row = slice(first + s, first + s + 1)
                        acc[3 * s] += kern[0, q, row, lanes] * both
                        acc[3 * s + 1] += kern[1, q, row, lanes] * imag
                        acc[3 * s + 2] += kern[2, q, row, lanes] * real
                return tuple(acc)

            zero = jnp.zeros((half, LANES), f32)
            acc = lax.fori_loop(0, blocks, source, (zero,) * (3 * sens))
            for s in range(sens):
                at = slice((first + s) * half, (first + s + 1) * half)
                real = acc[3 * s] - acc[3 * s + 1]
                imag = acc[3 * s] - acc[3 * s + 2]
                if earlier is not None:
                    real += earlier[at, lanes]
                    imag += earlier[at, shifted]
                data[at, lanes] = real
                data[at, shifted] = imag
        return carry

    lax.fori_loop(0, wide // LANES, tile_step, 0)


def paired(refs, count):
    return list(zip(refs[:count], refs[count : 2 * count]))


def first_kernel(table, *refs, count, points, sens, half, wide, packing):
    sources = paired(refs, count)
    kern, data, spec, rows = refs[2 * count :]
    spectra(sources, table, spec, rows, packing=packing, points=points, half=half, wide=wide)
    widen(sources, kern, packing=packing, points=points, sens=sens)
    forward_sum(kern, spec, data, None, points=points, sens=sens, half=half, wide=wide)


def bins_kernel(
    index, noise_far, noise_other_far, table, weights, kern_first, data_first, *refs,
    orders, points, sens, half, wide, packing, packing_back,
):
    count = len(orders[1])
    sources = paired(refs, count)
    out, kern, spec, rows, data, wdata, adjoint, noise_own, noise_other, sems = refs[2 * count :]
    copies = [
        pltpu.make_async_copy(noise_far, noise_own, sems.at[0]),
        pltpu.make_async_copy(noise_other_far, noise_other, sems.at[1]),
    ]
    for copy in copies:
        copy.start()
    tiles = wide // LANES
    f32 = jnp.float32
    bf16 = jnp.bfloat16
    spectra(sources, table, spec, rows, packing=packing, points=points, half=half, wide=wide)
    widen(sources, kern, packing=packing, points=points, sens=sens)
    forward_sum(kern, spec, data, data_first, points=points, sens=sens, half=half, wide=wide)
    table_v = table[...]
    weight_rows = weights[...]
    scaled = jnp.concatenate(
        [data[:, :wide] * weight_rows, data[:, wide:] * weight_rows], axis=1
    ).astype(bf16)
    observed = lax.dot_general(scaled, table_v, NT, preferred_element_type=f32)
    for copy in copies:
        copy.wait()
    mine = index[0] * sens
    scales = [noise_own[mine + s] for s in range(sens)]
    scales += [noise_other[mine + s] for s in range(sens)]
    residual = jnp.concatenate(
        [observed[s * half : (s + 1) * half] * scale for s, scale in enumerate(scales)], axis=0
    ).astype(bf16)
    weighted = jnp.dot(residual, table_v, preferred_element_type=f32)
    real = weighted[:, :wide] * weight_rows
    imag = weighted[:, wide:] * weight_rows
    wdata[0] = real + imag
    wdata[1] = imag
    wdata[2] = real

    base = 0
    group = 2 * points
    for source, order in ((kern_first, orders[0]), (kern, orders[1])):

        def adjoint_tile(step, carry, source=source, base=base):
            first = step // tiles * group
            ft = step % tiles
            lanes = pl.ds(pl.multiple_of(ft * LANES, LANES), LANES)
            shifted = pl.ds(pl.multiple_of(wide + ft * LANES, LANES), LANES)
            zero = jnp.zeros((half, LANES), f32)
            acc = [zero] * (3 * group)
            for s in range(2 * sens):
                at = slice(s * half, (s + 1) * half)
                both = wdata[0, at, lanes]
                imag = wdata[1, at, lanes]
                real = wdata[2, at, lanes]
                row = slice(s, s + 1)
                for p in range(group):
                    acc[3 * p] += source[0, first + p, row, lanes] * both
                    acc[3 * p + 1] += source[2, first + p, row, lanes] * imag
                    acc[3 * p + 2] += source[1, first + p, row, lanes] * real
            for p in range(group):
                at = pl.ds(pl.multiple_of((base + first + p) * half, ROWS), half)
                adjoint[at, lanes] = acc[3 * p] - acc[3 * p + 1]
                adjoint[at, shifted] = acc[3 * p] - acc[3 * p + 2]
            return carry

        lax.fori_loop(0, len(order) * points // group * tiles, adjoint_tile, 0)
        base += len(order) * points
    back = lax.dot_general(adjoint[...].astype(bf16), table_v, NT, preferred_element_type=f32)
    for b, relative in enumerate(orders[0] + orders[1]):
        there = index[0] ^ relative

        def out_tile(tile, value, there=there):
            out[there, tile] = value

        merged = {}
        for p in range(points):
            at = slice((b * points + p) * half, (b * points + p + 1) * half)
            store_packed(out_tile, packing_back, p, back[at], merged)
        store_tails(out_tile, merged)


def summed(parts):
    total = parts[0].astype(jnp.float32)
    for j in range(1, parts.shape[0]):
        total += parts[j].astype(jnp.float32)
    return total


def coeff_kernel(
    prior, parts, basis_own, basis_other, flat, coeff, *, points, steps, rank, packing
):
    f32 = jnp.float32
    total = summed(parts)
    for p in range(points):
        tiles = [total[p * packing.full + t] for t in range(packing.full)]
        tile, lane = packing.place(p)
        tiles.append(turned(total[tile], -lane))
        piece = jnp.concatenate(tiles, axis=1) * prior[:, p : p + 1]
        flat[:, p * steps : (p + 1) * steps] = piece[:, :steps]
    low = flat[...].astype(jnp.bfloat16)
    own = jnp.dot(low, basis_own[...], preferred_element_type=f32).astype(jnp.bfloat16)
    other = jnp.dot(low, basis_other[...], preferred_element_type=f32).astype(jnp.bfloat16)
    for j in range(coeff.shape[0]):
        coeff[j, :, :rank] = own
        coeff[j, :, rank:] = other


def deflate_kernel(
    core, parts_own, parts_other, deflation_own, deflation_other, flat_own, flat_other,
    basis_own, basis_other, out,
    *, points, steps, rank,
):
    f32 = jnp.float32
    bf16 = jnp.bfloat16
    own = summed(parts_own)
    other = summed(parts_other)
    half = own.shape[0]
    here = jnp.concatenate([own[:, :rank], other[:, rank:]], axis=0) * deflation_own[...]
    there = jnp.concatenate([own[:, rank:], other[:, :rank]], axis=0) * deflation_other[...]
    correction = lax.dot_general(here.astype(bf16), basis_own[...], NT, preferred_element_type=f32)
    correction += lax.dot_general(there.astype(bf16), basis_other[...], NT, preferred_element_type=f32)
    result = jnp.concatenate([flat_own[...], flat_other[...]], axis=0) - correction
    mine = core[0] * half
    for p in range(points):
        piece = result[:, p * steps : (p + 1) * steps]
        out[pl.ds(mine, half), p, :] = piece[:half]
        out[pl.ds(half - mine, half), p, :] = piece[half:]


def split_order(width):
    near = list(range(2, width // 2))
    far = list(range(width // 2, width))
    return [0, far[0]] + near, far[1:] + [1]


def stage_kernel(far, near, sem):
    copy = pltpu.make_async_copy(far, near, sem)
    copy.start()
    copy.wait()


def kept(space, *values):
    return [pltpu.with_memory_space_constraint(value, space) for value in values]


def in_vmem(count):
    return [pl.BlockSpec(memory_space=pltpu.VMEM) for _ in range(count)]


def in_smem(count):
    return [pl.BlockSpec(memory_space=pltpu.SMEM) for _ in range(count)]


def limit(mib):
    return pltpu.CompilerParams(vmem_limit_bytes=mib * 1024 * 1024)


def local_split(probes, kernel, noise_weight, prior_scale, basis, deflation):
    bf16 = jnp.bfloat16
    f32 = jnp.float32
    probe_count, points, steps = probes.shape
    bins_count = steps + 1
    width = lax.axis_size("pts")
    sens = noise_weight.shape[0] // width
    half = probe_count // 2
    rank = basis.shape[1]
    wide = round_up(bins_count, LANES)
    me = jnp.full((1,), lax.axis_index("pts"), jnp.int32)
    core_index = lax.axis_index("sen")
    core = jnp.full((1,), core_index, jnp.int32)

    def swap(value):
        return lax.ppermute(value, "sen", [(0, 1), (1, 0)])

    def exchange(value):
        return lax.all_to_all(value, "pts", split_axis=0, concat_axis=0, tiled=False)

    table, weights = packed_tables(steps, wide)
    packing = Packing(3 * points, bins_count)
    packing_back = Packing(points, steps)
    sizes = dict(points=points, sens=sens, half=half, wide=wide, packing=packing)
    orders = split_order(width)
    order = orders[0] + orders[1]
    places = jnp.stack([me[0], core[0]])
    chunk = jax.ShapeDtypeStruct((packing.tiles, sens, LANES), bf16)
    in_hbm = pl.BlockSpec(memory_space=pltpu.HBM)
    sent = pl.pallas_call(
        functools.partial(pack_kernel, order=order, half=half, packing=packing),
        out_shape=(chunk,) * width,
        in_specs=in_smem(1) + [in_hbm] * 3,
        out_specs=tuple(in_vmem(width)),
        scratch_shapes=[
            pltpu.SMEM(prior_scale.shape, f32),
            pltpu.VMEM((2, points, width, sens, bins_count), bf16),
            pltpu.VMEM((half, points, steps), bf16),
            pltpu.SemaphoreType.DMA((2 + 2 * points,)),
        ],
        compiler_params=limit(8),
        name="pack",
    )(places, *kept(pltpu.HBM, prior_scale, kernel.reshape(2, points, width, sens, bins_count), probes))
    blocks = {}
    others = {}
    for relative, value in zip(order, sent):
        if relative:
            value = lax.ppermute(value, "pts", [(i, i ^ relative) for i in range(width)])
        blocks[relative] = value
        others[relative] = swap(value)
    noise_other = swap(noise_weight)
    deflation_other = swap(deflation)
    basis_other = swap(basis)

    def scratch(count):
        return [
            pltpu.VMEM((3, count * points * half, wide), f32),
            pltpu.VMEM((count * points * half, wide), f32),
        ]

    def ready(part):
        return [blocks[r] for r in part] + [others[r] for r in part]

    table = pl.pallas_call(
        stage_kernel,
        out_shape=pltpu.VMEM(table.shape, bf16),
        in_specs=[in_hbm],
        out_specs=in_vmem(1)[0],
        scratch_shapes=[pltpu.SemaphoreType.DMA],
        compiler_params=limit(2),
        name="stage",
    )(*kept(pltpu.HBM, table))
    count = len(orders[0])
    kern_first, data_first = pl.pallas_call(
        functools.partial(first_kernel, count=count, **sizes),
        out_shape=(
            jax.ShapeDtypeStruct((3, count * points, 2 * sens, wide), f32),
            jax.ShapeDtypeStruct((2 * sens * half, 2 * wide), f32),
        ),
        in_specs=in_vmem(1 + 2 * count),
        out_specs=tuple(in_vmem(2)),
        scratch_shapes=scratch(count),
        compiler_params=limit(12),
        name="first",
    )(table, *ready(orders[0]))
    count = len(orders[1])
    back = pl.pallas_call(
        functools.partial(bins_kernel, orders=orders, packing_back=packing_back, **sizes),
        out_shape=jax.ShapeDtypeStruct((width, packing_back.tiles, half, LANES), bf16),
        in_specs=in_smem(1) + [in_hbm] + in_vmem(5 + 2 * count),
        out_specs=in_vmem(1)[0],
        scratch_shapes=[pltpu.VMEM((3, count * points, 2 * sens, wide), f32)]
        + scratch(count)
        + [
            pltpu.VMEM((2 * sens * half, 2 * wide), f32),
            pltpu.VMEM((3, 2 * sens * half, wide), f32),
            pltpu.VMEM((width * points * half, 2 * wide), f32),
            pltpu.SMEM(noise_weight.shape, f32),
            pltpu.SMEM(noise_weight.shape, f32),
            pltpu.SemaphoreType.DMA((2,)),
        ],
        compiler_params=limit(20),
        name="bins",
    )(
        me, *kept(pltpu.HBM, noise_weight), noise_other, table, weights, kern_first, data_first,
        *ready(orders[1]),
    )
    back, basis_other, deflation_other = lax.optimization_barrier(
        (back, basis_other, deflation_other)
    )
    basis, basis_other = kept(pltpu.VMEM, basis, basis_other)
    parts = exchange(back)
    flat, coeff = pl.pallas_call(
        functools.partial(coeff_kernel, points=points, steps=steps, rank=rank, packing=packing_back),
        out_shape=(
            jax.ShapeDtypeStruct((half, points * steps), f32),
            jax.ShapeDtypeStruct((width, half, 2 * rank), bf16),
        ),
        in_specs=in_vmem(4),
        out_specs=tuple(in_vmem(2)),
        compiler_params=limit(12),
        name="coeff",
    )(prior_scale[None, :], parts, basis, basis_other)
    flat_other = swap(flat)
    coeff_parts = exchange(coeff)
    coeff_other = swap(coeff_parts)
    return pl.pallas_call(
        functools.partial(deflate_kernel, points=points, steps=steps, rank=rank),
        out_shape=jax.ShapeDtypeStruct((probe_count, points, steps), f32),
        in_specs=in_smem(1) + in_vmem(8),
        out_specs=in_vmem(1)[0],
        compiler_params=limit(12),
        name="deflate",
    )(
        core, coeff_parts, coeff_other, deflation[None, :], deflation_other[None, :],
        flat, flat_other, basis, basis_other,
    )


def solution(mesh):
    placed = (
        P(None, ("grp", "pts"), None),
        P(None, ("grp", "pts"), "sen", None),
        P(("grp", "sen")),
        P("pts"),
        P("pts", "sen"),
        P("sen"),
    )

    def body(*args):
        width = mesh.shape["pts"]
        split = mesh.shape["sen"] == 2 and width == ROWS
        whole_tiles = args[2].shape[0] == width * ROWS and args[0].shape[0] == 2 * ROWS
        if not (split and whole_tiles):
            return local(*args)
        return local_split(*args)

    return jax.shard_map(
        body, mesh=mesh, in_specs=placed, out_specs=P(None, ("grp", "pts"), None), check_vma=False
    )
```

```python
import functools
import math

import jax
import jax.numpy as jnp
import numpy as np
from jax import lax
from jax.experimental import pallas as pl
from jax.experimental.pallas import tpu as pltpu
from jax.sharding import PartitionSpec as P

LANES = 128
ROWS = 8


def tables(steps_count):
    bins_count = steps_count + 1
    turns = (
        jnp.arange(steps_count, dtype=jnp.int32)[:, None]
        * jnp.arange(bins_count, dtype=jnp.int32)[None, :]
        % (2 * steps_count)
    )
    angle = turns.astype(jnp.float32) * (math.pi / steps_count)
    cosine = jnp.cos(angle)
    sine = jnp.sin(angle)
    freq = jnp.arange(bins_count, dtype=jnp.int32)
    edge = (freq == 0) | (freq == steps_count)
    weights = jnp.where(edge, 1.0, 2.0).astype(jnp.float32) / (2.0 * steps_count)
    forward = jnp.concatenate([cosine, -sine], axis=1)
    inverse = jnp.concatenate([cosine * weights[None, :], -sine * weights[None, :]], axis=1)
    return (forward, inverse)


def widened(value):
    return lax.optimization_barrier(value).astype(jnp.float32)


def complex_data(spec_real, spec_imag, kern_real, kern_imag):
    data_real = jnp.einsum(
        "kpf,psf->ksf", spec_real, kern_real, preferred_element_type=jnp.float32
    ) - jnp.einsum("kpf,psf->ksf", spec_imag, kern_imag, preferred_element_type=jnp.float32)
    data_imag = jnp.einsum(
        "kpf,psf->ksf", spec_real, kern_imag, preferred_element_type=jnp.float32
    ) + jnp.einsum("kpf,psf->ksf", spec_imag, kern_real, preferred_element_type=jnp.float32)
    return (data_real, data_imag)


def complex_adjoint(weight_real, weight_imag, kern_real, kern_imag):
    adj_real = jnp.einsum(
        "ksf,psf->kpf", weight_real, kern_real, preferred_element_type=jnp.float32
    ) + jnp.einsum("ksf,psf->kpf", weight_imag, kern_imag, preferred_element_type=jnp.float32)
    adj_imag = jnp.einsum(
        "ksf,psf->kpf", weight_imag, kern_real, preferred_element_type=jnp.float32
    ) - jnp.einsum("ksf,psf->kpf", weight_real, kern_imag, preferred_element_type=jnp.float32)
    return (adj_real, adj_imag)


def local(probes, kernel, noise_weight, prior_scale, basis, deflation):
    highest = lax.Precision.HIGHEST
    probe_count, point_count, steps_count = probes.shape
    bins_count = steps_count + 1
    sensor_count = noise_weight.shape[0]
    forward, inverse = tables(steps_count)
    scaled = probes.astype(jnp.float32) * prior_scale[None, :, None]
    spectrum = jnp.dot(scaled, forward, precision=highest).astype(jnp.bfloat16)
    noise_rows = jnp.tile(noise_weight, probe_count)
    width = lax.axis_size("pts")
    block = (bins_count + width - 1) // width
    extra = block * width - bins_count
    kern_pad = jnp.pad(kernel, ((0, 0), (0, 0), (0, 0), (0, extra)))
    spec_pad = jnp.pad(
        spectrum.reshape(probe_count, point_count, 2, bins_count),
        ((0, 0), (0, 0), (0, 0), (0, extra)),
    )
    kern_bins, spec_bins = (
        lax.all_to_all(kern_pad, "pts", split_axis=3, concat_axis=1, tiled=True),
        lax.all_to_all(spec_pad, "pts", split_axis=3, concat_axis=1, tiled=True),
    )
    bin_kern_real = kern_bins[0]
    bin_kern_imag = kern_bins[1]
    data_real, data_imag = complex_data(
        spec_bins[:, :, 0], spec_bins[:, :, 1], bin_kern_real, bin_kern_imag
    )
    data_bins = jnp.stack([data_real, data_imag], axis=2).reshape(
        probe_count * sensor_count, 2, block
    )
    rows_time = lax.all_to_all(
        data_bins.astype(jnp.bfloat16), "pts", split_axis=0, concat_axis=2, tiled=True
    ).astype(data_bins.dtype)
    local_rows = rows_time.shape[0]
    begin = lax.axis_index("pts") * local_rows
    local_noise = lax.dynamic_slice_in_dim(noise_rows, begin, local_rows)
    data_rows = rows_time[:, :, :bins_count].reshape(local_rows, 2 * bins_count)
    observed = jnp.dot(data_rows, inverse.T, precision=highest)
    residual = (observed * local_noise[:, None]).astype(jnp.bfloat16)
    weighted_local = (
        jnp.dot(widened(residual), inverse, precision=highest)
        .astype(jnp.bfloat16)
        .reshape(local_rows, 2, bins_count)
    )
    weighted_pad = jnp.pad(weighted_local, ((0, 0), (0, 0), (0, extra)))
    weighted_bins = lax.all_to_all(weighted_pad, "pts", split_axis=2, concat_axis=0, tiled=True)
    weighted_bins = weighted_bins.reshape(probe_count, sensor_count, 2, block)
    adj_real, adj_imag = complex_adjoint(
        weighted_bins[:, :, 0], weighted_bins[:, :, 1], bin_kern_real, bin_kern_imag
    )
    adj_bins = jnp.stack([adj_real, adj_imag], axis=2)
    adj_points = lax.all_to_all(
        adj_bins.astype(jnp.bfloat16), "pts", split_axis=1, concat_axis=3, tiled=True
    ).astype(adj_bins.dtype)
    adjoint = adj_points[..., :bins_count].reshape(probe_count, point_count, 2 * bins_count)
    back = jnp.dot(adjoint, forward.T, precision=highest)
    back = lax.psum(back.astype(jnp.bfloat16), "sen").astype(jnp.float32)
    hessian = back * prior_scale[None, :, None]
    flat = hessian.reshape(probe_count, point_count * steps_count)
    flat_low = flat.astype(jnp.bfloat16)
    coeff = jnp.dot(flat_low, basis, preferred_element_type=jnp.float32)
    coeff = lax.psum(coeff, "pts")
    shrunk = (coeff * deflation[None, :]).astype(jnp.bfloat16)
    correction = lax.dot_general(
        shrunk, basis, (((1,), (1,)), ((), ())), preferred_element_type=jnp.float32
    )
    correction = lax.psum(correction.astype(jnp.bfloat16), "sen").astype(jnp.float32)
    return (flat - correction).reshape(probe_count, point_count, steps_count)


def round_up(value, step):
    return (value + step - 1) // step * step


def packed_tables(steps_count, wide):
    bins_count = steps_count + 1
    turns = np.arange(steps_count)[:, None] * np.arange(bins_count)[None, :] % (2 * steps_count)
    angle = turns.astype(np.float64) * (math.pi / steps_count)
    table = np.zeros((wide, 2 * wide), np.float32)
    table[:steps_count, :bins_count] = np.cos(angle)
    table[:steps_count, wide : wide + bins_count] = -np.sin(angle)
    weights = np.zeros((1, wide), np.float32)
    weights[0, :bins_count] = 2.0 / (2.0 * steps_count)
    weights[0, 0] = weights[0, steps_count] = 1.0 / (2.0 * steps_count)
    return jnp.asarray(table.astype(jnp.bfloat16)), jnp.asarray(weights)


NT = (((1,), (1,)), ((), ()))


class Packing:
    def __init__(self, rows, length):
        self.full = length // LANES
        self.tail = length % LANES
        self.slots = LANES // self.tail
        self.first_tail = rows * self.full
        self.tiles = self.first_tail + -(-rows // self.slots)

    def place(self, row):
        return self.first_tail + row // self.slots, row % self.slots * self.tail


def turned(tile, lanes):
    lanes = lanes % LANES
    return pltpu.roll(tile, lanes, axis=tile.ndim - 1) if lanes else tile


def add_tail(packing, row, value, merged):
    tile, lane = packing.place(row)
    tail = value[..., packing.full * LANES : (packing.full + 1) * LANES]
    where = lax.broadcasted_iota(jnp.int32, tail.shape, tail.ndim - 1)
    tail = turned(jnp.where(where < packing.tail, tail, 0.0), lane)
    merged[tile] = merged[tile] + tail if tile in merged else tail


def store_packed(out_tile, packing, row, value, merged):
    for t in range(packing.full):
        lanes = slice(t * LANES, (t + 1) * LANES)
        out_tile(row * packing.full + t, value[..., lanes].astype(jnp.bfloat16))
    add_tail(packing, row, value, merged)


def store_tails(out_tile, merged):
    for tile, value in merged.items():
        out_tile(tile, value.astype(jnp.bfloat16))


def pack_kernel(index, prior_far, kernel, probes, *refs, order, lean, half, packing, packing_probes):
    outs = refs[: len(order)]
    prior, kernel_here, probes_here, sems = refs[len(order) :]
    f32 = jnp.float32
    _, points, _ = probes_here.shape
    edge = packing.full * LANES
    me = index[0]
    mine = pl.multiple_of(index[1] * half, half)
    copies = [
        pltpu.make_async_copy(probes.at[pl.ds(mine, half)], probes_here, sems.at[0]),
        pltpu.make_async_copy(prior_far, prior, sems.at[1]),
    ]
    for row in range(2 * points):
        at = (row // points, row % points)
        copies.append(pltpu.make_async_copy(kernel.at[at], kernel_here.at[at], sems.at[2 + row]))
    for copy in copies:
        copy.start()

    def padded(value):
        missing = jnp.zeros((value.shape[0], edge + LANES - value.shape[1]), f32)
        return jnp.concatenate([value, missing], axis=1)

    copies[0].wait()
    copies[1].wait()
    scaled = probes_here[...].astype(f32)
    tiles = {}
    tails = {}
    for p in range(points):
        value = padded(scaled[:, p, :] * prior[p])
        store_packed(tiles.__setitem__, packing_probes, p, value, tails)
    store_tails(tiles.__setitem__, tails)
    for copy in copies[2:]:
        copy.wait()
    for relative, out in zip(order, outs):

        def out_tile(tile, value, out=out):
            out[tile] = value

        if relative not in lean:
            for tile, value in tiles.items():
                out_tile(packing.tiles + tile, value)
        merged = {}
        for row in range(2 * points):
            value = padded(kernel_here[row // points, row % points, me ^ relative].astype(f32))
            store_packed(out_tile, packing, row, value, merged)
        store_tails(out_tile, merged)


def unpack(source, row, packing, base=0):
    f32 = jnp.float32
    tiles = [source[base + row * packing.full + t].astype(f32) for t in range(packing.full)]
    tile, lane = packing.place(row)
    tiles.append(turned(source[base + tile].astype(f32), -lane))
    return tiles


def widen(sources, kern, *, packing, points, sens):
    for b, pair in enumerate(sources):
        for half, source in enumerate(pair):
            at = slice(half * sens, (half + 1) * sens)
            for p in range(points):
                real = unpack(source, p, packing)
                imag = unpack(source, points + p, packing)
                for t, (x, y) in enumerate(zip(real, imag)):
                    lanes = slice(t * LANES, (t + 1) * LANES)
                    kern[0, b * points + p, at, lanes] = x
                    kern[1, b * points + p, at, lanes] = x + y
                    kern[2, b * points + p, at, lanes] = x - y


def spectra(sources, table, spec, rows, *, packing, points, half, wide):
    for b, (source, base) in enumerate(sources):
        for p in range(points):
            at = slice((b * points + p) * half, (b * points + p + 1) * half)
            for t, tile in enumerate(unpack(source, p, packing, base)):
                rows[at, t * LANES : (t + 1) * LANES] = tile
    got = jnp.dot(rows[...].astype(jnp.bfloat16), table[...], preferred_element_type=jnp.float32)
    real = got[:, :wide]
    imag = got[:, wide:]
    spec[0] = real + imag
    spec[1] = imag
    spec[2] = real


def forward_sum(kern, spec, data, earlier, *, points, sens, half, wide):
    f32 = jnp.float32
    blocks = kern.shape[1] // points

    def tile_step(ft, carry):
        lanes = pl.ds(pl.multiple_of(ft * LANES, LANES), LANES)
        shifted = pl.ds(pl.multiple_of(wide + ft * LANES, LANES), LANES)
        for first in range(0, 2 * sens, sens):

            def source(b, acc, first=first):
                acc = list(acc)
                for p in range(points):
                    q = b * points + p
                    at = pl.ds(pl.multiple_of(q * half, ROWS), half)
                    both = spec[0, at, lanes]
                    imag = spec[1, at, lanes]
                    real = spec[2, at, lanes]
                    for s in range(sens):
                        row = slice(first + s, first + s + 1)
                        acc[3 * s] += kern[0, q, row, lanes] * both
                        acc[3 * s + 1] += kern[1, q, row, lanes] * imag
                        acc[3 * s + 2] += kern[2, q, row, lanes] * real
                return tuple(acc)

            zero = jnp.zeros((half, LANES), f32)
            acc = lax.fori_loop(0, blocks, source, (zero,) * (3 * sens))
            for s in range(sens):
                at = slice((first + s) * half, (first + s + 1) * half)
                real = acc[3 * s] - acc[3 * s + 1]
                imag = acc[3 * s] - acc[3 * s + 2]
                if earlier is not None:
                    real += earlier[at, lanes]
                    imag += earlier[at, shifted]
                data[at, lanes] = real
                data[at, shifted] = imag
        return carry

    lax.fori_loop(0, wide // LANES, tile_step, 0)


def paired(refs, count):
    return list(zip(refs[:count], refs[count : 2 * count]))


def first_kernel(table, *refs, count, points, sens, half, wide, packing, packing_probes):
    sources = paired(refs, count)
    kern, data, spec, rows = refs[2 * count :]
    probes = [(own, packing.tiles) for own, _ in sources]
    spectra(probes, table, spec, rows, packing=packing_probes, points=points, half=half, wide=wide)
    widen(sources, kern, packing=packing, points=points, sens=sens)
    forward_sum(kern, spec, data, None, points=points, sens=sens, half=half, wide=wide)


def bins_kernel(
    index, noise_far, noise_other_far, table, weights, kern_first, data_first, relayed, *refs,
    orders, lean, points, sens, half, wide, packing, packing_probes,
):
    count = len(orders[1])
    sources = paired(refs, count)
    out, kern, spec, rows, data, wdata, adjoint, noise_own, noise_other, sems = refs[2 * count :]
    copies = [
        pltpu.make_async_copy(noise_far, noise_own, sems.at[0]),
        pltpu.make_async_copy(noise_other_far, noise_other, sems.at[1]),
    ]
    for copy in copies:
        copy.start()
    tiles = wide // LANES
    f32 = jnp.float32
    bf16 = jnp.bfloat16
    probes = []
    for relative, (own, _) in zip(orders[1], sources):
        if relative in lean:
            probes.append((relayed, lean.index(relative) * packing_probes.tiles))
        else:
            probes.append((own, packing.tiles))
    spectra(probes, table, spec, rows, packing=packing_probes, points=points, half=half, wide=wide)
    widen(sources, kern, packing=packing, points=points, sens=sens)
    forward_sum(kern, spec, data, data_first, points=points, sens=sens, half=half, wide=wide)
    table_v = table[...]
    weight_rows = weights[...]
    scaled = jnp.concatenate(
        [data[:, :wide] * weight_rows, data[:, wide:] * weight_rows], axis=1
    ).astype(bf16)
    observed = lax.dot_general(scaled, table_v, NT, preferred_element_type=f32)
    for copy in copies:
        copy.wait()
    mine = index[0] * sens
    scales = [noise_own[mine + s] for s in range(sens)]
    scales += [noise_other[mine + s] for s in range(sens)]
    residual = jnp.concatenate(
        [observed[s * half : (s + 1) * half] * scale for s, scale in enumerate(scales)], axis=0
    ).astype(bf16)
    weighted = jnp.dot(residual, table_v, preferred_element_type=f32)
    real = weighted[:, :wide] * weight_rows
    imag = weighted[:, wide:] * weight_rows
    wdata[0] = real + imag
    wdata[1] = imag
    wdata[2] = real

    base = 0
    for source, order in ((kern_first, orders[0]), (kern, orders[1])):

        group = points if len(order) % 2 else 2 * points

        def adjoint_tile(step, carry, source=source, base=base, group=group):
            first = step // tiles * group
            ft = step % tiles
            lanes = pl.ds(pl.multiple_of(ft * LANES, LANES), LANES)
            shifted = pl.ds(pl.multiple_of(wide + ft * LANES, LANES), LANES)
            zero = jnp.zeros((half, LANES), f32)
            acc = [zero] * (3 * group)
            for s in range(2 * sens):
                at = slice(s * half, (s + 1) * half)
                both = wdata[0, at, lanes]
                imag = wdata[1, at, lanes]
                real = wdata[2, at, lanes]
                row = slice(s, s + 1)
                for p in range(group):
                    acc[3 * p] += source[0, first + p, row, lanes] * both
                    acc[3 * p + 1] += source[2, first + p, row, lanes] * imag
                    acc[3 * p + 2] += source[1, first + p, row, lanes] * real
            for p in range(group):
                at = pl.ds(pl.multiple_of((base + first + p) * half, ROWS), half)
                adjoint[at, lanes] = acc[3 * p] - acc[3 * p + 1]
                adjoint[at, shifted] = acc[3 * p] - acc[3 * p + 2]
            return carry

        lax.fori_loop(0, len(order) * points // group * tiles, adjoint_tile, 0)
        base += len(order) * points
    back = lax.dot_general(adjoint[...].astype(bf16), table_v, NT, preferred_element_type=f32)
    for b, relative in enumerate(orders[0] + orders[1]):
        there = index[0] ^ relative

        def out_tile(tile, value, there=there):
            out[there, tile] = value

        merged = {}
        for p in range(points):
            at = slice((b * points + p) * half, (b * points + p + 1) * half)
            store_packed(out_tile, packing_probes, p, back[at], merged)
        store_tails(out_tile, merged)


def summed(parts):
    total = parts[0].astype(jnp.float32)
    for j in range(1, parts.shape[0]):
        total += parts[j].astype(jnp.float32)
    return total


def coeff_kernel(
    prior, parts, basis_own, basis_other, flat, coeff, *, points, steps, rank, packing
):
    f32 = jnp.float32
    total = summed(parts)
    for p in range(points):
        tiles = [total[p * packing.full + t] for t in range(packing.full)]
        tile, lane = packing.place(p)
        tiles.append(turned(total[tile], -lane))
        piece = jnp.concatenate(tiles, axis=1) * prior[:, p : p + 1]
        flat[:, p * steps : (p + 1) * steps] = piece[:, :steps]
    low = flat[...].astype(jnp.bfloat16)
    own = jnp.dot(low, basis_own[...], preferred_element_type=f32).astype(jnp.bfloat16)
    other = jnp.dot(low, basis_other[...], preferred_element_type=f32).astype(jnp.bfloat16)
    for j in range(coeff.shape[0]):
        coeff[j, :, :rank] = own
        coeff[j, :, rank:] = other


def deflate_kernel(
    core, parts_own, parts_other, deflation_own, deflation_other, flat_own, flat_other,
    basis_own, basis_other, out,
    *, points, steps, rank,
):
    f32 = jnp.float32
    bf16 = jnp.bfloat16
    own = summed(parts_own)
    other = summed(parts_other)
    half = own.shape[0]
    here = jnp.concatenate([own[:, :rank], other[:, rank:]], axis=0) * deflation_own[...]
    there = jnp.concatenate([own[:, rank:], other[:, :rank]], axis=0) * deflation_other[...]
    correction = lax.dot_general(here.astype(bf16), basis_own[...], NT, preferred_element_type=f32)
    correction += lax.dot_general(there.astype(bf16), basis_other[...], NT, preferred_element_type=f32)
    result = jnp.concatenate([flat_own[...], flat_other[...]], axis=0) - correction
    mine = core[0] * half
    for p in range(points):
        piece = result[:, p * steps : (p + 1) * steps]
        out[pl.ds(mine, half), p, :] = piece[:half]
        out[pl.ds(half - mine, half), p, :] = piece[half:]


def split_order(width):
    near = list(range(2, width // 2))
    far = list(range(width // 2, width))
    return [0] + [r for r in far if r % 2 == 0] + near, [r for r in far if r % 2] + [1]


def lean_partners(width):
    return [r for r in range(width // 2, width) if r % 2]


def relay_kernel(*refs, first_tile):
    sources, out = refs[:-1], refs[-1]
    count = out.shape[0] // len(sources)
    for n, source in enumerate(sources):
        out[n * count : (n + 1) * count] = source[first_tile:]


def stage_kernel(far, near, sem):
    copy = pltpu.make_async_copy(far, near, sem)
    copy.start()
    copy.wait()


def kept(space, *values):
    return [pltpu.with_memory_space_constraint(value, space) for value in values]


def in_vmem(count):
    return [pl.BlockSpec(memory_space=pltpu.VMEM) for _ in range(count)]


def in_smem(count):
    return [pl.BlockSpec(memory_space=pltpu.SMEM) for _ in range(count)]


def limit(mib):
    return pltpu.CompilerParams(vmem_limit_bytes=mib * 1024 * 1024)


def local_split(probes, kernel, noise_weight, prior_scale, basis, deflation):
    bf16 = jnp.bfloat16
    f32 = jnp.float32
    probe_count, points, steps = probes.shape
    bins_count = steps + 1
    width = lax.axis_size("pts")
    sens = noise_weight.shape[0] // width
    half = probe_count // 2
    rank = basis.shape[1]
    wide = round_up(bins_count, LANES)
    me = jnp.full((1,), lax.axis_index("pts"), jnp.int32)
    core_index = lax.axis_index("sen")
    core = jnp.full((1,), core_index, jnp.int32)

    def swap(value):
        return lax.ppermute(value, "sen", [(0, 1), (1, 0)])

    def exchange(value):
        return lax.all_to_all(value, "pts", split_axis=0, concat_axis=0, tiled=False)

    table, weights = packed_tables(steps, wide)
    packing = Packing(2 * points, bins_count)
    packing_probes = Packing(points, steps)
    packings = dict(packing=packing, packing_probes=packing_probes)
    sizes = dict(points=points, sens=sens, half=half, wide=wide, **packings)
    orders = split_order(width)
    order = orders[0] + orders[1]
    places = jnp.stack([me[0], core[0]])
    lean = lean_partners(width)

    def chunk(tiles):
        return jax.ShapeDtypeStruct((tiles, sens, LANES), bf16)

    both = packing.tiles + packing_probes.tiles
    in_hbm = pl.BlockSpec(memory_space=pltpu.HBM)
    sent = pl.pallas_call(
        functools.partial(pack_kernel, order=order, lean=lean, half=half, **packings),
        out_shape=tuple(chunk(packing.tiles if r in lean else both) for r in order),
        in_specs=in_smem(1) + [in_hbm] * 3,
        out_specs=tuple(in_vmem(width)),
        scratch_shapes=[
            pltpu.SMEM(prior_scale.shape, f32),
            pltpu.VMEM((2, points, width, sens, bins_count), bf16),
            pltpu.VMEM((half, points, steps), bf16),
            pltpu.SemaphoreType.DMA((2 + 2 * points,)),
        ],
        compiler_params=limit(8),
        name="pack",
    )(places, *kept(pltpu.HBM, prior_scale, kernel.reshape(2, points, width, sens, bins_count), probes))
    blocks = {}
    others = {}
    for relative, value in zip(order, sent):
        if relative:
            value = lax.ppermute(value, "pts", [(i, i ^ relative) for i in range(width)])
        blocks[relative] = value
        others[relative] = swap(value)
    relayed = pl.pallas_call(
        functools.partial(relay_kernel, first_tile=packing.tiles),
        out_shape=chunk(len(lean) * packing_probes.tiles),
        in_specs=in_vmem(len(lean)),
        out_specs=in_vmem(1)[0],
        compiler_params=limit(2),
        name="relay",
    )(*[blocks[r ^ 1] for r in lean])
    relayed = lax.ppermute(relayed, "pts", [(i, i ^ 1) for i in range(width)])
    noise_other = swap(noise_weight)
    deflation_other = swap(deflation)
    basis_other = swap(basis)

    def scratch(count):
        return [
            pltpu.VMEM((3, count * points * half, wide), f32),
            pltpu.VMEM((count * points * half, wide), f32),
        ]

    def ready(part):
        return [blocks[r] for r in part] + [others[r] for r in part]

    table = pl.pallas_call(
        stage_kernel,
        out_shape=pltpu.VMEM(table.shape, bf16),
        in_specs=[in_hbm],
        out_specs=in_vmem(1)[0],
        scratch_shapes=[pltpu.SemaphoreType.DMA],
        compiler_params=limit(2),
        name="stage",
    )(*kept(pltpu.HBM, table))
    count = len(orders[0])
    kern_first, data_first = pl.pallas_call(
        functools.partial(first_kernel, count=count, **sizes),
        out_shape=(
            jax.ShapeDtypeStruct((3, count * points, 2 * sens, wide), f32),
            jax.ShapeDtypeStruct((2 * sens * half, 2 * wide), f32),
        ),
        in_specs=in_vmem(1 + 2 * count),
        out_specs=tuple(in_vmem(2)),
        scratch_shapes=scratch(count),
        compiler_params=limit(12),
        name="first",
    )(table, *ready(orders[0]))
    count = len(orders[1])
    back = pl.pallas_call(
        functools.partial(bins_kernel, orders=orders, lean=lean, **sizes),
        out_shape=jax.ShapeDtypeStruct((width, packing_probes.tiles, half, LANES), bf16),
        in_specs=in_smem(1) + [in_hbm] + in_vmem(6 + 2 * count),
        out_specs=in_vmem(1)[0],
        scratch_shapes=[pltpu.VMEM((3, count * points, 2 * sens, wide), f32)]
        + scratch(count)
        + [
            pltpu.VMEM((2 * sens * half, 2 * wide), f32),
            pltpu.VMEM((3, 2 * sens * half, wide), f32),
            pltpu.VMEM((width * points * half, 2 * wide), f32),
            pltpu.SMEM(noise_weight.shape, f32),
            pltpu.SMEM(noise_weight.shape, f32),
            pltpu.SemaphoreType.DMA((2,)),
        ],
        compiler_params=limit(20),
        name="bins",
    )(
        me, *kept(pltpu.HBM, noise_weight), noise_other, table, weights, kern_first, data_first,
        relayed, *ready(orders[1]),
    )
    back, basis_other, deflation_other = lax.optimization_barrier(
        (back, basis_other, deflation_other)
    )
    basis, basis_other = kept(pltpu.VMEM, basis, basis_other)
    parts = exchange(back)
    flat, coeff = pl.pallas_call(
        functools.partial(coeff_kernel, points=points, steps=steps, rank=rank, packing=packing_probes),
        out_shape=(
            jax.ShapeDtypeStruct((half, points * steps), f32),
            jax.ShapeDtypeStruct((width, half, 2 * rank), bf16),
        ),
        in_specs=in_vmem(4),
        out_specs=tuple(in_vmem(2)),
        compiler_params=limit(12),
        name="coeff",
    )(prior_scale[None, :], parts, basis, basis_other)
    flat_other = swap(flat)
    coeff_parts = exchange(coeff)
    coeff_other = swap(coeff_parts)
    return pl.pallas_call(
        functools.partial(deflate_kernel, points=points, steps=steps, rank=rank),
        out_shape=jax.ShapeDtypeStruct((probe_count, points, steps), f32),
        in_specs=in_smem(1) + in_vmem(8),
        out_specs=in_vmem(1)[0],
        compiler_params=limit(12),
        name="deflate",
    )(
        core, coeff_parts, coeff_other, deflation[None, :], deflation_other[None, :],
        flat, flat_other, basis, basis_other,
    )


def solution(mesh):
    placed = (
        P(None, ("grp", "pts"), None),
        P(None, ("grp", "pts"), "sen", None),
        P(("grp", "sen")),
        P("pts"),
        P("pts", "sen"),
        P("sen"),
    )

    def body(*args):
        width = mesh.shape["pts"]
        split = mesh.shape["sen"] == 2 and width == ROWS
        whole_tiles = args[2].shape[0] == width * ROWS and args[0].shape[0] == 2 * ROWS
        if not (split and whole_tiles):
            return local(*args)
        return local_split(*args)

    return jax.shard_map(
        body, mesh=mesh, in_specs=placed, out_specs=P(None, ("grp", "pts"), None), check_vma=False
    )
```

```python
import functools
import math

import jax
import jax.numpy as jnp
import numpy as np
from jax import lax
from jax.experimental import pallas as pl
from jax.experimental.pallas import tpu as pltpu
from jax.sharding import PartitionSpec as P

LANES = 128
ROWS = 8


def tables(steps_count):
    bins_count = steps_count + 1
    turns = (
        jnp.arange(steps_count, dtype=jnp.int32)[:, None]
        * jnp.arange(bins_count, dtype=jnp.int32)[None, :]
        % (2 * steps_count)
    )
    angle = turns.astype(jnp.float32) * (math.pi / steps_count)
    cosine = jnp.cos(angle)
    sine = jnp.sin(angle)
    freq = jnp.arange(bins_count, dtype=jnp.int32)
    edge = (freq == 0) | (freq == steps_count)
    weights = jnp.where(edge, 1.0, 2.0).astype(jnp.float32) / (2.0 * steps_count)
    forward = jnp.concatenate([cosine, -sine], axis=1)
    inverse = jnp.concatenate([cosine * weights[None, :], -sine * weights[None, :]], axis=1)
    return (forward, inverse)


def widened(value):
    return lax.optimization_barrier(value).astype(jnp.float32)


def complex_data(spec_real, spec_imag, kern_real, kern_imag):
    data_real = jnp.einsum(
        "kpf,psf->ksf", spec_real, kern_real, preferred_element_type=jnp.float32
    ) - jnp.einsum("kpf,psf->ksf", spec_imag, kern_imag, preferred_element_type=jnp.float32)
    data_imag = jnp.einsum(
        "kpf,psf->ksf", spec_real, kern_imag, preferred_element_type=jnp.float32
    ) + jnp.einsum("kpf,psf->ksf", spec_imag, kern_real, preferred_element_type=jnp.float32)
    return (data_real, data_imag)


def complex_adjoint(weight_real, weight_imag, kern_real, kern_imag):
    adj_real = jnp.einsum(
        "ksf,psf->kpf", weight_real, kern_real, preferred_element_type=jnp.float32
    ) + jnp.einsum("ksf,psf->kpf", weight_imag, kern_imag, preferred_element_type=jnp.float32)
    adj_imag = jnp.einsum(
        "ksf,psf->kpf", weight_imag, kern_real, preferred_element_type=jnp.float32
    ) - jnp.einsum("ksf,psf->kpf", weight_real, kern_imag, preferred_element_type=jnp.float32)
    return (adj_real, adj_imag)


def local(probes, kernel, noise_weight, prior_scale, basis, deflation):
    highest = lax.Precision.HIGHEST
    probe_count, point_count, steps_count = probes.shape
    bins_count = steps_count + 1
    sensor_count = noise_weight.shape[0]
    forward, inverse = tables(steps_count)
    scaled = probes.astype(jnp.float32) * prior_scale[None, :, None]
    spectrum = jnp.dot(scaled, forward, precision=highest).astype(jnp.bfloat16)
    noise_rows = jnp.tile(noise_weight, probe_count)
    width = lax.axis_size("pts")
    block = (bins_count + width - 1) // width
    extra = block * width - bins_count
    kern_pad = jnp.pad(kernel, ((0, 0), (0, 0), (0, 0), (0, extra)))
    spec_pad = jnp.pad(
        spectrum.reshape(probe_count, point_count, 2, bins_count),
        ((0, 0), (0, 0), (0, 0), (0, extra)),
    )
    kern_bins, spec_bins = (
        lax.all_to_all(kern_pad, "pts", split_axis=3, concat_axis=1, tiled=True),
        lax.all_to_all(spec_pad, "pts", split_axis=3, concat_axis=1, tiled=True),
    )
    bin_kern_real = kern_bins[0]
    bin_kern_imag = kern_bins[1]
    data_real, data_imag = complex_data(
        spec_bins[:, :, 0], spec_bins[:, :, 1], bin_kern_real, bin_kern_imag
    )
    data_bins = jnp.stack([data_real, data_imag], axis=2).reshape(
        probe_count * sensor_count, 2, block
    )
    rows_time = lax.all_to_all(
        data_bins.astype(jnp.bfloat16), "pts", split_axis=0, concat_axis=2, tiled=True
    ).astype(data_bins.dtype)
    local_rows = rows_time.shape[0]
    begin = lax.axis_index("pts") * local_rows
    local_noise = lax.dynamic_slice_in_dim(noise_rows, begin, local_rows)
    data_rows = rows_time[:, :, :bins_count].reshape(local_rows, 2 * bins_count)
    observed = jnp.dot(data_rows, inverse.T, precision=highest)
    residual = (observed * local_noise[:, None]).astype(jnp.bfloat16)
    weighted_local = (
        jnp.dot(widened(residual), inverse, precision=highest)
        .astype(jnp.bfloat16)
        .reshape(local_rows, 2, bins_count)
    )
    weighted_pad = jnp.pad(weighted_local, ((0, 0), (0, 0), (0, extra)))
    weighted_bins = lax.all_to_all(weighted_pad, "pts", split_axis=2, concat_axis=0, tiled=True)
    weighted_bins = weighted_bins.reshape(probe_count, sensor_count, 2, block)
    adj_real, adj_imag = complex_adjoint(
        weighted_bins[:, :, 0], weighted_bins[:, :, 1], bin_kern_real, bin_kern_imag
    )
    adj_bins = jnp.stack([adj_real, adj_imag], axis=2)
    adj_points = lax.all_to_all(
        adj_bins.astype(jnp.bfloat16), "pts", split_axis=1, concat_axis=3, tiled=True
    ).astype(adj_bins.dtype)
    adjoint = adj_points[..., :bins_count].reshape(probe_count, point_count, 2 * bins_count)
    back = jnp.dot(adjoint, forward.T, precision=highest)
    back = lax.psum(back.astype(jnp.bfloat16), "sen").astype(jnp.float32)
    hessian = back * prior_scale[None, :, None]
    flat = hessian.reshape(probe_count, point_count * steps_count)
    flat_low = flat.astype(jnp.bfloat16)
    coeff = jnp.dot(flat_low, basis, preferred_element_type=jnp.float32)
    coeff = lax.psum(coeff, "pts")
    shrunk = (coeff * deflation[None, :]).astype(jnp.bfloat16)
    correction = lax.dot_general(
        shrunk, basis, (((1,), (1,)), ((), ())), preferred_element_type=jnp.float32
    )
    correction = lax.psum(correction.astype(jnp.bfloat16), "sen").astype(jnp.float32)
    return (flat - correction).reshape(probe_count, point_count, steps_count)


def round_up(value, step):
    return (value + step - 1) // step * step


def packed_tables(steps_count, wide):
    bins_count = steps_count + 1
    turns = np.arange(steps_count)[:, None] * np.arange(bins_count)[None, :] % (2 * steps_count)
    angle = turns.astype(np.float64) * (math.pi / steps_count)
    table = np.zeros((wide, 2 * wide), np.float32)
    table[:steps_count, :bins_count] = np.cos(angle)
    table[:steps_count, wide : wide + bins_count] = -np.sin(angle)
    weights = np.zeros((1, wide), np.float32)
    weights[0, :bins_count] = 2.0 / (2.0 * steps_count)
    weights[0, 0] = weights[0, steps_count] = 1.0 / (2.0 * steps_count)
    return jnp.asarray(table.astype(jnp.bfloat16)), jnp.asarray(weights)


NT = (((1,), (1,)), ((), ()))


class Packing:
    def __init__(self, rows, length):
        self.full = length // LANES
        self.tail = length % LANES
        self.slots = LANES // self.tail
        self.first_tail = rows * self.full
        self.tiles = self.first_tail + -(-rows // self.slots)

    def place(self, row):
        return self.first_tail + row // self.slots, row % self.slots * self.tail


def turned(tile, lanes):
    lanes = lanes % LANES
    return pltpu.roll(tile, lanes, axis=tile.ndim - 1) if lanes else tile


def add_tail(packing, row, value, merged):
    tile, lane = packing.place(row)
    tail = value[..., packing.full * LANES : (packing.full + 1) * LANES]
    where = lax.broadcasted_iota(jnp.int32, tail.shape, tail.ndim - 1)
    tail = turned(jnp.where(where < packing.tail, tail, 0.0), lane)
    merged[tile] = merged[tile] + tail if tile in merged else tail


def store_packed(out_tile, packing, row, value, merged):
    for t in range(packing.full):
        lanes = slice(t * LANES, (t + 1) * LANES)
        out_tile(row * packing.full + t, value[..., lanes].astype(jnp.bfloat16))
    add_tail(packing, row, value, merged)


def store_tails(out_tile, merged):
    for tile, value in merged.items():
        out_tile(tile, value.astype(jnp.bfloat16))


def pack_kernel(
    index, prior_far, noise_far, kernel, probes, table_far, *refs,
    order, lean, half, packing, packing_probes,
):
    outs = refs[: len(order)]
    table, prior, noise, kernel_here, probes_here, sems = refs[len(order) :]
    f32 = jnp.float32
    bf16 = jnp.bfloat16
    _, points, _ = probes_here.shape
    edge = packing.full * LANES
    me = index[0]
    mine = pl.multiple_of(index[1] * half, half)
    copies = [
        pltpu.make_async_copy(probes.at[pl.ds(mine, half)], probes_here, sems.at[0]),
        pltpu.make_async_copy(prior_far, prior, sems.at[1]),
    ]
    for row in range(2 * points):
        at = (row // points, row % points)
        copies.append(pltpu.make_async_copy(kernel.at[at], kernel_here.at[at], sems.at[2 + row]))
    copies.append(pltpu.make_async_copy(noise_far, noise, sems.at[2 + 2 * points]))
    copies.append(pltpu.make_async_copy(table_far, table, sems.at[3 + 2 * points]))
    for copy in copies:
        copy.start()

    def padded(value):
        missing = jnp.zeros((value.shape[0], edge + LANES - value.shape[1]), f32)
        return jnp.concatenate([value, missing], axis=1)

    copies[0].wait()
    copies[1].wait()
    scaled = probes_here[...].astype(f32)
    tiles = {}
    tails = {}
    for p in range(points):
        value = padded(scaled[:, p, :] * prior[p])
        store_packed(tiles.__setitem__, packing_probes, p, value, tails)
    store_tails(tiles.__setitem__, tails)
    for copy in copies[2:-1]:
        copy.wait()
    for relative, out in zip(order, outs):

        def out_tile(tile, value, out=out):
            out[tile] = value

        if relative not in lean:
            for tile, value in tiles.items():
                out_tile(packing.tiles + tile, value)
        merged = {}
        for row in range(2 * points):
            value = padded(kernel_here[row // points, row % points, me ^ relative].astype(f32))
            store_packed(out_tile, packing, row, value, merged)
        store_tails(out_tile, merged)
    sens = outs[0].shape[1]
    shape = (sens, LANES)
    where = lax.broadcasted_iota(jnp.int32, shape, 0)
    lane = lax.broadcasted_iota(jnp.int32, shape, 1)
    column = jnp.zeros(shape, f32)
    for s in range(sens):
        column = jnp.where(where == s, noise[me * sens + s], column)
    high = column.astype(bf16).astype(f32)
    middle = (column - high).astype(bf16).astype(f32)
    low = column - high - middle
    pieces = jnp.where(lane == 0, high, jnp.where(lane == 1, middle, jnp.where(lane == 2, low, 0.0)))
    outs[0][outs[0].shape[0] - 1] = pieces.astype(bf16)
    copies[-1].wait()


def unpack(source, row, packing, base=0):
    f32 = jnp.float32
    tiles = [source[base + row * packing.full + t].astype(f32) for t in range(packing.full)]
    tile, lane = packing.place(row)
    tiles.append(turned(source[base + tile].astype(f32), -lane))
    return tiles


def widen(sources, kern, *, packing, points, sens):
    for b, pair in enumerate(sources):
        for half, source in enumerate(pair):
            at = slice(half * sens, (half + 1) * sens)
            for p in range(points):
                real = unpack(source, p, packing)
                imag = unpack(source, points + p, packing)
                for t, (x, y) in enumerate(zip(real, imag)):
                    lanes = slice(t * LANES, (t + 1) * LANES)
                    kern[0, b * points + p, at, lanes] = x
                    kern[1, b * points + p, at, lanes] = x + y
                    kern[2, b * points + p, at, lanes] = x - y


def spectra(sources, table, spec, rows, *, packing, points, half, wide):
    for b, (source, base) in enumerate(sources):
        for p in range(points):
            at = slice((b * points + p) * half, (b * points + p + 1) * half)
            for t, tile in enumerate(unpack(source, p, packing, base)):
                rows[at, t * LANES : (t + 1) * LANES] = tile
    got = jnp.dot(rows[...].astype(jnp.bfloat16), table[...], preferred_element_type=jnp.float32)
    real = got[:, :wide]
    imag = got[:, wide:]
    spec[0] = real + imag
    spec[1] = imag
    spec[2] = real


def forward_sum(kern, spec, data, earlier, *, points, sens, half, wide):
    f32 = jnp.float32
    blocks = kern.shape[1] // points

    def tile_step(ft, carry):
        lanes = pl.ds(pl.multiple_of(ft * LANES, LANES), LANES)
        shifted = pl.ds(pl.multiple_of(wide + ft * LANES, LANES), LANES)
        for first in range(0, 2 * sens, sens):

            def source(b, acc, first=first):
                acc = list(acc)
                for p in range(points):
                    q = b * points + p
                    at = pl.ds(pl.multiple_of(q * half, ROWS), half)
                    both = spec[0, at, lanes]
                    imag = spec[1, at, lanes]
                    real = spec[2, at, lanes]
                    for s in range(sens):
                        row = slice(first + s, first + s + 1)
                        acc[3 * s] += kern[0, q, row, lanes] * both
                        acc[3 * s + 1] += kern[1, q, row, lanes] * imag
                        acc[3 * s + 2] += kern[2, q, row, lanes] * real
                return tuple(acc)

            zero = jnp.zeros((half, LANES), f32)
            acc = lax.fori_loop(0, blocks, source, (zero,) * (3 * sens))
            for s in range(sens):
                at = slice((first + s) * half, (first + s + 1) * half)
                real = acc[3 * s] - acc[3 * s + 1]
                imag = acc[3 * s] - acc[3 * s + 2]
                if earlier is not None:
                    real += earlier[at, lanes]
                    imag += earlier[at, shifted]
                data[at, lanes] = real
                data[at, shifted] = imag
        return carry

    lax.fori_loop(0, wide // LANES, tile_step, 0)


def paired(refs, count):
    return list(zip(refs[:count], refs[count : 2 * count]))


def first_kernel(table, *refs, count, points, sens, half, wide, packing, packing_probes):
    sources = paired(refs, count)
    kern, data, spec, rows = refs[2 * count :]
    probes = [(own, packing.tiles) for own, _ in sources]
    spectra(probes, table, spec, rows, packing=packing_probes, points=points, half=half, wide=wide)
    widen(sources, kern, packing=packing, points=points, sens=sens)
    forward_sum(kern, spec, data, None, points=points, sens=sens, half=half, wide=wide)


def bins_kernel(
    index, noise_far, neighbour, table, weights, kern_first, data_first, *refs,
    orders, lean, points, sens, half, wide, packing, packing_probes,
):
    count = len(orders[1])
    sources = paired(refs, count)
    out, kern, spec, rows, data, wdata, adjoint, noise_own, sem = refs[2 * count :]
    copy = pltpu.make_async_copy(noise_far, noise_own, sem)
    copy.start()
    tiles = wide // LANES
    f32 = jnp.float32
    bf16 = jnp.bfloat16
    probes = []
    for relative, (own, _) in zip(orders[1], sources):
        if relative in lean:
            behind = packing.tiles + (1 + lean.index(relative)) * packing_probes.tiles
            probes.append((sources[orders[1].index(1)][0], behind))
        else:
            probes.append((own, packing.tiles))
    spectra(probes, table, spec, rows, packing=packing_probes, points=points, half=half, wide=wide)
    widen(sources, kern, packing=packing, points=points, sens=sens)
    forward_sum(kern, spec, data, data_first, points=points, sens=sens, half=half, wide=wide)
    table_v = table[...]
    weight_rows = weights[...]
    scaled = jnp.concatenate(
        [data[:, :wide] * weight_rows, data[:, wide:] * weight_rows], axis=1
    ).astype(bf16)
    observed = lax.dot_general(scaled, table_v, NT, preferred_element_type=f32)
    copy.wait()
    pieces = neighbour[neighbour.shape[0] - 1].astype(f32)
    column = pieces[:, 0:1] + pieces[:, 1:2] + pieces[:, 2:3]
    scales = [noise_own[index[0] * sens + s] for s in range(sens)]
    scales += [column[s : s + 1] for s in range(sens)]
    residual = jnp.concatenate(
        [observed[s * half : (s + 1) * half] * scale for s, scale in enumerate(scales)], axis=0
    ).astype(bf16)
    weighted = jnp.dot(residual, table_v, preferred_element_type=f32)
    real = weighted[:, :wide] * weight_rows
    imag = weighted[:, wide:] * weight_rows
    wdata[0] = real + imag
    wdata[1] = imag
    wdata[2] = real

    base = 0
    for source, order in ((kern_first, orders[0]), (kern, orders[1])):

        group = points if len(order) % 2 else 2 * points

        def adjoint_tile(step, carry, source=source, base=base, group=group):
            first = step // tiles * group
            ft = step % tiles
            lanes = pl.ds(pl.multiple_of(ft * LANES, LANES), LANES)
            shifted = pl.ds(pl.multiple_of(wide + ft * LANES, LANES), LANES)
            zero = jnp.zeros((half, LANES), f32)
            acc = [zero] * (3 * group)
            for s in range(2 * sens):
                at = slice(s * half, (s + 1) * half)
                both = wdata[0, at, lanes]
                imag = wdata[1, at, lanes]
                real = wdata[2, at, lanes]
                row = slice(s, s + 1)
                for p in range(group):
                    acc[3 * p] += source[0, first + p, row, lanes] * both
                    acc[3 * p + 1] += source[2, first + p, row, lanes] * imag
                    acc[3 * p + 2] += source[1, first + p, row, lanes] * real
            for p in range(group):
                at = pl.ds(pl.multiple_of((base + first + p) * half, ROWS), half)
                adjoint[at, lanes] = acc[3 * p] - acc[3 * p + 1]
                adjoint[at, shifted] = acc[3 * p] - acc[3 * p + 2]
            return carry

        lax.fori_loop(0, len(order) * points // group * tiles, adjoint_tile, 0)
        base += len(order) * points
    back = lax.dot_general(adjoint[...].astype(bf16), table_v, NT, preferred_element_type=f32)
    for b, relative in enumerate(orders[0] + orders[1]):
        there = index[0] ^ relative

        def out_tile(tile, value, there=there):
            out[there, tile] = value

        merged = {}
        for p in range(points):
            at = slice((b * points + p) * half, (b * points + p + 1) * half)
            store_packed(out_tile, packing_probes, p, back[at], merged)
        store_tails(out_tile, merged)


def summed(parts):
    total = parts[0].astype(jnp.float32)
    for j in range(1, parts.shape[0]):
        total += parts[j].astype(jnp.float32)
    return total


def coeff_kernel(
    prior, deflation, parts, basis_own, basis_other, flat, coeff, *, points, steps, rank, packing
):
    f32 = jnp.float32
    total = summed(parts)
    for p in range(points):
        tiles = [total[p * packing.full + t] for t in range(packing.full)]
        tile, lane = packing.place(p)
        tiles.append(turned(total[tile], -lane))
        piece = jnp.concatenate(tiles, axis=1) * prior[:, p : p + 1]
        flat[:, p * steps : (p + 1) * steps] = piece[:, :steps]
    low = flat[:, : points * steps].astype(jnp.bfloat16)
    behind = flat.shape[1] - rank
    flat[:, behind:] = jnp.broadcast_to(deflation[...], (flat.shape[0], rank))
    own = jnp.dot(low, basis_own[...], preferred_element_type=f32).astype(jnp.bfloat16)
    other = jnp.dot(low, basis_other[...], preferred_element_type=f32).astype(jnp.bfloat16)
    for j in range(coeff.shape[0]):
        coeff[j, :, :rank] = own
        coeff[j, :, rank:] = other


def deflate_kernel(
    core, parts_own, parts_other, flat_own, flat_other, basis_own, basis_other, out,
    *, points, steps, rank,
):
    f32 = jnp.float32
    bf16 = jnp.bfloat16
    own = summed(parts_own)
    other = summed(parts_other)
    half = own.shape[0]
    behind = flat_own.shape[1] - rank
    deflation_own = flat_own[0:1, behind:]
    deflation_other = flat_other[0:1, behind:]
    size = points * steps
    here = jnp.concatenate([own[:, :rank], other[:, rank:]], axis=0) * deflation_own
    there = jnp.concatenate([own[:, rank:], other[:, :rank]], axis=0) * deflation_other
    correction = lax.dot_general(here.astype(bf16), basis_own[...], NT, preferred_element_type=f32)
    correction += lax.dot_general(there.astype(bf16), basis_other[...], NT, preferred_element_type=f32)
    result = jnp.concatenate([flat_own[:, :size], flat_other[:, :size]], axis=0) - correction
    mine = core[0] * half
    for p in range(points):
        piece = result[:, p * steps : (p + 1) * steps]
        out[pl.ds(mine, half), p, :] = piece[:half]
        out[pl.ds(half - mine, half), p, :] = piece[half:]


def split_order(width):
    near = list(range(2, width // 2))
    far = list(range(width // 2, width))
    order = [0] + [r for r in far if r % 2 == 0] + near + [r for r in far if r % 2] + [1]
    return order[: width // 2], order[width // 2 :]


def lean_partners(width):
    return [r for r in range(width // 2, width) if r % 2]


def relay_kernel(ours, *refs, first_tile):
    sources, out = refs[:-1], refs[-1]
    base = ours.shape[0]
    out[:base] = ours[...]
    for source in sources:
        count = source.shape[0] - first_tile
        out[base : base + count] = source[first_tile:]
        base += count


def kept(space, *values):
    return [pltpu.with_memory_space_constraint(value, space) for value in values]


def in_vmem(count):
    return [pl.BlockSpec(memory_space=pltpu.VMEM) for _ in range(count)]


def in_smem(count):
    return [pl.BlockSpec(memory_space=pltpu.SMEM) for _ in range(count)]


def limit(mib):
    return pltpu.CompilerParams(vmem_limit_bytes=mib * 1024 * 1024)


def local_split(probes, kernel, noise_weight, prior_scale, basis, deflation):
    bf16 = jnp.bfloat16
    f32 = jnp.float32
    probe_count, points, steps = probes.shape
    bins_count = steps + 1
    width = lax.axis_size("pts")
    sens = noise_weight.shape[0] // width
    half = probe_count // 2
    rank = basis.shape[1]
    wide = round_up(bins_count, LANES)
    me = jnp.full((1,), lax.axis_index("pts"), jnp.int32)
    core_index = lax.axis_index("sen")
    core = jnp.full((1,), core_index, jnp.int32)

    def swap(value):
        return lax.ppermute(value, "sen", [(0, 1), (1, 0)])

    def exchange(value):
        return lax.all_to_all(value, "pts", split_axis=0, concat_axis=0, tiled=False)

    table, weights = packed_tables(steps, wide)
    packing = Packing(2 * points, bins_count)
    packing_probes = Packing(points, steps)
    packings = dict(packing=packing, packing_probes=packing_probes)
    sizes = dict(points=points, sens=sens, half=half, wide=wide, **packings)
    orders = split_order(width)
    order = orders[0] + orders[1]
    places = jnp.stack([me[0], core[0]])
    lean = lean_partners(width)

    def chunk(tiles):
        return jax.ShapeDtypeStruct((tiles, sens, LANES), bf16)

    both = packing.tiles + packing_probes.tiles
    tiles = [packing.tiles if r in lean else both for r in order]
    tiles[0] += 1
    in_hbm = pl.BlockSpec(memory_space=pltpu.HBM)
    *sent, table = pl.pallas_call(
        functools.partial(pack_kernel, order=order, lean=lean, half=half, **packings),
        out_shape=tuple(chunk(count) for count in tiles) + (pltpu.VMEM(table.shape, bf16),),
        in_specs=in_smem(1) + [in_hbm] * 5,
        out_specs=tuple(in_vmem(width + 1)),
        scratch_shapes=[
            pltpu.SMEM(prior_scale.shape, f32),
            pltpu.SMEM(noise_weight.shape, f32),
            pltpu.VMEM((2, points, width, sens, bins_count), bf16),
            pltpu.VMEM((half, points, steps), bf16),
            pltpu.SemaphoreType.DMA((4 + 2 * points,)),
        ],
        compiler_params=limit(8),
        name="pack",
    )(
        places,
        *kept(
            pltpu.HBM,
            prior_scale,
            noise_weight,
            kernel.reshape(2, points, width, sens, bins_count),
            probes,
            table,
        ),
    )
    blocks = {}
    others = {}
    for relative, value in zip(order, sent):
        if relative == 1:
            value = pl.pallas_call(
                functools.partial(relay_kernel, first_tile=packing.tiles),
                out_shape=chunk(both + len(lean) * packing_probes.tiles),
                in_specs=in_vmem(1 + len(lean)),
                out_specs=in_vmem(1)[0],
                compiler_params=limit(2),
                name="relay",
            )(value, *[blocks[r ^ 1] for r in lean])
        if relative:
            value = lax.ppermute(value, "pts", [(i, i ^ relative) for i in range(width)])
        blocks[relative] = value
        others[relative] = swap(value)
    basis_other = swap(basis)

    def scratch(count):
        return [
            pltpu.VMEM((3, count * points * half, wide), f32),
            pltpu.VMEM((count * points * half, wide), f32),
        ]

    def ready(part):
        return [blocks[r] for r in part] + [others[r] for r in part]

    count = len(orders[0])
    kern_first, data_first = pl.pallas_call(
        functools.partial(first_kernel, count=count, **sizes),
        out_shape=(
            jax.ShapeDtypeStruct((3, count * points, 2 * sens, wide), f32),
            jax.ShapeDtypeStruct((2 * sens * half, 2 * wide), f32),
        ),
        in_specs=in_vmem(1 + 2 * count),
        out_specs=tuple(in_vmem(2)),
        scratch_shapes=scratch(count),
        compiler_params=limit(12),
        name="first",
    )(table, *ready(orders[0]))
    count = len(orders[1])
    back = pl.pallas_call(
        functools.partial(bins_kernel, orders=orders, lean=lean, **sizes),
        out_shape=jax.ShapeDtypeStruct((width, packing_probes.tiles, half, LANES), bf16),
        in_specs=in_smem(1) + [in_hbm] + in_vmem(5 + 2 * count),
        out_specs=in_vmem(1)[0],
        scratch_shapes=[pltpu.VMEM((3, count * points, 2 * sens, wide), f32)]
        + scratch(count)
        + [
            pltpu.VMEM((2 * sens * half, 2 * wide), f32),
            pltpu.VMEM((3, 2 * sens * half, wide), f32),
            pltpu.VMEM((width * points * half, 2 * wide), f32),
            pltpu.SMEM(noise_weight.shape, f32),
            pltpu.SemaphoreType.DMA,
        ],
        compiler_params=limit(20),
        name="bins",
    )(
        me, *kept(pltpu.HBM, noise_weight), others[0], table, weights, kern_first, data_first,
        *ready(orders[1]),
    )
    back, basis_other = lax.optimization_barrier((back, basis_other))
    basis, basis_other = kept(pltpu.VMEM, basis, basis_other)
    parts = exchange(back)
    flat, coeff = pl.pallas_call(
        functools.partial(coeff_kernel, points=points, steps=steps, rank=rank, packing=packing_probes),
        out_shape=(
            jax.ShapeDtypeStruct((half, round_up(points * steps, LANES) + rank), f32),
            jax.ShapeDtypeStruct((width, half, 2 * rank), bf16),
        ),
        in_specs=in_vmem(5),
        out_specs=tuple(in_vmem(2)),
        compiler_params=limit(12),
        name="coeff",
    )(prior_scale[None, :], deflation[None, :], parts, basis, basis_other)
    flat_other = swap(flat)
    coeff_parts = exchange(coeff)
    coeff_other = swap(coeff_parts)
    return pl.pallas_call(
        functools.partial(deflate_kernel, points=points, steps=steps, rank=rank),
        out_shape=jax.ShapeDtypeStruct((probe_count, points, steps), f32),
        in_specs=in_smem(1) + in_vmem(6),
        out_specs=in_vmem(1)[0],
        compiler_params=limit(12),
        name="deflate",
    )(
        core, coeff_parts, coeff_other, flat, flat_other, basis, basis_other,
    )


def solution(mesh):
    placed = (
        P(None, ("grp", "pts"), None),
        P(None, ("grp", "pts"), "sen", None),
        P(("grp", "sen")),
        P("pts"),
        P("pts", "sen"),
        P("sen"),
    )

    def body(*args):
        width = mesh.shape["pts"]
        split = mesh.shape["sen"] == 2 and width == ROWS
        whole_tiles = args[2].shape[0] == width * ROWS and args[0].shape[0] == 2 * ROWS
        if not (split and whole_tiles):
            return local(*args)
        return local_split(*args)

    return jax.shard_map(
        body, mesh=mesh, in_specs=placed, out_specs=P(None, ("grp", "pts"), None), check_vma=False
    )
```

```python
import functools
import math

import jax
import jax.numpy as jnp
import numpy as np
from jax import lax
from jax.experimental import pallas as pl
from jax.experimental.pallas import tpu as pltpu
from jax.sharding import PartitionSpec as P

LANES = 128
ROWS = 8


def tables(steps_count):
    bins_count = steps_count + 1
    turns = (
        jnp.arange(steps_count, dtype=jnp.int32)[:, None]
        * jnp.arange(bins_count, dtype=jnp.int32)[None, :]
        % (2 * steps_count)
    )
    angle = turns.astype(jnp.float32) * (math.pi / steps_count)
    cosine = jnp.cos(angle)
    sine = jnp.sin(angle)
    freq = jnp.arange(bins_count, dtype=jnp.int32)
    edge = (freq == 0) | (freq == steps_count)
    weights = jnp.where(edge, 1.0, 2.0).astype(jnp.float32) / (2.0 * steps_count)
    forward = jnp.concatenate([cosine, -sine], axis=1)
    inverse = jnp.concatenate([cosine * weights[None, :], -sine * weights[None, :]], axis=1)
    return (forward, inverse)


def widened(value):
    return lax.optimization_barrier(value).astype(jnp.float32)


def complex_data(spec_real, spec_imag, kern_real, kern_imag):
    data_real = jnp.einsum(
        "kpf,psf->ksf", spec_real, kern_real, preferred_element_type=jnp.float32
    ) - jnp.einsum("kpf,psf->ksf", spec_imag, kern_imag, preferred_element_type=jnp.float32)
    data_imag = jnp.einsum(
        "kpf,psf->ksf", spec_real, kern_imag, preferred_element_type=jnp.float32
    ) + jnp.einsum("kpf,psf->ksf", spec_imag, kern_real, preferred_element_type=jnp.float32)
    return (data_real, data_imag)


def complex_adjoint(weight_real, weight_imag, kern_real, kern_imag):
    adj_real = jnp.einsum(
        "ksf,psf->kpf", weight_real, kern_real, preferred_element_type=jnp.float32
    ) + jnp.einsum("ksf,psf->kpf", weight_imag, kern_imag, preferred_element_type=jnp.float32)
    adj_imag = jnp.einsum(
        "ksf,psf->kpf", weight_imag, kern_real, preferred_element_type=jnp.float32
    ) - jnp.einsum("ksf,psf->kpf", weight_real, kern_imag, preferred_element_type=jnp.float32)
    return (adj_real, adj_imag)


def local(probes, kernel, noise_weight, prior_scale, basis, deflation):
    highest = lax.Precision.HIGHEST
    probe_count, point_count, steps_count = probes.shape
    bins_count = steps_count + 1
    sensor_count = noise_weight.shape[0]
    forward, inverse = tables(steps_count)
    scaled = probes.astype(jnp.float32) * prior_scale[None, :, None]
    spectrum = jnp.dot(scaled, forward, precision=highest).astype(jnp.bfloat16)
    noise_rows = jnp.tile(noise_weight, probe_count)
    width = lax.axis_size("pts")
    block = (bins_count + width - 1) // width
    extra = block * width - bins_count
    kern_pad = jnp.pad(kernel, ((0, 0), (0, 0), (0, 0), (0, extra)))
    spec_pad = jnp.pad(
        spectrum.reshape(probe_count, point_count, 2, bins_count),
        ((0, 0), (0, 0), (0, 0), (0, extra)),
    )
    kern_bins, spec_bins = (
        lax.all_to_all(kern_pad, "pts", split_axis=3, concat_axis=1, tiled=True),
        lax.all_to_all(spec_pad, "pts", split_axis=3, concat_axis=1, tiled=True),
    )
    bin_kern_real = kern_bins[0]
    bin_kern_imag = kern_bins[1]
    data_real, data_imag = complex_data(
        spec_bins[:, :, 0], spec_bins[:, :, 1], bin_kern_real, bin_kern_imag
    )
    data_bins = jnp.stack([data_real, data_imag], axis=2).reshape(
        probe_count * sensor_count, 2, block
    )
    rows_time = lax.all_to_all(
        data_bins.astype(jnp.bfloat16), "pts", split_axis=0, concat_axis=2, tiled=True
    ).astype(data_bins.dtype)
    local_rows = rows_time.shape[0]
    begin = lax.axis_index("pts") * local_rows
    local_noise = lax.dynamic_slice_in_dim(noise_rows, begin, local_rows)
    data_rows = rows_time[:, :, :bins_count].reshape(local_rows, 2 * bins_count)
    observed = jnp.dot(data_rows, inverse.T, precision=highest)
    residual = (observed * local_noise[:, None]).astype(jnp.bfloat16)
    weighted_local = (
        jnp.dot(widened(residual), inverse, precision=highest)
        .astype(jnp.bfloat16)
        .reshape(local_rows, 2, bins_count)
    )
    weighted_pad = jnp.pad(weighted_local, ((0, 0), (0, 0), (0, extra)))
    weighted_bins = lax.all_to_all(weighted_pad, "pts", split_axis=2, concat_axis=0, tiled=True)
    weighted_bins = weighted_bins.reshape(probe_count, sensor_count, 2, block)
    adj_real, adj_imag = complex_adjoint(
        weighted_bins[:, :, 0], weighted_bins[:, :, 1], bin_kern_real, bin_kern_imag
    )
    adj_bins = jnp.stack([adj_real, adj_imag], axis=2)
    adj_points = lax.all_to_all(
        adj_bins.astype(jnp.bfloat16), "pts", split_axis=1, concat_axis=3, tiled=True
    ).astype(adj_bins.dtype)
    adjoint = adj_points[..., :bins_count].reshape(probe_count, point_count, 2 * bins_count)
    back = jnp.dot(adjoint, forward.T, precision=highest)
    back = lax.psum(back.astype(jnp.bfloat16), "sen").astype(jnp.float32)
    hessian = back * prior_scale[None, :, None]
    flat = hessian.reshape(probe_count, point_count * steps_count)
    flat_low = flat.astype(jnp.bfloat16)
    coeff = jnp.dot(flat_low, basis, preferred_element_type=jnp.float32)
    coeff = lax.psum(coeff, "pts")
    shrunk = (coeff * deflation[None, :]).astype(jnp.bfloat16)
    correction = lax.dot_general(
        shrunk, basis, (((1,), (1,)), ((), ())), preferred_element_type=jnp.float32
    )
    correction = lax.psum(correction.astype(jnp.bfloat16), "sen").astype(jnp.float32)
    return (flat - correction).reshape(probe_count, point_count, steps_count)


def round_up(value, step):
    return (value + step - 1) // step * step


def packed_tables(steps_count, wide):
    bins_count = steps_count + 1
    turns = np.arange(steps_count)[:, None] * np.arange(bins_count)[None, :] % (2 * steps_count)
    angle = turns.astype(np.float64) * (math.pi / steps_count)
    table = np.zeros((wide, 2 * wide), np.float32)
    table[:steps_count, :bins_count] = np.cos(angle)
    table[:steps_count, wide : wide + bins_count] = -np.sin(angle)
    weights = np.zeros((1, wide), np.float32)
    weights[0, :bins_count] = 2.0 / (2.0 * steps_count)
    weights[0, 0] = weights[0, steps_count] = 1.0 / (2.0 * steps_count)
    return jnp.asarray(table.astype(jnp.bfloat16)), jnp.asarray(weights)


NT = (((1,), (1,)), ((), ()))


class Packing:
    def __init__(self, rows, length):
        self.full = length // LANES
        self.tail = length % LANES
        self.slots = LANES // self.tail
        self.first_tail = rows * self.full
        self.tiles = self.first_tail + -(-rows // self.slots)

    def place(self, row):
        return self.first_tail + row // self.slots, row % self.slots * self.tail


def turned(tile, lanes):
    lanes = lanes % LANES
    return pltpu.roll(tile, lanes, axis=tile.ndim - 1) if lanes else tile


def add_tail(packing, row, value, merged):
    tile, lane = packing.place(row)
    tail = value[..., packing.full * LANES : (packing.full + 1) * LANES]
    where = lax.broadcasted_iota(jnp.int32, tail.shape, tail.ndim - 1)
    tail = turned(jnp.where(where < packing.tail, tail, 0.0), lane)
    merged[tile] = merged[tile] + tail if tile in merged else tail


def store_packed(out_tile, packing, row, value, merged):
    for t in range(packing.full):
        lanes = slice(t * LANES, (t + 1) * LANES)
        out_tile(row * packing.full + t, value[..., lanes].astype(jnp.bfloat16))
    add_tail(packing, row, value, merged)


def store_tails(out_tile, merged):
    for tile, value in merged.items():
        out_tile(tile, value.astype(jnp.bfloat16))


def pack_kernel(
    index, prior_far, noise_far, kernel, probes, table_far, *refs,
    order, lean, half, packing, packing_probes,
):
    outs = refs[: len(order)]
    table, prior, noise, kernel_here, probes_here, sems = refs[len(order) :]
    f32 = jnp.float32
    bf16 = jnp.bfloat16
    _, points, _ = probes_here.shape
    edge = packing.full * LANES
    me = index[0]
    mine = pl.multiple_of(index[1] * half, half)
    copies = [
        pltpu.make_async_copy(probes.at[pl.ds(mine, half)], probes_here, sems.at[0]),
        pltpu.make_async_copy(prior_far, prior, sems.at[1]),
    ]
    for row in range(2 * points):
        at = (row // points, row % points)
        copies.append(pltpu.make_async_copy(kernel.at[at], kernel_here.at[at], sems.at[2 + row]))
    copies.append(pltpu.make_async_copy(noise_far, noise, sems.at[2 + 2 * points]))
    copies.append(pltpu.make_async_copy(table_far, table, sems.at[3 + 2 * points]))
    for copy in copies:
        copy.start()

    def padded(value):
        missing = jnp.zeros((value.shape[0], edge + LANES - value.shape[1]), f32)
        return jnp.concatenate([value, missing], axis=1)

    copies[0].wait()
    copies[1].wait()
    scaled = probes_here[...].astype(f32)
    tiles = {}
    tails = {}
    for p in range(points):
        value = padded(scaled[:, p, :] * prior[p])
        store_packed(tiles.__setitem__, packing_probes, p, value, tails)
    store_tails(tiles.__setitem__, tails)
    for copy in copies[2:-1]:
        copy.wait()
    for relative, out in zip(order, outs):

        def out_tile(tile, value, out=out):
            out[tile] = value

        if relative not in lean:
            for tile, value in tiles.items():
                out_tile(packing.tiles + tile, value)
        merged = {}
        for row in range(2 * points):
            value = padded(kernel_here[row // points, row % points, me ^ relative].astype(f32))
            store_packed(out_tile, packing, row, value, merged)
        store_tails(out_tile, merged)
    sens = outs[0].shape[1]
    shape = (sens, LANES)
    where = lax.broadcasted_iota(jnp.int32, shape, 0)
    lane = lax.broadcasted_iota(jnp.int32, shape, 1)
    column = jnp.zeros(shape, f32)
    for s in range(sens):
        column = jnp.where(where == s, noise[me * sens + s], column)
    high = column.astype(bf16).astype(f32)
    middle = (column - high).astype(bf16).astype(f32)
    low = column - high - middle
    pieces = jnp.where(lane == 0, high, jnp.where(lane == 1, middle, jnp.where(lane == 2, low, 0.0)))
    outs[0][outs[0].shape[0] - 1] = pieces.astype(bf16)
    copies[-1].wait()


def unpack(source, row, packing, base=0):
    f32 = jnp.float32
    tiles = [source[base + row * packing.full + t].astype(f32) for t in range(packing.full)]
    tile, lane = packing.place(row)
    tiles.append(turned(source[base + tile].astype(f32), -lane))
    return tiles


def widen(sources, kern, *, packing, points, sens):
    for b, pair in enumerate(sources):
        for half, source in enumerate(pair):
            at = slice(half * sens, (half + 1) * sens)
            for p in range(points):
                real = unpack(source, p, packing)
                imag = unpack(source, points + p, packing)
                for t, (x, y) in enumerate(zip(real, imag)):
                    lanes = slice(t * LANES, (t + 1) * LANES)
                    kern[0, b * points + p, at, lanes] = x
                    kern[1, b * points + p, at, lanes] = x + y
                    kern[2, b * points + p, at, lanes] = x - y


def spectra(sources, table, spec, rows, *, packing, points, half, wide):
    for b, (source, base) in enumerate(sources):
        for p in range(points):
            at = slice((b * points + p) * half, (b * points + p + 1) * half)
            for t, tile in enumerate(unpack(source, p, packing, base)):
                rows[at, t * LANES : (t + 1) * LANES] = tile
    got = jnp.dot(rows[...].astype(jnp.bfloat16), table[...], preferred_element_type=jnp.float32)
    real = got[:, :wide]
    imag = got[:, wide:]
    spec[0] = real + imag
    spec[1] = imag
    spec[2] = real


def forward_sum(kern, spec, data, earlier, *, points, sens, half, wide):
    f32 = jnp.float32
    blocks = kern.shape[1] // points

    def tile_step(ft, carry):
        lanes = pl.ds(pl.multiple_of(ft * LANES, LANES), LANES)
        shifted = pl.ds(pl.multiple_of(wide + ft * LANES, LANES), LANES)
        for first in range(0, 2 * sens, sens):

            def source(b, acc, first=first):
                acc = list(acc)
                for p in range(points):
                    q = b * points + p
                    at = pl.ds(pl.multiple_of(q * half, ROWS), half)
                    both = spec[0, at, lanes]
                    imag = spec[1, at, lanes]
                    real = spec[2, at, lanes]
                    for s in range(sens):
                        row = slice(first + s, first + s + 1)
                        acc[3 * s] += kern[0, q, row, lanes] * both
                        acc[3 * s + 1] += kern[1, q, row, lanes] * imag
                        acc[3 * s + 2] += kern[2, q, row, lanes] * real
                return tuple(acc)

            zero = jnp.zeros((half, LANES), f32)
            acc = lax.fori_loop(0, blocks, source, (zero,) * (3 * sens))
            for s in range(sens):
                at = slice((first + s) * half, (first + s + 1) * half)
                real = acc[3 * s] - acc[3 * s + 1]
                imag = acc[3 * s] - acc[3 * s + 2]
                if earlier is not None:
                    real += earlier[at, lanes]
                    imag += earlier[at, shifted]
                data[at, lanes] = real
                data[at, shifted] = imag
        return carry

    lax.fori_loop(0, wide // LANES, tile_step, 0)


def paired(refs, count):
    return list(zip(refs[:count], refs[count : 2 * count]))


def first_kernel(table, *refs, count, points, sens, half, wide, packing, packing_probes):
    sources = paired(refs, count)
    kern, data, spec, rows = refs[2 * count :]
    probes = [(own, packing.tiles) for own, _ in sources]
    spectra(probes, table, spec, rows, packing=packing_probes, points=points, half=half, wide=wide)
    widen(sources, kern, packing=packing, points=points, sens=sens)
    forward_sum(kern, spec, data, None, points=points, sens=sens, half=half, wide=wide)


def bins_kernel(
    index, noise_far, neighbour, table, weights, kern_first, data_first, relayed, *refs,
    orders, lean, points, sens, half, wide, packing, packing_probes,
):
    count = len(orders[1])
    sources = paired(refs, count)
    out, kern, spec, rows, data, wdata, adjoint, noise_own, sem = refs[2 * count :]
    copy = pltpu.make_async_copy(noise_far, noise_own, sem)
    copy.start()
    tiles = wide // LANES
    f32 = jnp.float32
    bf16 = jnp.bfloat16
    probes = []
    for relative, (own, _) in zip(orders[1], sources):
        if relative in lean:
            probes.append((relayed, lean.index(relative) * packing_probes.tiles))
        else:
            probes.append((own, packing.tiles))
    spectra(probes, table, spec, rows, packing=packing_probes, points=points, half=half, wide=wide)
    widen(sources, kern, packing=packing, points=points, sens=sens)
    forward_sum(kern, spec, data, data_first, points=points, sens=sens, half=half, wide=wide)
    table_v = table[...]
    weight_rows = weights[...]
    scaled = jnp.concatenate(
        [data[:, :wide] * weight_rows, data[:, wide:] * weight_rows], axis=1
    ).astype(bf16)
    observed = lax.dot_general(scaled, table_v, NT, preferred_element_type=f32)
    copy.wait()
    pieces = neighbour[neighbour.shape[0] - 1].astype(f32)
    column = pieces[:, 0:1] + pieces[:, 1:2] + pieces[:, 2:3]
    scales = [noise_own[index[0] * sens + s] for s in range(sens)]
    scales += [column[s : s + 1] for s in range(sens)]
    residual = jnp.concatenate(
        [observed[s * half : (s + 1) * half] * scale for s, scale in enumerate(scales)], axis=0
    ).astype(bf16)
    weighted = jnp.dot(residual, table_v, preferred_element_type=f32)
    real = weighted[:, :wide] * weight_rows
    imag = weighted[:, wide:] * weight_rows
    wdata[0] = real + imag
    wdata[1] = imag
    wdata[2] = real

    base = 0
    for source, order in ((kern_first, orders[0]), (kern, orders[1])):

        group = points if len(order) % 2 else 2 * points

        def adjoint_tile(step, carry, source=source, base=base, group=group):
            first = step // tiles * group
            ft = step % tiles
            lanes = pl.ds(pl.multiple_of(ft * LANES, LANES), LANES)
            shifted = pl.ds(pl.multiple_of(wide + ft * LANES, LANES), LANES)
            zero = jnp.zeros((half, LANES), f32)
            acc = [zero] * (3 * group)
            for s in range(2 * sens):
                at = slice(s * half, (s + 1) * half)
                both = wdata[0, at, lanes]
                imag = wdata[1, at, lanes]
                real = wdata[2, at, lanes]
                row = slice(s, s + 1)
                for p in range(group):
                    acc[3 * p] += source[0, first + p, row, lanes] * both
                    acc[3 * p + 1] += source[2, first + p, row, lanes] * imag
                    acc[3 * p + 2] += source[1, first + p, row, lanes] * real
            for p in range(group):
                at = pl.ds(pl.multiple_of((base + first + p) * half, ROWS), half)
                adjoint[at, lanes] = acc[3 * p] - acc[3 * p + 1]
                adjoint[at, shifted] = acc[3 * p] - acc[3 * p + 2]
            return carry

        lax.fori_loop(0, len(order) * points // group * tiles, adjoint_tile, 0)
        base += len(order) * points
    back = lax.dot_general(adjoint[...].astype(bf16), table_v, NT, preferred_element_type=f32)
    for b, relative in enumerate(orders[0] + orders[1]):
        there = index[0] ^ relative

        def out_tile(tile, value, there=there):
            out[there, tile] = value

        merged = {}
        for p in range(points):
            at = slice((b * points + p) * half, (b * points + p + 1) * half)
            store_packed(out_tile, packing_probes, p, back[at], merged)
        store_tails(out_tile, merged)


def summed(parts):
    total = parts[0].astype(jnp.float32)
    for j in range(1, parts.shape[0]):
        total += parts[j].astype(jnp.float32)
    return total


def coeff_kernel(
    prior, deflation, parts, basis_own, basis_other, flat, coeff, *, points, steps, rank, packing
):
    f32 = jnp.float32
    total = summed(parts)
    for p in range(points):
        tiles = [total[p * packing.full + t] for t in range(packing.full)]
        tile, lane = packing.place(p)
        tiles.append(turned(total[tile], -lane))
        piece = jnp.concatenate(tiles, axis=1) * prior[:, p : p + 1]
        flat[:, p * steps : (p + 1) * steps] = piece[:, :steps]
    low = flat[:, : points * steps].astype(jnp.bfloat16)
    behind = flat.shape[1] - rank
    flat[:, behind:] = jnp.broadcast_to(deflation[...], (flat.shape[0], rank))
    own = jnp.dot(low, basis_own[...], preferred_element_type=f32).astype(jnp.bfloat16)
    other = jnp.dot(low, basis_other[...], preferred_element_type=f32).astype(jnp.bfloat16)
    for j in range(coeff.shape[0]):
        coeff[j, :, :rank] = own
        coeff[j, :, rank:] = other


def deflate_kernel(
    core, parts_own, parts_other, flat_own, flat_other, basis_own, basis_other, out,
    *, points, steps, rank,
):
    f32 = jnp.float32
    bf16 = jnp.bfloat16
    own = summed(parts_own)
    other = summed(parts_other)
    half = own.shape[0]
    behind = flat_own.shape[1] - rank
    deflation_own = flat_own[0:1, behind:]
    deflation_other = flat_other[0:1, behind:]
    size = points * steps
    here = jnp.concatenate([own[:, :rank], other[:, rank:]], axis=0) * deflation_own
    there = jnp.concatenate([own[:, rank:], other[:, :rank]], axis=0) * deflation_other
    correction = lax.dot_general(here.astype(bf16), basis_own[...], NT, preferred_element_type=f32)
    correction += lax.dot_general(there.astype(bf16), basis_other[...], NT, preferred_element_type=f32)
    result = jnp.concatenate([flat_own[:, :size], flat_other[:, :size]], axis=0) - correction
    mine = core[0] * half
    for p in range(points):
        piece = result[:, p * steps : (p + 1) * steps]
        out[pl.ds(mine, half), p, :] = piece[:half]
        out[pl.ds(half - mine, half), p, :] = piece[half:]


def split_order(width):
    middle, half = width // 4, width // 2
    soon = [0, half, 1, middle]
    return soon, [r for r in (half + middle, half + 1, half + middle + 1, middle + 1)]


def lean_partners(width):
    return [r for r in range(width // 2, width) if r % 2]


def relay_kernel(*refs, first_tile):
    sources, out = refs[:-1], refs[-1]
    count = out.shape[0] // len(sources)
    for n, source in enumerate(sources):
        out[n * count : (n + 1) * count] = source[first_tile:]


def kept(space, *values):
    return [pltpu.with_memory_space_constraint(value, space) for value in values]


def in_vmem(count):
    return [pl.BlockSpec(memory_space=pltpu.VMEM) for _ in range(count)]


def in_smem(count):
    return [pl.BlockSpec(memory_space=pltpu.SMEM) for _ in range(count)]


def limit(mib):
    return pltpu.CompilerParams(vmem_limit_bytes=mib * 1024 * 1024)


def local_split(probes, kernel, noise_weight, prior_scale, basis, deflation):
    bf16 = jnp.bfloat16
    f32 = jnp.float32
    probe_count, points, steps = probes.shape
    bins_count = steps + 1
    width = lax.axis_size("pts")
    sens = noise_weight.shape[0] // width
    half = probe_count // 2
    rank = basis.shape[1]
    wide = round_up(bins_count, LANES)
    me = jnp.full((1,), lax.axis_index("pts"), jnp.int32)
    core_index = lax.axis_index("sen")
    core = jnp.full((1,), core_index, jnp.int32)

    def swap(value):
        return lax.ppermute(value, "sen", [(0, 1), (1, 0)])

    def exchange(value):
        return lax.all_to_all(value, "pts", split_axis=0, concat_axis=0, tiled=False)

    table, weights = packed_tables(steps, wide)
    packing = Packing(2 * points, bins_count)
    packing_probes = Packing(points, steps)
    packings = dict(packing=packing, packing_probes=packing_probes)
    sizes = dict(points=points, sens=sens, half=half, wide=wide, **packings)
    orders = split_order(width)
    order = orders[0] + orders[1]
    places = jnp.stack([me[0], core[0]])
    lean = lean_partners(width)

    def chunk(tiles):
        return jax.ShapeDtypeStruct((tiles, sens, LANES), bf16)

    both = packing.tiles + packing_probes.tiles
    tiles = [packing.tiles if r in lean else both for r in order]
    tiles[0] += 1
    in_hbm = pl.BlockSpec(memory_space=pltpu.HBM)
    *sent, table = pl.pallas_call(
        functools.partial(pack_kernel, order=order, lean=lean, half=half, **packings),
        out_shape=tuple(chunk(count) for count in tiles) + (pltpu.VMEM(table.shape, bf16),),
        in_specs=in_smem(1) + [in_hbm] * 5,
        out_specs=tuple(in_vmem(width + 1)),
        scratch_shapes=[
            pltpu.SMEM(prior_scale.shape, f32),
            pltpu.SMEM(noise_weight.shape, f32),
            pltpu.VMEM((2, points, width, sens, bins_count), bf16),
            pltpu.VMEM((half, points, steps), bf16),
            pltpu.SemaphoreType.DMA((4 + 2 * points,)),
        ],
        compiler_params=limit(8),
        name="pack",
    )(
        places,
        *kept(
            pltpu.HBM,
            prior_scale,
            noise_weight,
            kernel.reshape(2, points, width, sens, bins_count),
            probes,
            table,
        ),
    )
    blocks = {}
    others = {}
    for relative, value in zip(order, sent):
        if relative:
            value = lax.ppermute(value, "pts", [(i, i ^ relative) for i in range(width)])
        blocks[relative] = value
        others[relative] = swap(value)
    relayed = pl.pallas_call(
        functools.partial(relay_kernel, first_tile=packing.tiles),
        out_shape=chunk(len(lean) * packing_probes.tiles),
        in_specs=in_vmem(len(lean)),
        out_specs=in_vmem(1)[0],
        compiler_params=limit(2),
        name="relay",
    )(*[blocks[r ^ 1] for r in lean])
    relayed = lax.ppermute(relayed, "pts", [(i, i ^ 1) for i in range(width)])
    basis_other = swap(basis)

    def scratch(count):
        return [
            pltpu.VMEM((3, count * points * half, wide), f32),
            pltpu.VMEM((count * points * half, wide), f32),
        ]

    def ready(part):
        return [blocks[r] for r in part] + [others[r] for r in part]

    count = len(orders[0])
    kern_first, data_first = pl.pallas_call(
        functools.partial(first_kernel, count=count, **sizes),
        out_shape=(
            jax.ShapeDtypeStruct((3, count * points, 2 * sens, wide), f32),
            jax.ShapeDtypeStruct((2 * sens * half, 2 * wide), f32),
        ),
        in_specs=in_vmem(1 + 2 * count),
        out_specs=tuple(in_vmem(2)),
        scratch_shapes=scratch(count),
        compiler_params=limit(12),
        name="first",
    )(table, *ready(orders[0]))
    count = len(orders[1])
    back = pl.pallas_call(
        functools.partial(bins_kernel, orders=orders, lean=lean, **sizes),
        out_shape=jax.ShapeDtypeStruct((width, packing_probes.tiles, half, LANES), bf16),
        in_specs=in_smem(1) + [in_hbm] + in_vmem(6 + 2 * count),
        out_specs=in_vmem(1)[0],
        scratch_shapes=[pltpu.VMEM((3, count * points, 2 * sens, wide), f32)]
        + scratch(count)
        + [
            pltpu.VMEM((2 * sens * half, 2 * wide), f32),
            pltpu.VMEM((3, 2 * sens * half, wide), f32),
            pltpu.VMEM((width * points * half, 2 * wide), f32),
            pltpu.SMEM(noise_weight.shape, f32),
            pltpu.SemaphoreType.DMA,
        ],
        compiler_params=limit(20),
        name="bins",
    )(
        me, *kept(pltpu.HBM, noise_weight), others[0], table, weights, kern_first, data_first,
        relayed, *ready(orders[1]),
    )
    back, basis_other = lax.optimization_barrier((back, basis_other))
    basis, basis_other = kept(pltpu.VMEM, basis, basis_other)
    parts = exchange(back)
    flat, coeff = pl.pallas_call(
        functools.partial(coeff_kernel, points=points, steps=steps, rank=rank, packing=packing_probes),
        out_shape=(
            jax.ShapeDtypeStruct((half, round_up(points * steps, LANES) + rank), f32),
            jax.ShapeDtypeStruct((width, half, 2 * rank), bf16),
        ),
        in_specs=in_vmem(5),
        out_specs=tuple(in_vmem(2)),
        compiler_params=limit(12),
        name="coeff",
    )(prior_scale[None, :], deflation[None, :], parts, basis, basis_other)
    flat_other = swap(flat)
    coeff_parts = exchange(coeff)
    coeff_other = swap(coeff_parts)
    return pl.pallas_call(
        functools.partial(deflate_kernel, points=points, steps=steps, rank=rank),
        out_shape=jax.ShapeDtypeStruct((probe_count, points, steps), f32),
        in_specs=in_smem(1) + in_vmem(6),
        out_specs=in_vmem(1)[0],
        compiler_params=limit(12),
        name="deflate",
    )(
        core, coeff_parts, coeff_other, flat, flat_other, basis, basis_other,
    )


def solution(mesh):
    placed = (
        P(None, ("grp", "pts"), None),
        P(None, ("grp", "pts"), "sen", None),
        P(("grp", "sen")),
        P("pts"),
        P("pts", "sen"),
        P("sen"),
    )

    def body(*args):
        width = mesh.shape["pts"]
        split = mesh.shape["sen"] == 2 and width == ROWS
        whole_tiles = args[2].shape[0] == width * ROWS and args[0].shape[0] == 2 * ROWS
        if not (split and whole_tiles):
            return local(*args)
        return local_split(*args)

    return jax.shard_map(
        body, mesh=mesh, in_specs=placed, out_specs=P(None, ("grp", "pts"), None), check_vma=False
    )
```

```python
import functools
import math

import jax
import jax.numpy as jnp
import numpy as np
from jax import lax
from jax.experimental import pallas as pl
from jax.experimental.pallas import tpu as pltpu
from jax.sharding import PartitionSpec as P

LANES = 128
ROWS = 8


def tables(steps_count):
    bins_count = steps_count + 1
    turns = (
        jnp.arange(steps_count, dtype=jnp.int32)[:, None]
        * jnp.arange(bins_count, dtype=jnp.int32)[None, :]
        % (2 * steps_count)
    )
    angle = turns.astype(jnp.float32) * (math.pi / steps_count)
    cosine = jnp.cos(angle)
    sine = jnp.sin(angle)
    freq = jnp.arange(bins_count, dtype=jnp.int32)
    edge = (freq == 0) | (freq == steps_count)
    weights = jnp.where(edge, 1.0, 2.0).astype(jnp.float32) / (2.0 * steps_count)
    forward = jnp.concatenate([cosine, -sine], axis=1)
    inverse = jnp.concatenate([cosine * weights[None, :], -sine * weights[None, :]], axis=1)
    return (forward, inverse)


def widened(value):
    return lax.optimization_barrier(value).astype(jnp.float32)


def complex_data(spec_real, spec_imag, kern_real, kern_imag):
    data_real = jnp.einsum(
        "kpf,psf->ksf", spec_real, kern_real, preferred_element_type=jnp.float32
    ) - jnp.einsum("kpf,psf->ksf", spec_imag, kern_imag, preferred_element_type=jnp.float32)
    data_imag = jnp.einsum(
        "kpf,psf->ksf", spec_real, kern_imag, preferred_element_type=jnp.float32
    ) + jnp.einsum("kpf,psf->ksf", spec_imag, kern_real, preferred_element_type=jnp.float32)
    return (data_real, data_imag)


def complex_adjoint(weight_real, weight_imag, kern_real, kern_imag):
    adj_real = jnp.einsum(
        "ksf,psf->kpf", weight_real, kern_real, preferred_element_type=jnp.float32
    ) + jnp.einsum("ksf,psf->kpf", weight_imag, kern_imag, preferred_element_type=jnp.float32)
    adj_imag = jnp.einsum(
        "ksf,psf->kpf", weight_imag, kern_real, preferred_element_type=jnp.float32
    ) - jnp.einsum("ksf,psf->kpf", weight_real, kern_imag, preferred_element_type=jnp.float32)
    return (adj_real, adj_imag)


def local(probes, kernel, noise_weight, prior_scale, basis, deflation):
    highest = lax.Precision.HIGHEST
    probe_count, point_count, steps_count = probes.shape
    bins_count = steps_count + 1
    sensor_count = noise_weight.shape[0]
    forward, inverse = tables(steps_count)
    scaled = probes.astype(jnp.float32) * prior_scale[None, :, None]
    spectrum = jnp.dot(scaled, forward, precision=highest).astype(jnp.bfloat16)
    noise_rows = jnp.tile(noise_weight, probe_count)
    width = lax.axis_size("pts")
    block = (bins_count + width - 1) // width
    extra = block * width - bins_count
    kern_pad = jnp.pad(kernel, ((0, 0), (0, 0), (0, 0), (0, extra)))
    spec_pad = jnp.pad(
        spectrum.reshape(probe_count, point_count, 2, bins_count),
        ((0, 0), (0, 0), (0, 0), (0, extra)),
    )
    kern_bins, spec_bins = (
        lax.all_to_all(kern_pad, "pts", split_axis=3, concat_axis=1, tiled=True),
        lax.all_to_all(spec_pad, "pts", split_axis=3, concat_axis=1, tiled=True),
    )
    bin_kern_real = kern_bins[0]
    bin_kern_imag = kern_bins[1]
    data_real, data_imag = complex_data(
        spec_bins[:, :, 0], spec_bins[:, :, 1], bin_kern_real, bin_kern_imag
    )
    data_bins = jnp.stack([data_real, data_imag], axis=2).reshape(
        probe_count * sensor_count, 2, block
    )
    rows_time = lax.all_to_all(
        data_bins.astype(jnp.bfloat16), "pts", split_axis=0, concat_axis=2, tiled=True
    ).astype(data_bins.dtype)
    local_rows = rows_time.shape[0]
    begin = lax.axis_index("pts") * local_rows
    local_noise = lax.dynamic_slice_in_dim(noise_rows, begin, local_rows)
    data_rows = rows_time[:, :, :bins_count].reshape(local_rows, 2 * bins_count)
    observed = jnp.dot(data_rows, inverse.T, precision=highest)
    residual = (observed * local_noise[:, None]).astype(jnp.bfloat16)
    weighted_local = (
        jnp.dot(widened(residual), inverse, precision=highest)
        .astype(jnp.bfloat16)
        .reshape(local_rows, 2, bins_count)
    )
    weighted_pad = jnp.pad(weighted_local, ((0, 0), (0, 0), (0, extra)))
    weighted_bins = lax.all_to_all(weighted_pad, "pts", split_axis=2, concat_axis=0, tiled=True)
    weighted_bins = weighted_bins.reshape(probe_count, sensor_count, 2, block)
    adj_real, adj_imag = complex_adjoint(
        weighted_bins[:, :, 0], weighted_bins[:, :, 1], bin_kern_real, bin_kern_imag
    )
    adj_bins = jnp.stack([adj_real, adj_imag], axis=2)
    adj_points = lax.all_to_all(
        adj_bins.astype(jnp.bfloat16), "pts", split_axis=1, concat_axis=3, tiled=True
    ).astype(adj_bins.dtype)
    adjoint = adj_points[..., :bins_count].reshape(probe_count, point_count, 2 * bins_count)
    back = jnp.dot(adjoint, forward.T, precision=highest)
    back = lax.psum(back.astype(jnp.bfloat16), "sen").astype(jnp.float32)
    hessian = back * prior_scale[None, :, None]
    flat = hessian.reshape(probe_count, point_count * steps_count)
    flat_low = flat.astype(jnp.bfloat16)
    coeff = jnp.dot(flat_low, basis, preferred_element_type=jnp.float32)
    coeff = lax.psum(coeff, "pts")
    shrunk = (coeff * deflation[None, :]).astype(jnp.bfloat16)
    correction = lax.dot_general(
        shrunk, basis, (((1,), (1,)), ((), ())), preferred_element_type=jnp.float32
    )
    correction = lax.psum(correction.astype(jnp.bfloat16), "sen").astype(jnp.float32)
    return (flat - correction).reshape(probe_count, point_count, steps_count)


def round_up(value, step):
    return (value + step - 1) // step * step


def packed_tables(steps_count, wide):
    bins_count = steps_count + 1
    turns = np.arange(steps_count)[:, None] * np.arange(bins_count)[None, :] % (2 * steps_count)
    angle = turns.astype(np.float64) * (math.pi / steps_count)
    table = np.zeros((wide, 2 * wide), np.float32)
    table[:steps_count, :bins_count] = np.cos(angle)
    table[:steps_count, wide : wide + bins_count] = -np.sin(angle)
    weights = np.zeros((1, wide), np.float32)
    weights[0, :bins_count] = 2.0 / (2.0 * steps_count)
    weights[0, 0] = weights[0, steps_count] = 1.0 / (2.0 * steps_count)
    return jnp.asarray(table.astype(jnp.bfloat16)), jnp.asarray(weights)


NT = (((1,), (1,)), ((), ()))


class Packing:
    def __init__(self, rows, length):
        self.full = length // LANES
        self.tail = length % LANES
        self.slots = LANES // self.tail
        self.first_tail = rows * self.full
        self.tiles = self.first_tail + -(-rows // self.slots)

    def place(self, row):
        return self.first_tail + row // self.slots, row % self.slots * self.tail


def turned(tile, lanes):
    lanes = lanes % LANES
    return pltpu.roll(tile, lanes, axis=tile.ndim - 1) if lanes else tile


def add_tail(packing, row, value, merged):
    tile, lane = packing.place(row)
    tail = value[..., packing.full * LANES : (packing.full + 1) * LANES]
    where = lax.broadcasted_iota(jnp.int32, tail.shape, tail.ndim - 1)
    tail = turned(jnp.where(where < packing.tail, tail, 0.0), lane)
    merged[tile] = merged[tile] + tail if tile in merged else tail


def store_packed(out_tile, packing, row, value, merged):
    for t in range(packing.full):
        lanes = slice(t * LANES, (t + 1) * LANES)
        out_tile(row * packing.full + t, value[..., lanes].astype(jnp.bfloat16))
    add_tail(packing, row, value, merged)


def store_tails(out_tile, merged):
    for tile, value in merged.items():
        out_tile(tile, value.astype(jnp.bfloat16))


def pack_kernel(
    index, core, prior_far, noise_far, kernel, probes, table_far, *refs,
    order, lean, half, packing, packing_probes,
):
    outs = refs[: len(order)]
    table, prior, noise, kernel_here, probes_here, sems = refs[len(order) :]
    f32 = jnp.float32
    bf16 = jnp.bfloat16
    _, points, _ = probes_here.shape
    edge = packing.full * LANES
    me = index[0]
    mine = pl.multiple_of(core[0] * half, half)
    copies = [
        pltpu.make_async_copy(probes.at[pl.ds(mine, half)], probes_here, sems.at[0]),
        pltpu.make_async_copy(prior_far, prior, sems.at[1]),
    ]
    for row in range(2 * points):
        at = (row // points, row % points)
        copies.append(pltpu.make_async_copy(kernel.at[at], kernel_here.at[at], sems.at[2 + row]))
    copies.append(pltpu.make_async_copy(noise_far, noise, sems.at[2 + 2 * points]))
    copies.append(pltpu.make_async_copy(table_far, table, sems.at[3 + 2 * points]))
    for copy in copies:
        copy.start()

    def padded(value):
        missing = jnp.zeros((value.shape[0], edge + LANES - value.shape[1]), f32)
        return jnp.concatenate([value, missing], axis=1)

    copies[0].wait()
    copies[1].wait()
    scaled = probes_here[...].astype(f32)
    tiles = {}
    tails = {}
    for p in range(points):
        value = padded(scaled[:, p, :] * prior[p])
        store_packed(tiles.__setitem__, packing_probes, p, value, tails)
    store_tails(tiles.__setitem__, tails)
    for copy in copies[2:-1]:
        copy.wait()
    for relative, out in zip(order, outs):

        def out_tile(tile, value, out=out):
            out[tile] = value

        if relative not in lean:
            for tile, value in tiles.items():
                out_tile(packing.tiles + tile, value)
        merged = {}
        for row in range(2 * points):
            value = padded(kernel_here[row // points, row % points, me ^ relative].astype(f32))
            store_packed(out_tile, packing, row, value, merged)
        store_tails(out_tile, merged)
    sens = outs[0].shape[1]
    shape = (sens, LANES)
    where = lax.broadcasted_iota(jnp.int32, shape, 0)
    lane = lax.broadcasted_iota(jnp.int32, shape, 1)
    column = jnp.zeros(shape, f32)
    for s in range(sens):
        column = jnp.where(where == s, noise[me * sens + s], column)
    high = column.astype(bf16).astype(f32)
    middle = (column - high).astype(bf16).astype(f32)
    low = column - high - middle
    pieces = jnp.where(lane == 0, high, jnp.where(lane == 1, middle, jnp.where(lane == 2, low, 0.0)))
    outs[0][outs[0].shape[0] - 1] = pieces.astype(bf16)
    copies[-1].wait()


def unpack(source, row, packing, base=0):
    f32 = jnp.float32
    tiles = [source[base + row * packing.full + t].astype(f32) for t in range(packing.full)]
    tile, lane = packing.place(row)
    tiles.append(turned(source[base + tile].astype(f32), -lane))
    return tiles


def widen(sources, kern, *, packing, points):
    for b, source in enumerate(sources):
        for p in range(points):
            real = unpack(source, p, packing)
            imag = unpack(source, points + p, packing)
            for t, (x, y) in enumerate(zip(real, imag)):
                lanes = slice(t * LANES, (t + 1) * LANES)
                kern[0, b * points + p, :, lanes] = x
                kern[1, b * points + p, :, lanes] = x + y
                kern[2, b * points + p, :, lanes] = x - y


def spectra(sources, table, spec, rows, *, packing, points, half, wide):
    for b, (source, base) in enumerate(sources):
        for p in range(points):
            at = slice((b * points + p) * half, (b * points + p + 1) * half)
            for t, tile in enumerate(unpack(source, p, packing, base)):
                rows[at, t * LANES : (t + 1) * LANES] = tile
    got = jnp.dot(rows[...].astype(jnp.bfloat16), table[...], preferred_element_type=jnp.float32)
    real = got[:, :wide]
    imag = got[:, wide:]
    spec[0] = real + imag
    spec[1] = imag
    spec[2] = real


def forward_sum(kern, spec, data, earlier, *, points, sens, half, wide):
    f32 = jnp.float32
    blocks = kern.shape[1] // points

    def tile_step(ft, carry):
        lanes = pl.ds(pl.multiple_of(ft * LANES, LANES), LANES)
        shifted = pl.ds(pl.multiple_of(wide + ft * LANES, LANES), LANES)

        def source(b, acc):
            acc = list(acc)
            for p in range(points):
                q = b * points + p
                at = pl.ds(pl.multiple_of(q * half, ROWS), half)
                both = spec[0, at, lanes]
                imag = spec[1, at, lanes]
                real = spec[2, at, lanes]
                for s in range(sens):
                    row = slice(s, s + 1)
                    acc[3 * s] += kern[0, q, row, lanes] * both
                    acc[3 * s + 1] += kern[1, q, row, lanes] * imag
                    acc[3 * s + 2] += kern[2, q, row, lanes] * real
            return tuple(acc)

        zero = jnp.zeros((half, LANES), f32)
        acc = lax.fori_loop(0, blocks, source, (zero,) * (3 * sens))
        for s in range(sens):
            at = slice(s * half, (s + 1) * half)
            real = acc[3 * s] - acc[3 * s + 1]
            imag = acc[3 * s] - acc[3 * s + 2]
            if earlier is not None:
                real += earlier[at, lanes]
                imag += earlier[at, shifted]
            data[at, lanes] = real
            data[at, shifted] = imag
        return carry

    lax.fori_loop(0, wide // LANES, tile_step, 0)


def own_kernel(table, *refs, places, points, sens, half, wide, packing, packing_probes):
    count = len(places)
    sources = refs[:count]
    *extra, spec, kern, data, rows = refs[count:]
    probes = [(sources[b] if at is None else extra[0], packing.tiles if at is None else at)
              for b, at in enumerate(places)]
    spectra(probes, table, spec, rows, packing=packing_probes, points=points, half=half, wide=wide)
    widen(sources, kern, packing=packing, points=points)
    earlier = extra[-1] if len(extra) == 2 else None
    forward_sum(kern, spec, data, earlier, points=points, sens=sens, half=half, wide=wide)


def other_kernel(spec, *refs, count, points, sens, half, wide, packing, packing_probes):
    kern, data = refs[count:]
    widen(refs[:count], kern, packing=packing, points=points)
    forward_sum(kern, spec, data, None, points=points, sens=sens, half=half, wide=wide)


def bins_kernel(
    index, noise_far, neighbour, table, weights, kern_soon, kern_soon_other, data_other, spec,
    kern_later, data_own, *refs,
    orders, points, sens, half, wide, packing, packing_probes,
):
    count = len(orders[1])
    out, kern, data, wdata, adjoint, noise_own, sem = refs[count:]
    copy = pltpu.make_async_copy(noise_far, noise_own, sem)
    copy.start()
    tiles = wide // LANES
    f32 = jnp.float32
    bf16 = jnp.bfloat16
    own_rows = sens * half
    widen(refs[:count], kern, packing=packing, points=points)
    forward_sum(
        kern, spec, data.at[own_rows:], data_other, points=points, sens=sens, half=half, wide=wide
    )
    data[:own_rows] = data_own[...]
    table_v = table[...]
    weight_rows = weights[...]
    scaled = jnp.concatenate(
        [data[:, :wide] * weight_rows, data[:, wide:] * weight_rows], axis=1
    ).astype(bf16)
    observed = lax.dot_general(scaled, table_v, NT, preferred_element_type=f32)
    copy.wait()
    pieces = neighbour[neighbour.shape[0] - 1].astype(f32)
    column = pieces[:, 0:1] + pieces[:, 1:2] + pieces[:, 2:3]
    scales = [noise_own[index[0] * sens + s] for s in range(sens)]
    scales += [column[s : s + 1] for s in range(sens)]
    residual = jnp.concatenate(
        [observed[s * half : (s + 1) * half] * scale for s, scale in enumerate(scales)], axis=0
    ).astype(bf16)
    weighted = jnp.dot(residual, table_v, preferred_element_type=f32)
    real = weighted[:, :wide] * weight_rows
    imag = weighted[:, wide:] * weight_rows
    wdata[0] = real + imag
    wdata[1] = imag
    wdata[2] = real

    base = 0
    group = 2 * points
    for sources, order in (
        ((kern_soon, kern_soon_other), orders[0]),
        ((kern_later, kern), orders[1]),
    ):

        def adjoint_tile(step, carry, sources=sources, base=base):
            first = step // tiles * group
            ft = step % tiles
            lanes = pl.ds(pl.multiple_of(ft * LANES, LANES), LANES)
            shifted = pl.ds(pl.multiple_of(wide + ft * LANES, LANES), LANES)
            zero = jnp.zeros((half, LANES), f32)
            acc = [zero] * (3 * group)
            for s in range(2 * sens):
                at = slice(s * half, (s + 1) * half)
                both = wdata[0, at, lanes]
                imag = wdata[1, at, lanes]
                real = wdata[2, at, lanes]
                source = sources[s // sens]
                row = slice(s % sens, s % sens + 1)
                for p in range(group):
                    acc[3 * p] += source[0, first + p, row, lanes] * both
                    acc[3 * p + 1] += source[2, first + p, row, lanes] * imag
                    acc[3 * p + 2] += source[1, first + p, row, lanes] * real
            for p in range(group):
                at = pl.ds(pl.multiple_of((base + first + p) * half, ROWS), half)
                adjoint[at, lanes] = acc[3 * p] - acc[3 * p + 1]
                adjoint[at, shifted] = acc[3 * p] - acc[3 * p + 2]
            return carry

        lax.fori_loop(0, len(order) * points // group * tiles, adjoint_tile, 0)
        base += len(order) * points
    back = lax.dot_general(adjoint[...].astype(bf16), table_v, NT, preferred_element_type=f32)
    for b, relative in enumerate(orders[0] + orders[1]):
        there = index[0] ^ relative

        def out_tile(tile, value, there=there):
            out[there, tile] = value

        merged = {}
        for p in range(points):
            at = slice((b * points + p) * half, (b * points + p + 1) * half)
            store_packed(out_tile, packing_probes, p, back[at], merged)
        store_tails(out_tile, merged)


def summed(parts):
    total = parts[0].astype(jnp.float32)
    for j in range(1, parts.shape[0]):
        total += parts[j].astype(jnp.float32)
    return total


def coeff_kernel(
    prior, deflation, parts, basis_own, basis_other, flat, coeff, *, points, steps, rank, packing
):
    f32 = jnp.float32
    total = summed(parts)
    for p in range(points):
        tiles = [total[p * packing.full + t] for t in range(packing.full)]
        tile, lane = packing.place(p)
        tiles.append(turned(total[tile], -lane))
        piece = jnp.concatenate(tiles, axis=1) * prior[:, p : p + 1]
        flat[:, p * steps : (p + 1) * steps] = piece[:, :steps]
    low = flat[:, : points * steps].astype(jnp.bfloat16)
    behind = flat.shape[1] - rank
    flat[:, behind:] = jnp.broadcast_to(deflation[...], (flat.shape[0], rank))
    own = jnp.dot(low, basis_own[...], preferred_element_type=f32).astype(jnp.bfloat16)
    other = jnp.dot(low, basis_other[...], preferred_element_type=f32).astype(jnp.bfloat16)
    for j in range(coeff.shape[0]):
        coeff[j, :, :rank] = own
        coeff[j, :, rank:] = other


def deflate_kernel(
    core, parts_own, parts_other, flat_own, flat_other, basis_own, basis_other, out,
    *, points, steps, rank,
):
    f32 = jnp.float32
    bf16 = jnp.bfloat16
    own = summed(parts_own)
    other = summed(parts_other)
    half = own.shape[0]
    behind = flat_own.shape[1] - rank
    deflation_own = flat_own[0:1, behind:]
    deflation_other = flat_other[0:1, behind:]
    size = points * steps
    here = jnp.concatenate([own[:, :rank], other[:, rank:]], axis=0) * deflation_own
    there = jnp.concatenate([own[:, rank:], other[:, :rank]], axis=0) * deflation_other
    correction = lax.dot_general(here.astype(bf16), basis_own[...], NT, preferred_element_type=f32)
    correction += lax.dot_general(there.astype(bf16), basis_other[...], NT, preferred_element_type=f32)
    result = jnp.concatenate([flat_own[:, :size], flat_other[:, :size]], axis=0) - correction
    mine = core[0] * half
    for p in range(points):
        piece = result[:, p * steps : (p + 1) * steps]
        out[pl.ds(mine, half), p, :] = piece[:half]
        out[pl.ds(half - mine, half), p, :] = piece[half:]


def split_order(width):
    middle, half = width // 4, width // 2
    soon = [0, half, 1, middle]
    return soon, [half + middle, half + 1, middle + 1, half + middle + 1]


def lean_partners(width):
    return [r for r in range(width // 2, width) if r % 2]


def relay_kernel(*refs, first_tile):
    sources, out = refs[:-1], refs[-1]
    count = out.shape[0] // len(sources)
    for n, source in enumerate(sources):
        out[n * count : (n + 1) * count] = source[first_tile:]


def kept(space, *values):
    return [pltpu.with_memory_space_constraint(value, space) for value in values]


def in_vmem(count):
    return [pl.BlockSpec(memory_space=pltpu.VMEM) for _ in range(count)]


def in_smem(count):
    return [pl.BlockSpec(memory_space=pltpu.SMEM) for _ in range(count)]


def limit(mib):
    return pltpu.CompilerParams(vmem_limit_bytes=mib * 1024 * 1024)


def local_split(probes, kernel, noise_weight, prior_scale, basis, deflation):
    bf16 = jnp.bfloat16
    f32 = jnp.float32
    probe_count, points, steps = probes.shape
    bins_count = steps + 1
    width = lax.axis_size("pts")
    sens = noise_weight.shape[0] // width
    half = probe_count // 2
    rank = basis.shape[1]
    wide = round_up(bins_count, LANES)
    me = jnp.full((1,), lax.axis_index("pts"), jnp.int32)
    core_index = lax.axis_index("sen")
    core = jnp.full((1,), core_index, jnp.int32)

    def swap(value):
        return lax.ppermute(value, "sen", [(0, 1), (1, 0)])

    def exchange(value):
        return lax.all_to_all(value, "pts", split_axis=0, concat_axis=0, tiled=False)

    table, weights = packed_tables(steps, wide)
    packing = Packing(2 * points, bins_count)
    packing_probes = Packing(points, steps)
    packings = dict(packing=packing, packing_probes=packing_probes)
    sizes = dict(points=points, sens=sens, half=half, wide=wide, **packings)
    orders = split_order(width)
    order = orders[0] + orders[1]
    lean = lean_partners(width)

    def chunk(tiles):
        return jax.ShapeDtypeStruct((tiles, sens, LANES), bf16)

    both = packing.tiles + packing_probes.tiles
    tiles = [packing.tiles if r in lean else both for r in order]
    tiles[0] += 1
    in_hbm = pl.BlockSpec(memory_space=pltpu.HBM)
    *sent, table = pl.pallas_call(
        functools.partial(pack_kernel, order=order, lean=lean, half=half, **packings),
        out_shape=tuple(chunk(count) for count in tiles) + (pltpu.VMEM(table.shape, bf16),),
        in_specs=in_smem(2) + [in_hbm] * 5,
        out_specs=tuple(in_vmem(width + 1)),
        scratch_shapes=[
            pltpu.SMEM(prior_scale.shape, f32),
            pltpu.SMEM(noise_weight.shape, f32),
            pltpu.VMEM((2, points, width, sens, bins_count), bf16),
            pltpu.VMEM((half, points, steps), bf16),
            pltpu.SemaphoreType.DMA((4 + 2 * points,)),
        ],
        compiler_params=limit(8),
        name="pack",
    )(
        me,
        core,
        *kept(
            pltpu.HBM,
            prior_scale,
            noise_weight,
            kernel.reshape(2, points, width, sens, bins_count),
            probes,
            table,
        ),
    )
    blocks = {}
    others = {}
    for relative, value in zip(order, sent):
        if relative:
            value = lax.ppermute(value, "pts", [(i, i ^ relative) for i in range(width)])
        blocks[relative] = value
        others[relative] = swap(value)
    relayed = pl.pallas_call(
        functools.partial(relay_kernel, first_tile=packing.tiles),
        out_shape=chunk(len(lean) * packing_probes.tiles),
        in_specs=in_vmem(len(lean)),
        out_specs=in_vmem(1)[0],
        compiler_params=limit(2),
        name="relay",
    )(*[blocks[r ^ 1] for r in lean])
    relayed = lax.ppermute(relayed, "pts", [(i, i ^ 1) for i in range(width)])
    basis_other = swap(basis)

    def sums(rows):
        return jax.ShapeDtypeStruct((rows, 2 * wide), f32)

    def kern_of(part):
        return jax.ShapeDtypeStruct((3, len(part) * points, sens, wide), f32)

    def own_sums(part, extra):
        rows = len(part) * points * half
        at = [lean.index(r) * packing_probes.tiles if r in lean else None for r in part]
        values = [blocks[r] for r in part] + extra
        return pl.pallas_call(
            functools.partial(own_kernel, places=at, **sizes),
            out_shape=(jax.ShapeDtypeStruct((3, rows, wide), f32), kern_of(part), sums(sens * half)),
            in_specs=in_vmem(1 + len(values)),
            out_specs=tuple(in_vmem(3)),
            scratch_shapes=[pltpu.VMEM((rows, wide), f32)],
            compiler_params=limit(10),
        )(table, *values)

    soon, later = orders
    spec_soon, kern_soon, data_soon = own_sums(soon, [])
    kern_soon_other, data_other = pl.pallas_call(
        functools.partial(other_kernel, count=len(soon), **sizes),
        out_shape=(kern_of(soon), sums(sens * half)),
        in_specs=in_vmem(1 + len(soon)),
        out_specs=tuple(in_vmem(2)),
        compiler_params=limit(8),
        name="second",
    )(spec_soon, *[others[r] for r in soon])
    spec, kern_later, data_own = own_sums(later, [relayed, data_soon])
    back = pl.pallas_call(
        functools.partial(bins_kernel, orders=orders, **sizes),
        out_shape=jax.ShapeDtypeStruct((width, packing_probes.tiles, half, LANES), bf16),
        in_specs=in_smem(1) + [in_hbm] + in_vmem(9 + len(later)),
        out_specs=in_vmem(1)[0],
        scratch_shapes=[
            pltpu.VMEM((3, len(later) * points, sens, wide), f32),
            pltpu.VMEM((2 * sens * half, 2 * wide), f32),
            pltpu.VMEM((3, 2 * sens * half, wide), f32),
            pltpu.VMEM((width * points * half, 2 * wide), f32),
            pltpu.SMEM(noise_weight.shape, f32),
            pltpu.SemaphoreType.DMA,
        ],
        compiler_params=limit(20),
        name="bins",
    )(
        me, *kept(pltpu.HBM, noise_weight), others[0], table, weights, kern_soon, kern_soon_other,
        data_other, spec, kern_later, data_own, *[others[r] for r in later],
    )
    back, basis_other = lax.optimization_barrier((back, basis_other))
    basis, basis_other = kept(pltpu.VMEM, basis, basis_other)
    parts = exchange(back)
    flat, coeff = pl.pallas_call(
        functools.partial(coeff_kernel, points=points, steps=steps, rank=rank, packing=packing_probes),
        out_shape=(
            jax.ShapeDtypeStruct((half, round_up(points * steps, LANES) + rank), f32),
            jax.ShapeDtypeStruct((width, half, 2 * rank), bf16),
        ),
        in_specs=in_vmem(5),
        out_specs=tuple(in_vmem(2)),
        compiler_params=limit(12),
        name="coeff",
    )(prior_scale[None, :], deflation[None, :], parts, basis, basis_other)
    flat_other = swap(flat)
    coeff_parts = exchange(coeff)
    coeff_other = swap(coeff_parts)
    return pl.pallas_call(
        functools.partial(deflate_kernel, points=points, steps=steps, rank=rank),
        out_shape=jax.ShapeDtypeStruct((probe_count, points, steps), f32),
        in_specs=in_smem(1) + in_vmem(6),
        out_specs=in_vmem(1)[0],
        compiler_params=limit(12),
        name="deflate",
    )(
        core, coeff_parts, coeff_other, flat, flat_other, basis, basis_other,
    )


def solution(mesh):
    placed = (
        P(None, ("grp", "pts"), None),
        P(None, ("grp", "pts"), "sen", None),
        P(("grp", "sen")),
        P("pts"),
        P("pts", "sen"),
        P("sen"),
    )

    def body(*args):
        width = mesh.shape["pts"]
        split = mesh.shape["sen"] == 2 and width == ROWS
        whole_tiles = args[2].shape[0] == width * ROWS and args[0].shape[0] == 2 * ROWS
        if not (split and whole_tiles):
            return local(*args)
        return local_split(*args)

    return jax.shard_map(
        body, mesh=mesh, in_specs=placed, out_specs=P(None, ("grp", "pts"), None), check_vma=False
    )
```
